8 devices in a mesh: dp: 8 (over z, y, x, core).
Axes of the slice: x: 2, y: 2, z: 1, core: 2. Of those that a mesh axis runs over, the one named last changes fastest.
Arguments:
- u_norm: bfloat16 [16, 2048, 2048], P(None, 'dp')
- expert_idx: int32 [16, 2048, 8], P(None, 'dp')
- expert_out: bfloat16 [16, 2048, 8, 2048], P(None, 'dp')
- d_out: bfloat16 [16, 2048, 2048], P(None, 'dp')
- w_router: bfloat16 [16, 2048, 64], replicated
Outputs:
- output 1: float32 [], replicated
- output 2: float32 [16, 2048, 64], replicated
- output 3: bfloat16 [16, 2048, 2048], P(None, 'dp')
All inputs are finite; a program needn't handle non-finite values.
Results may differ from the reference program's by a relative error of at most 0.00919422.
Values sent between devices are 32-bit elements.
A program may use at most 1 GiB of HBM per device.

```python
import jax
import jax.numpy as jnp
from jax import lax

LAYERS = 16
GROUP = 8
TOK_DEV = 256
D = 2048
EXPERTS = 64
TOP = 8

TOKENS = GROUP * TOK_DEV
AUX_COEF = 0.02
LOSS_SCALE = 1.0 * TOKENS
DY_SCALE = 0.015 * (TOP / (EXPERTS * TOKENS * D)) ** 0.5


def draw_slots(slot_key):
    expert_ids = jnp.arange(EXPERTS)
    tok_pos = jnp.arange(TOKENS)
    tok_owner = tok_pos // TOK_DEV
    favored = (expert_ids[None, :] == (tok_owner % EXPERTS)[:, None]).astype(jnp.int32)
    weights = 1 + expert_ids[None, :] % 3 + 12 * favored
    tickets = jax.random.randint(slot_key, (LAYERS, TOKENS, EXPERTS), 0, 4096)
    int_score = weights[None] * tickets * EXPERTS + expert_ids
    drawn_ids = lax.top_k(int_score, TOP)[1]
    forced = (tok_pos[:, None] + jnp.arange(TOP)[None, :]) % EXPERTS
    chosen_ids = jnp.where((tok_pos < EXPERTS)[None, :, None], forced[None], drawn_ids)
    return chosen_ids.astype(jnp.int32)


def setup_inputs(seed: int = 0) -> dict:
    base_key = jax.random.key(seed)
    key_list = jax.random.split(base_key, 7)
    global_mean = 0.5 * jax.random.normal(key_list[0], (LAYERS, 1, D), jnp.float32)
    device_mean = 0.5 * jax.random.normal(key_list[1], (LAYERS, GROUP, 1, D), jnp.float32)
    noise_vals = jax.random.normal(key_list[2], (LAYERS, GROUP, TOK_DEV, D), jnp.float32)
    u_vals = (noise_vals + device_mean).reshape(LAYERS, TOKENS, D) + global_mean
    expert_out = jax.random.normal(key_list[4], (LAYERS, TOKENS, TOP, D), jnp.float32)
    d_out = DY_SCALE * jax.random.normal(key_list[5], (LAYERS, TOKENS, D), jnp.float32)
    w_router = jax.random.normal(key_list[6], (LAYERS, D, EXPERTS), jnp.float32) * D ** -0.5
    return {
        'u_norm': u_vals.astype(jnp.bfloat16),
        'expert_idx': draw_slots(key_list[3]),
        'expert_out': expert_out.astype(jnp.bfloat16),
        'd_out': d_out.astype(jnp.bfloat16),
        'w_router': w_router.astype(jnp.bfloat16),
    }


def reference(u_norm, expert_idx, expert_out, d_out, w_router):
    def one_layer(layer_in):
        u_layer, idx_layer, out_layer, dy_layer, w_layer = layer_in
        logits = jnp.dot(u_layer, w_layer, preferred_element_type=jnp.float32)
        slot_dots = jnp.einsum('tkd,td->tk', out_layer.astype(jnp.float32), dy_layer.astype(jnp.float32))
        one_hot = jax.nn.one_hot(idx_layer, EXPERTS, dtype=jnp.float32)
        exp_frac = jnp.sum(one_hot, axis=(0, 1)) / (TOP * TOKENS)

        def loss_of(logit_in):
            prob_vals = jax.nn.softmax(logit_in, axis=-1)
            gate_vals = jax.nn.softmax(jnp.take_along_axis(logit_in, idx_layer, axis=-1), axis=-1)
            main_part = jnp.sum(gate_vals * slot_dots)
            aux_part = EXPERTS * jnp.sum(exp_frac * jnp.mean(prob_vals, axis=0))
            return main_part + AUX_COEF * aux_part

        layer_loss, pull_back = jax.vjp(loss_of, logits)
        d_logits = pull_back(jnp.ones_like(layer_loss) * LOSS_SCALE)[0]
        d_log16 = d_logits.astype(jnp.bfloat16)
        grad_w = jnp.dot(u_layer.T, d_log16, preferred_element_type=jnp.float32)
        grad_u = jnp.dot(d_log16, w_layer.T, preferred_element_type=jnp.float32).astype(jnp.bfloat16)
        return layer_loss, grad_w, grad_u

    layer_losses, d_router, d_norm = lax.map(one_layer, (u_norm, expert_idx, expert_out, d_out, w_router))
    return (jnp.sum(layer_losses), d_router, d_norm)
```

```python
import jax
import jax.numpy as jnp
from jax import lax
from jax.experimental import pallas as pl
from jax.experimental.pallas import tpu as pltpu
from jax.sharding import PartitionSpec as P

AUX_COEF = 0.02
MESH = pl.DeviceIdType.MESH

NB = 8
NC = 4
NU = 3
AGL = 7

NT = (((1,), (1,)), ((), ()))
TN = (((0,), (0,)), ((), ()))


def step_kernel(n_lay, n_dev, tok_all, idx_hbm, eo_hbm, dy_hbm, u_hbm, w_hbm,
                fin, gout, wv, loss_out,
                idx_v, ebuf, ubuf, dbuf, part, rd, r1, r2, cnt_src, cnt_in, loss_src, loss_in,
                fcol, slot_v, loss_acc,
                idx_sem, e_sem, u_sem, d_sem, w_sem, cs_sem, cr_sem, ls_sem, lr_sem, s_sem, r_sem):
    me = lax.axis_index('dp')
    core = me % 2
    xpos = (me // 2) % 2
    ypos = me // 4
    partner = me + 1 - 2 * core
    xn = me + 2 - 4 * xpos
    yn = me + 4 - 8 * ypos
    nbr_a = xn * (1 - core) + yn * core
    nbr_b = yn * (1 - core) + xn * core
    pa = xpos * (1 - core) + ypos * core
    pb = ypos * (1 - core) + xpos * core
    half = 4 * core
    quart = half + 2 * pa
    mine = quart + pb
    n_exp = w_hbm.shape[1]
    top_k = idx_hbm.shape[1]
    tok = u_hbm.shape[1]
    rows = ebuf.shape[1]
    ctok = rows // top_k

    def e_copy(lay, c, slot):
        return pltpu.make_async_copy(eo_hbm.at[lay, pl.ds(c * rows, rows)], ebuf.at[slot], e_sem.at[slot])

    def u_copy(lay):
        return pltpu.make_async_copy(u_hbm.at[lay], ubuf.at[lay % NU], u_sem.at[lay % NU])

    def d_copy(lay):
        return pltpu.make_async_copy(dy_hbm.at[lay], dbuf.at[lay % NU], d_sem.at[lay % NU])

    def w_copy(lay):
        return pltpu.make_async_copy(w_hbm.at[lay], wv.at[lay], w_sem.at[lay])

    idx_copy = pltpu.make_async_copy(idx_hbm, idx_v, idx_sem)
    idx_copy.start()
    for c in range(2):
        if c == 0:
            w_copy(0).start()
            u_copy(0).start()
            d_copy(0).start()
        else:
            w_copy(1).start()
            u_copy(1).start()
            d_copy(1).start()
        for j in range(NC):
            e_copy(c, j, c * NC + j).start()

    barrier = pltpu.get_barrier_semaphore()
    for d in range(1, n_dev):
        pl.semaphore_signal(barrier, inc=1, device_id=((me + d) % n_dev,), device_id_type=MESH)

    idx_copy.wait()
    ones = jnp.ones((8, tok), jnp.bfloat16)
    row_id = lax.broadcasted_iota(jnp.int32, (8, 2 * n_exp), 0)
    e_id = lax.broadcasted_iota(jnp.int32, (n_exp, tok), 0)
    cnt = jnp.zeros((8, 2 * n_exp), jnp.float32)
    for r in range(n_lay // 2):
        hots = []
        for h in range(2):
            ids = idx_v[2 * r + h]
            acc = jnp.zeros((n_exp, tok), jnp.float32)
            for k in range(top_k):
                acc = jnp.where(e_id == ids[k:k + 1], 1.0, acc)
            hots.append(acc.astype(jnp.bfloat16))
        both = jnp.concatenate(hots, axis=0)
        res = lax.dot_general(ones, both, NT, preferred_element_type=jnp.float32)
        cnt = jnp.where(row_id == r, res, cnt)
    cnt_src[...] = cnt
    cnt_in[me] = cnt
    loss_acc[...] = jnp.zeros_like(loss_acc)
    pl.semaphore_wait(barrier, n_dev - 1)

    def cnt_copy(to, frm):
        return pltpu.make_async_remote_copy(
            src_ref=cnt_src, dst_ref=cnt_in.at[frm], send_sem=cs_sem.at[to], recv_sem=cr_sem.at[frm],
            device_id=(to,), device_id_type=MESH)

    def loss_copy(to, frm):
        return pltpu.make_async_remote_copy(
            src_ref=loss_src, dst_ref=loss_in.at[frm], send_sem=ls_sem.at[to], recv_sem=lr_sem.at[frm],
            device_id=(to,), device_id_type=MESH)

    for d in range(1, n_dev):
        cnt_copy((me + d) % n_dev, me).start()

    def rcopy(stage, src, dst, m, dev):
        return pltpu.make_async_remote_copy(
            src_ref=src, dst_ref=dst, send_sem=s_sem.at[stage, m], recv_sem=r_sem.at[stage, m],
            device_id=(dev,), device_id_type=MESH)

    def c_pair(m):
        return rcopy(0, part.at[m, pl.ds(4 - half, 4)], rd.at[m], m, partner)

    def c_rs1(m):
        return rcopy(1, part.at[m, pl.ds(half + 2 - 2 * pa, 2)], r1.at[m], m, nbr_a)

    def c_rs2(m):
        return rcopy(2, part.at[m, pl.ds(quart + 1 - pb, 1)], r2.at[m], m, nbr_b)

    def c_ag1(m, p):
        return rcopy(3, fin.at[m, pl.ds(p, 1)], fin.at[m, pl.ds(p, 1)], m, nbr_b)

    def c_ag2(m, p):
        return rcopy(4, fin.at[m, pl.ds(p, 2)], fin.at[m, pl.ds(p, 2)], m, nbr_a)

    def c_out(m, p):
        return rcopy(5, fin.at[m, pl.ds(p, 4)], fin.at[m, pl.ds(p, 4)], m, partner)

    def do_a(m):
        c_pair(m).wait_recv()
        o = 2 - 2 * pa
        part[m, pl.ds(half + o, 2)] += rd[m, pl.ds(o, 2)]
        part[m, pl.ds(quart, 2)] += rd[m, pl.ds(2 * pa, 2)]
        c_rs1(m).start()

    def do_b(m):
        c_rs1(m).wait_recv()
        o = 1 - pb
        part[m, pl.ds(quart + o, 1)] += r1[m, pl.ds(o, 1)]
        part[m, pl.ds(mine, 1)] += r1[m, pl.ds(pb, 1)]
        c_rs2(m).start()

    def do_c(m):
        c_rs2(m).wait_recv()
        fin[m, pl.ds(mine, 1)] = part[m, pl.ds(mine, 1)] + r2[m]

    def do_ag1(m):
        c_ag1(m, mine).start()

    def do_d(m):
        c_ag1(m, quart + 1 - pb).wait_recv()
        c_ag2(m, quart).start()

    def do_e(m):
        c_ag2(m, half + 2 - 2 * pa).wait_recv()
        c_out(m, half).start()

    def do_f(m):
        c_out(m, 4 - half).wait_recv()

    def slot_chunk(lay, c, slot):
        e_copy(lay, c, slot).wait()
        lanes = 2 * ctok
        lo = (c // 2) * lanes
        dcols = dbuf[lay % NU, lo:lo + lanes, :]
        s = lax.dot_general(ebuf[slot], dcols, NT, preferred_element_type=jnp.float32)
        lane = lax.broadcasted_iota(jnp.int32, (top_k, lanes), 1)
        acc = jnp.zeros((top_k, lanes), jnp.float32)
        for i in range(ctok):
            acc = jnp.where(lane == (c % 2) * ctok + i, s[i * top_k:(i + 1) * top_k], acc)
        if c % 2:
            slot_v[:, lo:lo + lanes] += acc
        else:
            slot_v[:, lo:lo + lanes] = acc

        @pl.when(lay + 2 < n_lay)
        def _():
            e_copy(lay + 2, c, slot).start()

    scale = float(tok_all)
    pull = AUX_COEF * n_exp / (top_k * tok_all)

    @pl.loop(0, n_lay)
    def _(lay):
        @pl.when(lay + 2 < n_lay)
        def _():
            w_copy(lay + 2).start()
            u_copy(lay + 2).start()
            d_copy(lay + 2).start()

        base = (lay % 2) * NC
        w_copy(lay).wait()
        u_copy(lay).wait()
        d_copy(lay).wait()
        slot_chunk(lay, 0, base)

        @pl.when(lay >= 1)
        def _():
            do_a(lay - 1)

        slot_chunk(lay, 1, base + 1)

        @pl.when(lay >= 2)
        def _():
            do_b(lay - 2)

        slot_chunk(lay, 2, base + 2)

        @pl.when(lay >= 3)
        def _():
            do_c(lay - 3)

            @pl.when(lay - 3 < AGL)
            def _():
                do_ag1(lay - 3)

        slot_chunk(lay, 3, base + 3)

        @pl.when(jnp.logical_and(lay >= 4, lay - 4 < AGL))
        def _():
            do_d(lay - 4)

        @pl.when(jnp.logical_and(lay >= 5, lay - 5 < AGL))
        def _():
            do_e(lay - 5)

        u = ubuf[lay % NU]
        logits = lax.dot_general(wv[lay], u, NT, preferred_element_type=jnp.float32)
        ex = jnp.exp(logits - jnp.max(logits, axis=0, keepdims=True))
        prob = ex / jnp.sum(ex, axis=0, keepdims=True)
        ids = idx_v[lay]
        chosen = jnp.concatenate(
            [jnp.sum(jnp.where(e_id == ids[k:k + 1], logits, 0.0), axis=0, keepdims=True) for k in range(top_k)], axis=0)
        ge = jnp.exp(chosen - jnp.max(chosen, axis=0, keepdims=True))
        gate = ge / jnp.sum(ge, axis=0, keepdims=True)

        @pl.when(lay == 0)
        def _():
            for d in range(1, n_dev):
                cnt_copy((me + d) % n_dev, (me + d) % n_dev).wait_recv()
            tot = cnt_in[0]
            for j in range(1, n_dev):
                tot = tot + cnt_in[j]
            cols = jnp.transpose(tot * pull)
            for i in range(n_lay):
                o = (i % 2) * n_exp
                fcol[i] = jnp.broadcast_to(cols[o:o + n_exp, i // 2:i // 2 + 1], (n_exp, fcol.shape[2]))

        slots = slot_v[...]
        dd = scale * slots
        dch = gate * (dd - jnp.sum(gate * dd, axis=0, keepdims=True))
        fc = fcol[lay]
        fa = jnp.concatenate([fc] * (tok // fc.shape[1]), axis=1)
        pf = prob * fa
        pf_sum = jnp.sum(pf, axis=0, keepdims=True)
        g = pf - prob * pf_sum
        for k in range(top_k):
            g = g + jnp.where(e_id == ids[k:k + 1], dch[k:k + 1], 0.0)
        main = gate * slots
        first = lax.broadcasted_iota(jnp.int32, (top_k, tok), 0) == 0
        main = main + jnp.where(first, pf_sum * (1.0 / tok_all), 0.0)
        loss_acc[...] += main
        g16 = g.astype(jnp.bfloat16)
        gout[lay] = g16
        pg = jnp.dot(g16, u, preferred_element_type=jnp.float32)
        part[lay] = pg.reshape(part.shape[1:])
        c_pair(lay).start()

    last = n_lay - 1
    la = loss_acc[...]
    lv = la[:, :128]
    for j in range(1, tok // 128):
        lv = lv + la[:, 128 * j:128 * (j + 1)]
    loss_src[...] = lv
    loss_in[me] = lv
    do_a(last)
    do_b(last - 1)
    for d in range(1, n_dev):
        loss_copy((me + d) % n_dev, me).start()
    do_c(last - 2)

    @pl.loop(AGL, last - 1)
    def _(m):
        do_ag1(m)

    do_b(last)
    do_c(last - 1)
    do_ag1(last - 1)

    @pl.loop(AGL, last - 1)
    def _(m):
        do_d(m)

    do_c(last)
    do_ag1(last)
    do_d(last - 1)

    @pl.loop(AGL, last - 1)
    def _(m):
        do_e(m)

    do_d(last)
    do_e(last - 1)
    do_e(last)

    for d in range(1, n_dev):
        loss_copy((me + d) % n_dev, (me + d) % n_dev).wait_recv()
    tot = loss_in[0]
    for j in range(1, n_dev):
        tot = tot + loss_in[j]
    loss_out[...] = tot
    for d in range(1, n_dev):
        cnt_copy((me + d) % n_dev, me).wait_send()
        loss_copy((me + d) % n_dev, me).wait_send()

    @pl.loop(0, n_lay)
    def _(m):
        do_f(m)
        c_pair(m).wait_send()
        c_rs1(m).wait_send()
        c_rs2(m).wait_send()
        c_ag1(m, mine).wait_send()
        c_ag2(m, quart).wait_send()
        c_out(m, half).wait_send()


NS = 4


def out_kernel(n_lay, g_v, w_v, f_v, l_v, dn_hbm, dr_hbm, loss, stage, st_sem, f_sem):
    f_copy = pltpu.make_async_copy(f_v, dr_hbm, f_sem)

    def put(lay):
        return pltpu.make_async_copy(stage.at[lay % NS], dn_hbm.at[lay], st_sem.at[lay % NS])

    f_copy.start()
    loss[0, 0] = jnp.sum(l_v[...])

    @pl.loop(0, n_lay)
    def _(lay):
        @pl.when(lay >= NS)
        def _():
            put(lay - NS).wait()

        dn = lax.dot_general(g_v[lay], w_v[lay], TN, preferred_element_type=jnp.float32)
        stage[lay % NS] = dn.astype(jnp.bfloat16)
        put(lay).start()

    for i in range(NS):
        put(n_lay - NS + i).wait()
    f_copy.wait()


def solution(mesh):
    n_dev = mesh.shape['dp']

    def local_step(u_norm, expert_idx, expert_out, d_out, w_router):
        n_lay, tok, dim = u_norm.shape
        n_exp = w_router.shape[2]
        top_k = expert_idx.shape[2]
        tok_all = tok * n_dev
        f32, bf16 = jnp.float32, jnp.bfloat16
        idx_t = jnp.swapaxes(expert_idx, 1, 2)
        w_t = jnp.swapaxes(w_router, 1, 2)
        eo = expert_out.reshape(n_lay, tok * top_k, dim)
        rows = tok * top_k // NC
        pieces = 8
        prow = n_exp // pieces
        any_spec = pl.BlockSpec(memory_space=pl.ANY)
        vm_spec = pl.BlockSpec(memory_space=pltpu.VMEM)
        dma = pltpu.SemaphoreType.DMA
        fin, g_all, w_all, loss_v = pl.pallas_call(
            lambda *refs: step_kernel(n_lay, n_dev, tok_all, *refs),
            out_shape=(
                pltpu.VMEM((n_lay, pieces, prow, dim), f32),
                pltpu.VMEM((n_lay, n_exp, tok), bf16),
                pltpu.VMEM((n_lay, n_exp, dim), bf16),
                pltpu.VMEM((8, 128), f32),
            ),
            in_specs=[any_spec] * 5,
            out_specs=(vm_spec,) * 4,
            scratch_shapes=[
                pltpu.VMEM((n_lay, top_k, tok), jnp.int32),
                pltpu.VMEM((NB, rows, dim), bf16),
                pltpu.VMEM((NU, tok, dim), bf16),
                pltpu.VMEM((NU, tok, dim), bf16),
                pltpu.VMEM((n_lay, pieces, prow, dim), f32),
                pltpu.VMEM((n_lay, pieces // 2, prow, dim), f32),
                pltpu.VMEM((n_lay, pieces // 4, prow, dim), f32),
                pltpu.VMEM((n_lay, pieces // 8, prow, dim), f32),
                pltpu.VMEM((8, 128), f32),
                pltpu.VMEM((n_dev, 8, 128), f32),
                pltpu.VMEM((8, 128), f32),
                pltpu.VMEM((n_dev, 8, 128), f32),
                pltpu.VMEM((n_lay, n_exp, 128), f32),
                pltpu.VMEM((top_k, tok), f32),
                pltpu.VMEM((top_k, tok), f32),
                dma, dma((NB,)), dma((NU,)), dma((NU,)), dma((n_lay,)),
                dma((n_dev,)), dma((n_dev,)), dma((n_dev,)), dma((n_dev,)),
                dma((6, n_lay)), dma((6, n_lay)),
            ],
            compiler_params=pltpu.CompilerParams(
                collective_id=0, has_side_effects=True, vmem_limit_bytes=48 << 20),
            name='router_step',
        )(idx_t, eo, d_out, u_norm, w_t)
        d_norm, d_rt, loss = pl.pallas_call(
            lambda *refs: out_kernel(n_lay, *refs),
            out_shape=(
                jax.ShapeDtypeStruct((n_lay, tok, dim), bf16),
                jax.ShapeDtypeStruct((n_lay, pieces, prow, dim), f32),
                jax.ShapeDtypeStruct((1, 1), f32),
            ),
            in_specs=[vm_spec] * 4,
            out_specs=(any_spec, any_spec, pl.BlockSpec(memory_space=pltpu.SMEM)),
            scratch_shapes=[pltpu.VMEM((NS, tok, dim), bf16), dma((NS,)), dma],
            compiler_params=pltpu.CompilerParams(vmem_limit_bytes=12 << 20),
            name='router_out',
        )(g_all, w_all, fin, loss_v)
        d_router = jnp.swapaxes(d_rt.reshape(n_lay, n_exp, dim), 1, 2)
        return loss[0, 0], d_router, d_norm

    tok_spec = P(None, 'dp', None)
    return jax.shard_map(local_step, mesh=mesh, in_specs=(tok_spec, tok_spec, P(None, 'dp', None, None), tok_spec, P()), out_specs=(P(), P(), tok_spec), check_vma=False)
```

```python
import jax
import jax.numpy as jnp
from jax import lax
from jax.experimental import pallas as pl
from jax.experimental.pallas import tpu as pltpu
from jax.sharding import PartitionSpec as P

AUX_COEF = 0.02
MESH = pl.DeviceIdType.MESH

NB = 8
NC = 4
NU = 3
AGL = 7

NT = (((1,), (1,)), ((), ()))
TN = (((0,), (0,)), ((), ()))


def step_kernel(n_lay, n_dev, tok_all, idx_hbm, eo_hbm, dy_hbm, u_hbm, w_hbm,
                fin, gout, wv, loss_out,
                idx_v, ebuf, ubuf, dbuf, part, rd, r1, r2, cnt_src, cnt_in, loss_src, loss_in,
                fcol, slot_v, loss_acc,
                idx_sem, e_sem, u_sem, d_sem, w_sem, cs_sem, cr_sem, ls_sem, lr_sem, s_sem, r_sem):
    me = lax.axis_index('dp')
    core = me % 2
    xpos = (me // 2) % 2
    ypos = me // 4
    partner = me + 1 - 2 * core
    xn = me + 2 - 4 * xpos
    yn = me + 4 - 8 * ypos
    nbr_a = xn * (1 - core) + yn * core
    nbr_b = yn * (1 - core) + xn * core
    pa = xpos * (1 - core) + ypos * core
    pb = ypos * (1 - core) + xpos * core
    half = 4 * core
    quart = half + 2 * pa
    mine = quart + pb
    n_exp = w_hbm.shape[1]
    top_k = idx_hbm.shape[1]
    tok = u_hbm.shape[1]
    rows = ebuf.shape[1]
    ctok = rows // top_k

    def e_copy(lay, c, slot):
        return pltpu.make_async_copy(eo_hbm.at[lay, pl.ds(c * rows, rows)], ebuf.at[slot], e_sem.at[slot])

    def u_copy(lay):
        return pltpu.make_async_copy(u_hbm.at[lay], ubuf.at[lay % NU], u_sem.at[lay % NU])

    def d_copy(lay):
        return pltpu.make_async_copy(dy_hbm.at[lay], dbuf.at[lay % NU], d_sem.at[lay % NU])

    def w_copy(lay):
        return pltpu.make_async_copy(w_hbm.at[lay], wv.at[lay], w_sem.at[lay])

    idx_copy = pltpu.make_async_copy(idx_hbm, idx_v, idx_sem)
    idx_copy.start()
    for c in range(2):
        if c == 0:
            w_copy(0).start()
            u_copy(0).start()
            d_copy(0).start()
        else:
            w_copy(1).start()
            u_copy(1).start()
            d_copy(1).start()
        for j in range(NC):
            e_copy(c, j, c * NC + j).start()

    barrier = pltpu.get_barrier_semaphore()
    for d in range(1, n_dev):
        pl.semaphore_signal(barrier, inc=1, device_id=((me + d) % n_dev,), device_id_type=MESH)

    idx_copy.wait()
    ones = jnp.ones((8, tok), jnp.bfloat16)
    row_id = lax.broadcasted_iota(jnp.int32, (8, 2 * n_exp), 0)
    e_id = lax.broadcasted_iota(jnp.int32, (n_exp, tok), 0)
    cnt = jnp.zeros((8, 2 * n_exp), jnp.float32)
    for r in range(n_lay // 2):
        hots = []
        for h in range(2):
            ids = idx_v[2 * r + h]
            acc = jnp.zeros((n_exp, tok), jnp.float32)
            for k in range(top_k):
                acc = jnp.where(e_id == ids[k:k + 1], 1.0, acc)
            hots.append(acc.astype(jnp.bfloat16))
        both = jnp.concatenate(hots, axis=0)
        res = lax.dot_general(ones, both, NT, preferred_element_type=jnp.float32)
        cnt = jnp.where(row_id == r, res, cnt)
    cnt_src[...] = cnt
    cnt_in[me] = cnt
    loss_acc[...] = jnp.zeros_like(loss_acc)
    pl.semaphore_wait(barrier, n_dev - 1)

    def cnt_copy(to, frm):
        return pltpu.make_async_remote_copy(
            src_ref=cnt_src, dst_ref=cnt_in.at[frm], send_sem=cs_sem.at[to], recv_sem=cr_sem.at[frm],
            device_id=(to,), device_id_type=MESH)

    def loss_copy(to, frm):
        return pltpu.make_async_remote_copy(
            src_ref=loss_src, dst_ref=loss_in.at[frm], send_sem=ls_sem.at[to], recv_sem=lr_sem.at[frm],
            device_id=(to,), device_id_type=MESH)

    for d in range(1, n_dev):
        cnt_copy((me + d) % n_dev, me).start()

    def rcopy(stage, src, dst, m, dev):
        return pltpu.make_async_remote_copy(
            src_ref=src, dst_ref=dst, send_sem=s_sem.at[stage, m], recv_sem=r_sem.at[stage, m],
            device_id=(dev,), device_id_type=MESH)

    def c_pair(m):
        return rcopy(0, part.at[m, pl.ds(4 - half, 4)], rd.at[m], m, partner)

    def c_rs1(m):
        return rcopy(1, part.at[m, pl.ds(half + 2 - 2 * pa, 2)], r1.at[m], m, nbr_a)

    def c_rs2(m):
        return rcopy(2, part.at[m, pl.ds(quart + 1 - pb, 1)], r2.at[m], m, nbr_b)

    def c_ag1(m, p):
        return rcopy(3, fin.at[m, pl.ds(p, 1)], fin.at[m, pl.ds(p, 1)], m, nbr_b)

    def c_ag2(m, p):
        return rcopy(4, fin.at[m, pl.ds(p, 2)], fin.at[m, pl.ds(p, 2)], m, nbr_a)

    def c_out(m, p):
        return rcopy(5, fin.at[m, pl.ds(p, 4)], fin.at[m, pl.ds(p, 4)], m, partner)

    def do_a(m):
        c_pair(m).wait_recv()
        o = 2 - 2 * pa
        part[m, pl.ds(half + o, 2)] += rd[m, pl.ds(o, 2)]
        part[m, pl.ds(quart, 2)] += rd[m, pl.ds(2 * pa, 2)]
        c_rs1(m).start()

    def do_b(m):
        c_rs1(m).wait_recv()
        o = 1 - pb
        part[m, pl.ds(quart + o, 1)] += r1[m, pl.ds(o, 1)]
        part[m, pl.ds(mine, 1)] += r1[m, pl.ds(pb, 1)]
        c_rs2(m).start()

    def do_c(m):
        c_rs2(m).wait_recv()
        fin[m, pl.ds(mine, 1)] = part[m, pl.ds(mine, 1)] + r2[m]

    def do_ag1(m):
        c_ag1(m, mine).start()

    def do_d(m):
        c_ag1(m, quart + 1 - pb).wait_recv()
        c_ag2(m, quart).start()

    def do_e(m):
        c_ag2(m, half + 2 - 2 * pa).wait_recv()
        c_out(m, half).start()

    def do_f(m):
        c_out(m, 4 - half).wait_recv()

    def slot_chunk(lay, c, slot):
        e_copy(lay, c, slot).wait()
        lanes = 2 * ctok
        lo = (c // 2) * lanes
        dcols = dbuf[lay % NU, lo:lo + lanes, :]
        hr = rows // 2
        s = [lax.dot_general(ebuf[slot, h * hr:(h + 1) * hr, :], dcols, NT, preferred_element_type=jnp.float32) for h in range(2)]
        lane = lax.broadcasted_iota(jnp.int32, (top_k, lanes), 1)
        acc = jnp.zeros((top_k, lanes), jnp.float32)
        for i in range(ctok):
            j = i * top_k
            acc = jnp.where(lane == (c % 2) * ctok + i, s[j // hr][j % hr:j % hr + top_k], acc)
        if c % 2:
            slot_v[:, lo:lo + lanes] += acc
        else:
            slot_v[:, lo:lo + lanes] = acc

        @pl.when(lay + 2 < n_lay)
        def _():
            e_copy(lay + 2, c, slot).start()

    scale = float(tok_all)
    pull = AUX_COEF * n_exp / (top_k * tok_all)

    @pl.loop(0, n_lay)
    def _(lay):
        @pl.when(lay + 2 < n_lay)
        def _():
            w_copy(lay + 2).start()
            u_copy(lay + 2).start()
            d_copy(lay + 2).start()

        base = (lay % 2) * NC
        w_copy(lay).wait()
        u_copy(lay).wait()
        d_copy(lay).wait()
        slot_chunk(lay, 0, base)

        @pl.when(lay >= 1)
        def _():
            do_a(lay - 1)

        slot_chunk(lay, 1, base + 1)

        @pl.when(lay >= 2)
        def _():
            do_b(lay - 2)

        slot_chunk(lay, 2, base + 2)

        @pl.when(lay >= 3)
        def _():
            do_c(lay - 3)

            @pl.when(lay - 3 < AGL)
            def _():
                do_ag1(lay - 3)

        slot_chunk(lay, 3, base + 3)

        @pl.when(jnp.logical_and(lay >= 4, lay - 4 < AGL))
        def _():
            do_d(lay - 4)

        @pl.when(jnp.logical_and(lay >= 5, lay - 5 < AGL))
        def _():
            do_e(lay - 5)

        u = ubuf[lay % NU]
        logits = lax.dot_general(wv[lay], u, NT, preferred_element_type=jnp.float32)
        ex = jnp.exp(logits - jnp.max(logits, axis=0, keepdims=True))
        prob = ex / jnp.sum(ex, axis=0, keepdims=True)
        ids = idx_v[lay]
        chosen = jnp.concatenate(
            [jnp.sum(jnp.where(e_id == ids[k:k + 1], logits, 0.0), axis=0, keepdims=True) for k in range(top_k)], axis=0)
        ge = jnp.exp(chosen - jnp.max(chosen, axis=0, keepdims=True))
        gate = ge / jnp.sum(ge, axis=0, keepdims=True)

        @pl.when(lay == 0)
        def _():
            for d in range(1, n_dev):
                cnt_copy((me + d) % n_dev, (me + d) % n_dev).wait_recv()
            tot = cnt_in[0]
            for j in range(1, n_dev):
                tot = tot + cnt_in[j]
            cols = jnp.transpose(tot * pull)
            for i in range(n_lay):
                o = (i % 2) * n_exp
                fcol[i] = jnp.broadcast_to(cols[o:o + n_exp, i // 2:i // 2 + 1], (n_exp, fcol.shape[2]))

        slots = slot_v[...]
        dd = scale * slots
        dch = gate * (dd - jnp.sum(gate * dd, axis=0, keepdims=True))
        fc = fcol[lay]
        fa = jnp.concatenate([fc] * (tok // fc.shape[1]), axis=1)
        pf = prob * fa
        pf_sum = jnp.sum(pf, axis=0, keepdims=True)
        g = pf - prob * pf_sum
        for k in range(top_k):
            g = g + jnp.where(e_id == ids[k:k + 1], dch[k:k + 1], 0.0)
        main = gate * slots
        first = lax.broadcasted_iota(jnp.int32, (top_k, tok), 0) == 0
        main = main + jnp.where(first, pf_sum * (1.0 / tok_all), 0.0)
        loss_acc[...] += main
        g16 = g.astype(jnp.bfloat16)
        gout[lay] = g16
        pg = jnp.dot(g16, u, preferred_element_type=jnp.float32)
        part[lay] = pg.reshape(part.shape[1:])
        c_pair(lay).start()

    last = n_lay - 1
    la = loss_acc[...]
    lv = la[:, :128]
    for j in range(1, tok // 128):
        lv = lv + la[:, 128 * j:128 * (j + 1)]
    loss_src[...] = lv
    loss_in[me] = lv
    do_a(last)
    do_b(last - 1)
    for d in range(1, n_dev):
        loss_copy((me + d) % n_dev, me).start()
    do_c(last - 2)

    @pl.loop(AGL, last - 1)
    def _(m):
        do_ag1(m)

    do_b(last)
    do_c(last - 1)
    do_ag1(last - 1)

    @pl.loop(AGL, last - 1)
    def _(m):
        do_d(m)

    do_c(last)
    do_ag1(last)
    do_d(last - 1)

    @pl.loop(AGL, last - 1)
    def _(m):
        do_e(m)

    do_d(last)
    do_e(last - 1)
    do_e(last)

    for d in range(1, n_dev):
        loss_copy((me + d) % n_dev, (me + d) % n_dev).wait_recv()
    tot = loss_in[0]
    for j in range(1, n_dev):
        tot = tot + loss_in[j]
    loss_out[...] = tot
    for d in range(1, n_dev):
        cnt_copy((me + d) % n_dev, me).wait_send()
        loss_copy((me + d) % n_dev, me).wait_send()

    @pl.loop(0, n_lay)
    def _(m):
        do_f(m)
        c_pair(m).wait_send()
        c_rs1(m).wait_send()
        c_rs2(m).wait_send()
        c_ag1(m, mine).wait_send()
        c_ag2(m, quart).wait_send()
        c_out(m, half).wait_send()


NS = 4


def out_kernel(n_lay, g_v, w_v, f_v, l_v, dn_hbm, dr_hbm, loss, stage, st_sem, f_sem):
    f_copy = pltpu.make_async_copy(f_v, dr_hbm, f_sem)

    def put(lay):
        return pltpu.make_async_copy(stage.at[lay % NS], dn_hbm.at[lay], st_sem.at[lay % NS])

    f_copy.start()
    loss[0, 0] = jnp.sum(l_v[...])

    @pl.loop(0, n_lay)
    def _(lay):
        @pl.when(lay >= NS)
        def _():
            put(lay - NS).wait()

        dn = lax.dot_general(g_v[lay], w_v[lay], TN, preferred_element_type=jnp.float32)
        stage[lay % NS] = dn.astype(jnp.bfloat16)
        put(lay).start()

    for i in range(NS):
        put(n_lay - NS + i).wait()
    f_copy.wait()


def solution(mesh):
    n_dev = mesh.shape['dp']

    def local_step(u_norm, expert_idx, expert_out, d_out, w_router):
        n_lay, tok, dim = u_norm.shape
        n_exp = w_router.shape[2]
        top_k = expert_idx.shape[2]
        tok_all = tok * n_dev
        f32, bf16 = jnp.float32, jnp.bfloat16
        idx_t = jnp.swapaxes(expert_idx, 1, 2)
        w_t = jnp.swapaxes(w_router, 1, 2)
        eo = expert_out.reshape(n_lay, tok * top_k, dim)
        rows = tok * top_k // NC
        pieces = 8
        prow = n_exp // pieces
        any_spec = pl.BlockSpec(memory_space=pl.ANY)
        vm_spec = pl.BlockSpec(memory_space=pltpu.VMEM)
        dma = pltpu.SemaphoreType.DMA
        fin, g_all, w_all, loss_v = pl.pallas_call(
            lambda *refs: step_kernel(n_lay, n_dev, tok_all, *refs),
            out_shape=(
                pltpu.VMEM((n_lay, pieces, prow, dim), f32),
                pltpu.VMEM((n_lay, n_exp, tok), bf16),
                pltpu.VMEM((n_lay, n_exp, dim), bf16),
                pltpu.VMEM((8, 128), f32),
            ),
            in_specs=[any_spec] * 5,
            out_specs=(vm_spec,) * 4,
            scratch_shapes=[
                pltpu.VMEM((n_lay, top_k, tok), jnp.int32),
                pltpu.VMEM((NB, rows, dim), bf16),
                pltpu.VMEM((NU, tok, dim), bf16),
                pltpu.VMEM((NU, tok, dim), bf16),
                pltpu.VMEM((n_lay, pieces, prow, dim), f32),
                pltpu.VMEM((n_lay, pieces // 2, prow, dim), f32),
                pltpu.VMEM((n_lay, pieces // 4, prow, dim), f32),
                pltpu.VMEM((n_lay, pieces // 8, prow, dim), f32),
                pltpu.VMEM((8, 128), f32),
                pltpu.VMEM((n_dev, 8, 128), f32),
                pltpu.VMEM((8, 128), f32),
                pltpu.VMEM((n_dev, 8, 128), f32),
                pltpu.VMEM((n_lay, n_exp, 128), f32),
                pltpu.VMEM((top_k, tok), f32),
                pltpu.VMEM((top_k, tok), f32),
                dma, dma((NB,)), dma((NU,)), dma((NU,)), dma((n_lay,)),
                dma((n_dev,)), dma((n_dev,)), dma((n_dev,)), dma((n_dev,)),
                dma((6, n_lay)), dma((6, n_lay)),
            ],
            compiler_params=pltpu.CompilerParams(
                collective_id=0, has_side_effects=True, vmem_limit_bytes=48 << 20),
            name='router_step',
        )(idx_t, eo, d_out, u_norm, w_t)
        d_norm, d_rt, loss = pl.pallas_call(
            lambda *refs: out_kernel(n_lay, *refs),
            out_shape=(
                jax.ShapeDtypeStruct((n_lay, tok, dim), bf16),
                jax.ShapeDtypeStruct((n_lay, pieces, prow, dim), f32),
                jax.ShapeDtypeStruct((1, 1), f32),
            ),
            in_specs=[vm_spec] * 4,
            out_specs=(any_spec, any_spec, pl.BlockSpec(memory_space=pltpu.SMEM)),
            scratch_shapes=[pltpu.VMEM((NS, tok, dim), bf16), dma((NS,)), dma],
            compiler_params=pltpu.CompilerParams(vmem_limit_bytes=12 << 20),
            name='router_out',
        )(g_all, w_all, fin, loss_v)
        d_router = jnp.swapaxes(d_rt.reshape(n_lay, n_exp, dim), 1, 2)
        return loss[0, 0], d_router, d_norm

    tok_spec = P(None, 'dp', None)
    return jax.shard_map(local_step, mesh=mesh, in_specs=(tok_spec, tok_spec, P(None, 'dp', None, None), tok_spec, P()), out_specs=(P(), P(), tok_spec), check_vma=False)
```

```python
import jax
import jax.numpy as jnp
from jax import lax
from jax.experimental import pallas as pl
from jax.experimental.pallas import tpu as pltpu
from jax.sharding import PartitionSpec as P

AUX_COEF = 0.02
MESH = pl.DeviceIdType.MESH

NB = 8
NC = 4
NU = 3

NT = (((1,), (1,)), ((), ()))
TN = (((0,), (0,)), ((), ()))


def step_kernel(n_lay, n_dev, tok_all, idx_hbm, eo_hbm, dy_hbm, u_hbm, w_hbm,
                fin, gout, wv, loss_out,
                idx_v, ebuf, ubuf, dbuf, part, rd, r1, r2, cnt_src, cnt_in, loss_src, loss_in,
                fcol, slot_v, lg_v, loss_acc,
                idx_sem, e_sem, u_sem, d_sem, w_sem, cs_sem, cr_sem, ls_sem, lr_sem, s_sem, r_sem):
    me = lax.axis_index('dp')
    core = me % 2
    xpos = (me // 2) % 2
    ypos = me // 4
    partner = me + 1 - 2 * core
    xn = me + 2 - 4 * xpos
    yn = me + 4 - 8 * ypos
    nbr_a = xn * (1 - core) + yn * core
    nbr_b = yn * (1 - core) + xn * core
    pa = xpos * (1 - core) + ypos * core
    pb = ypos * (1 - core) + xpos * core
    half = 4 * core
    quart = half + 2 * pa
    mine = quart + pb
    n_exp = w_hbm.shape[1]
    top_k = idx_hbm.shape[1]
    tok = u_hbm.shape[1]
    rows = ebuf.shape[1]
    ctok = rows // top_k

    def e_copy(lay, c, slot):
        return pltpu.make_async_copy(eo_hbm.at[lay, pl.ds(c * rows, rows)], ebuf.at[slot], e_sem.at[slot])

    def u_copy(lay):
        return pltpu.make_async_copy(u_hbm.at[lay], ubuf.at[lay % NU], u_sem.at[lay % NU])

    def d_copy(lay):
        return pltpu.make_async_copy(dy_hbm.at[lay], dbuf.at[lay % NU], d_sem.at[lay % NU])

    def w_copy(lay):
        return pltpu.make_async_copy(w_hbm.at[lay], wv.at[lay], w_sem.at[lay])

    idx_copy = pltpu.make_async_copy(idx_hbm, idx_v, idx_sem)
    idx_copy.start()
    for c in range(2):
        if c == 0:
            w_copy(0).start()
            u_copy(0).start()
            d_copy(0).start()
        else:
            w_copy(1).start()
            u_copy(1).start()
            d_copy(1).start()
        for j in range(NC):
            e_copy(c, j, c * NC + j).start()

    barrier = pltpu.get_barrier_semaphore()
    for d in range(1, n_dev):
        pl.semaphore_signal(barrier, inc=1, device_id=((me + d) % n_dev,), device_id_type=MESH)

    idx_copy.wait()
    ones = jnp.ones((8, tok), jnp.bfloat16)
    row_id = lax.broadcasted_iota(jnp.int32, (8, 2 * n_exp), 0)
    e_id = lax.broadcasted_iota(jnp.int32, (n_exp, tok), 0)
    cnt = jnp.zeros((8, 2 * n_exp), jnp.float32)
    for r in range(n_lay // 2):
        hots = []
        for h in range(2):
            ids = idx_v[2 * r + h]
            acc = jnp.zeros((n_exp, tok), jnp.float32)
            for k in range(top_k):
                acc = jnp.where(e_id == ids[k:k + 1], 1.0, acc)
            hots.append(acc.astype(jnp.bfloat16))
        both = jnp.concatenate(hots, axis=0)
        res = lax.dot_general(ones, both, NT, preferred_element_type=jnp.float32)
        cnt = jnp.where(row_id == r, res, cnt)
    cnt_src[...] = cnt
    cnt_in[me] = cnt
    loss_acc[...] = jnp.zeros_like(loss_acc)
    pl.semaphore_wait(barrier, n_dev - 1)

    def cnt_copy(to, frm):
        return pltpu.make_async_remote_copy(
            src_ref=cnt_src, dst_ref=cnt_in.at[frm], send_sem=cs_sem.at[to], recv_sem=cr_sem.at[frm],
            device_id=(to,), device_id_type=MESH)

    def loss_copy(to, frm):
        return pltpu.make_async_remote_copy(
            src_ref=loss_src, dst_ref=loss_in.at[frm], send_sem=ls_sem.at[to], recv_sem=lr_sem.at[frm],
            device_id=(to,), device_id_type=MESH)

    for d in range(1, n_dev):
        cnt_copy((me + d) % n_dev, me).start()

    def rcopy(stage, src, dst, m, dev):
        return pltpu.make_async_remote_copy(
            src_ref=src, dst_ref=dst, send_sem=s_sem.at[stage, m], recv_sem=r_sem.at[stage, m],
            device_id=(dev,), device_id_type=MESH)

    def c_pair(m):
        return rcopy(0, part.at[m, pl.ds(4 - half, 4)], rd.at[m], m, partner)

    def c_rs1(m):
        return rcopy(1, part.at[m, pl.ds(half + 2 - 2 * pa, 2)], r1.at[m], m, nbr_a)

    def c_rs2(m):
        return rcopy(2, part.at[m, pl.ds(quart + 1 - pb, 1)], r2.at[m], m, nbr_b)

    def c_ag1(m, p):
        return rcopy(3, fin.at[m, pl.ds(p, 1)], fin.at[m, pl.ds(p, 1)], m, nbr_b)

    def c_ag2(m, p):
        return rcopy(4, fin.at[m, pl.ds(p, 2)], fin.at[m, pl.ds(p, 2)], m, nbr_a)

    def c_out(m, p):
        return rcopy(5, fin.at[m, pl.ds(p, 4)], fin.at[m, pl.ds(p, 4)], m, partner)

    def do_a(m):
        c_pair(m).wait_recv()
        o = 2 - 2 * pa
        part[m, pl.ds(half + o, 2)] += rd[m, pl.ds(o, 2)]
        part[m, pl.ds(quart, 2)] += rd[m, pl.ds(2 * pa, 2)]
        c_rs1(m).start()

    def do_b(m):
        c_rs1(m).wait_recv()
        o = 1 - pb
        part[m, pl.ds(quart + o, 1)] += r1[m, pl.ds(o, 1)]
        part[m, pl.ds(mine, 1)] += r1[m, pl.ds(pb, 1)]
        c_rs2(m).start()

    def do_c(m):
        c_rs2(m).wait_recv()
        fin[m, pl.ds(mine, 1)] = part[m, pl.ds(mine, 1)] + r2[m]

    def do_ag1(m):
        c_ag1(m, mine).start()

    def do_d(m):
        c_ag1(m, quart + 1 - pb).wait_recv()
        c_ag2(m, quart).start()

    def do_e(m):
        c_ag2(m, half + 2 - 2 * pa).wait_recv()
        c_out(m, half).start()

    def do_f(m):
        c_out(m, 4 - half).wait_recv()

    hr = rows // 2
    lanes = 2 * ctok
    lane = lax.broadcasted_iota(jnp.int32, (top_k, lanes), 1)
    e_half = lax.broadcasted_iota(jnp.int32, (n_exp, lanes), 0)
    first = lax.broadcasted_iota(jnp.int32, (top_k, lanes), 0) == 0
    scale = float(tok_all)
    pull = AUX_COEF * n_exp / (top_k * tok_all)

    def slot_chunk(lay, c, slot):
        lo = (c // 2) * lanes
        dcols = dbuf[lay % NU, lo:lo + lanes, :]
        s = [lax.dot_general(ebuf[slot, h * hr:(h + 1) * hr, :], dcols, NT, preferred_element_type=jnp.float32) for h in range(2)]
        acc = jnp.zeros((top_k, lanes), jnp.float32)
        for i in range(ctok):
            j = i * top_k
            acc = jnp.where(lane == (c % 2) * ctok + i, s[j // hr][j % hr:j % hr + top_k], acc)
        if c % 2:
            slot_v[lay % 2, :, lo:lo + lanes] += acc
        else:
            slot_v[lay % 2, :, lo:lo + lanes] = acc

    def logit_part(lay):
        for h in range(2):
            lo = h * lanes
            lg_v[:, lo:lo + lanes] = lax.dot_general(
                wv[lay], ubuf[lay % NU, lo:lo + lanes, :], NT, preferred_element_type=jnp.float32)

    def g_part(lay, h, keep):
        lo = h * lanes
        logits = lg_v[:, lo:lo + lanes]
        ids = idx_v[lay, :, lo:lo + lanes]
        ex = jnp.exp(logits - jnp.max(logits, axis=0, keepdims=True))
        prob = ex / jnp.sum(ex, axis=0, keepdims=True)
        chosen = jnp.concatenate(
            [jnp.sum(jnp.where(e_half == ids[k:k + 1], logits, 0.0), axis=0, keepdims=True) for k in range(top_k)], axis=0)
        ge = jnp.exp(chosen - jnp.max(chosen, axis=0, keepdims=True))
        gate = ge / jnp.sum(ge, axis=0, keepdims=True)
        slots = slot_v[lay % 2, :, lo:lo + lanes]
        dd = scale * slots
        dch = gate * (dd - jnp.sum(gate * dd, axis=0, keepdims=True))
        pf = prob * fcol[lay]
        pf_sum = jnp.sum(pf, axis=0, keepdims=True)
        g = pf - prob * pf_sum
        for k in range(top_k):
            g = g + jnp.where(e_half == ids[k:k + 1], dch[k:k + 1], 0.0)
        main = gate * slots + jnp.where(first, pf_sum * (1.0 / tok_all), 0.0)
        total = loss_acc[:, lo:lo + lanes] + main
        loss_acc[:, lo:lo + lanes] = total if keep is None else jnp.where(keep, total, 0.0)
        gout[lay, :, lo:lo + lanes] = g.astype(jnp.bfloat16)

    def p_part(lay):
        dim = ubuf.shape[2]
        for h in range(2):
            lo = h * (dim // 2)
            pg = jnp.dot(gout[lay], ubuf[lay % NU, :, lo:lo + dim // 2], preferred_element_type=jnp.float32)
            part[lay, :, :, lo:lo + dim // 2] = pg.reshape(part.shape[1:3] + (dim // 2,))

    slot_v[...] = jnp.zeros_like(slot_v)
    lg_v[...] = jnp.zeros_like(lg_v)
    fcol[0] = jnp.zeros(fcol.shape[1:], jnp.float32)

    @pl.loop(0, n_lay)
    def _(lay):
        base = (lay % 2) * NC
        prev = jnp.maximum(lay - 1, 0)
        keep = lay >= 1

        def refill(c):
            @pl.when(lay + 2 < n_lay)
            def _():
                e_copy(lay + 2, c, base + c).start()

        @pl.when(lay >= 2)
        def _():
            do_a(lay - 2)

        w_copy(lay).wait()
        u_copy(lay).wait()
        d_copy(lay).wait()
        e_copy(lay, 0, base).wait()
        slot_chunk(lay, 0, base)
        g_part(prev, 0, keep)
        refill(0)

        @pl.when(lay >= 3)
        def _():
            do_b(lay - 3)

        e_copy(lay, 1, base + 1).wait()
        slot_chunk(lay, 1, base + 1)
        g_part(prev, 1, keep)
        refill(1)

        @pl.when(lay >= 4)
        def _():
            do_c(lay - 4)
            do_ag1(lay - 4)

        e_copy(lay, 2, base + 2).wait()
        slot_chunk(lay, 2, base + 2)
        p_part(prev)
        refill(2)

        @pl.when(lay + 2 < n_lay)
        def _():
            w_copy(lay + 2).start()
            u_copy(lay + 2).start()
            d_copy(lay + 2).start()

        @pl.when(lay >= 1)
        def _():
            c_pair(lay - 1).start()

        @pl.when(lay >= 5)
        def _():
            do_d(lay - 5)

        e_copy(lay, 3, base + 3).wait()
        slot_chunk(lay, 3, base + 3)
        logit_part(lay)
        refill(3)

        @pl.when(lay >= 6)
        def _():
            do_e(lay - 6)

        @pl.when(lay == 0)
        def _():
            for d in range(1, n_dev):
                cnt_copy((me + d) % n_dev, (me + d) % n_dev).wait_recv()
            tot = cnt_in[0]
            for j in range(1, n_dev):
                tot = tot + cnt_in[j]
            cols = jnp.transpose(tot * pull)
            for i in range(n_lay):
                o = (i % 2) * n_exp
                fcol[i] = jnp.broadcast_to(cols[o:o + n_exp, i // 2:i // 2 + 1], (n_exp, fcol.shape[2]))

    last = n_lay - 1
    for h in range(2):
        g_part(last, h, None)
    p_part(last)
    la = loss_acc[...]
    lv = la[:, :128]
    for j in range(1, tok // 128):
        lv = lv + la[:, 128 * j:128 * (j + 1)]
    loss_src[...] = lv
    loss_in[me] = lv
    c_pair(last).start()

    def do_cg(m):
        do_c(m)
        do_ag1(m)

    steps = (do_a, do_b, do_cg, do_d, do_e)
    for r in range(6):
        for j in range(5):
            m = last - 1 + r - j
            if m <= last and j >= r - 1:
                steps[j](m)
        if r == 0:
            for d in range(1, n_dev):
                loss_copy((me + d) % n_dev, me).start()

    for d in range(1, n_dev):
        loss_copy((me + d) % n_dev, (me + d) % n_dev).wait_recv()
    tot = loss_in[0]
    for j in range(1, n_dev):
        tot = tot + loss_in[j]
    loss_out[...] = tot
    for d in range(1, n_dev):
        cnt_copy((me + d) % n_dev, me).wait_send()
        loss_copy((me + d) % n_dev, me).wait_send()

    @pl.loop(0, n_lay)
    def _(m):
        do_f(m)
        c_pair(m).wait_send()
        c_rs1(m).wait_send()
        c_rs2(m).wait_send()
        c_ag1(m, mine).wait_send()
        c_ag2(m, quart).wait_send()
        c_out(m, half).wait_send()


def out_kernel(n_lay, g_v, w_v, f_v, l_v, dn_hbm, dr_hbm, loss, stage, st_sem, f_sem):
    def put(lay):
        return pltpu.make_async_copy(stage.at[lay], dn_hbm.at[lay], st_sem.at[lay])

    def put_f(lay):
        return pltpu.make_async_copy(f_v.at[lay], dr_hbm.at[lay], f_sem.at[lay])

    @pl.loop(0, n_lay)
    def _(lay):
        put_f(lay).start()
        dn = lax.dot_general(g_v[lay], w_v[lay], TN, preferred_element_type=jnp.float32)
        stage[lay] = dn.astype(jnp.bfloat16)
        put(lay).start()

    loss[0, 0] = jnp.sum(l_v[...])

    @pl.loop(0, n_lay)
    def _(lay):
        put(lay).wait()
        put_f(lay).wait()


def solution(mesh):
    n_dev = mesh.shape['dp']

    def local_step(u_norm, expert_idx, expert_out, d_out, w_router):
        n_lay, tok, dim = u_norm.shape
        n_exp = w_router.shape[2]
        top_k = expert_idx.shape[2]
        tok_all = tok * n_dev
        f32, bf16 = jnp.float32, jnp.bfloat16
        idx_t = jnp.swapaxes(expert_idx, 1, 2)
        w_t = jnp.swapaxes(w_router, 1, 2)
        eo = expert_out.reshape(n_lay, tok * top_k, dim)
        rows = tok * top_k // NC
        pieces = 8
        prow = n_exp // pieces
        any_spec = pl.BlockSpec(memory_space=pl.ANY)
        vm_spec = pl.BlockSpec(memory_space=pltpu.VMEM)
        dma = pltpu.SemaphoreType.DMA
        fin, g_all, w_all, loss_v = pl.pallas_call(
            lambda *refs: step_kernel(n_lay, n_dev, tok_all, *refs),
            out_shape=(
                pltpu.VMEM((n_lay, pieces, prow, dim), f32),
                pltpu.VMEM((n_lay, n_exp, tok), bf16),
                pltpu.VMEM((n_lay, n_exp, dim), bf16),
                pltpu.VMEM((8, 128), f32),
            ),
            in_specs=[any_spec] * 5,
            out_specs=(vm_spec,) * 4,
            scratch_shapes=[
                pltpu.VMEM((n_lay, top_k, tok), jnp.int32),
                pltpu.VMEM((NB, rows, dim), bf16),
                pltpu.VMEM((NU, tok, dim), bf16),
                pltpu.VMEM((NU, tok, dim), bf16),
                pltpu.VMEM((n_lay, pieces, prow, dim), f32),
                pltpu.VMEM((n_lay, pieces // 2, prow, dim), f32),
                pltpu.VMEM((n_lay, pieces // 4, prow, dim), f32),
                pltpu.VMEM((n_lay, pieces // 8, prow, dim), f32),
                pltpu.VMEM((8, 128), f32),
                pltpu.VMEM((n_dev, 8, 128), f32),
                pltpu.VMEM((8, 128), f32),
                pltpu.VMEM((n_dev, 8, 128), f32),
                pltpu.VMEM((n_lay, n_exp, 128), f32),
                pltpu.VMEM((2, top_k, tok), f32),
                pltpu.VMEM((n_exp, tok), f32),
                pltpu.VMEM((top_k, tok), f32),
                dma, dma((NB,)), dma((NU,)), dma((NU,)), dma((n_lay,)),
                dma((n_dev,)), dma((n_dev,)), dma((n_dev,)), dma((n_dev,)),
                dma((6, n_lay)), dma((6, n_lay)),
            ],
            compiler_params=pltpu.CompilerParams(
                collective_id=0, has_side_effects=True, vmem_limit_bytes=48 << 20),
            name='router_step',
        )(idx_t, eo, d_out, u_norm, w_t)
        d_norm, d_rt, loss = pl.pallas_call(
            lambda *refs: out_kernel(n_lay, *refs),
            out_shape=(
                jax.ShapeDtypeStruct((n_lay, tok, dim), bf16),
                jax.ShapeDtypeStruct((n_lay, pieces, prow, dim), f32),
                jax.ShapeDtypeStruct((1, 1), f32),
            ),
            in_specs=[vm_spec] * 4,
            out_specs=(any_spec, any_spec, pl.BlockSpec(memory_space=pltpu.SMEM)),
            scratch_shapes=[pltpu.VMEM((n_lay, tok, dim), bf16), dma((n_lay,)), dma((n_lay,))],
            compiler_params=pltpu.CompilerParams(vmem_limit_bytes=20 << 20),
            name='router_out',
        )(g_all, w_all, fin, loss_v)
        d_router = jnp.swapaxes(d_rt.reshape(n_lay, n_exp, dim), 1, 2)
        return loss[0, 0], d_router, d_norm

    tok_spec = P(None, 'dp', None)
    return jax.shard_map(local_step, mesh=mesh, in_specs=(tok_spec, tok_spec, P(None, 'dp', None, None), tok_spec, P()), out_specs=(P(), P(), tok_spec), check_vma=False)
```

```python
import jax
import jax.numpy as jnp
from jax import lax
from jax.experimental import pallas as pl
from jax.experimental.pallas import tpu as pltpu
from jax.sharding import PartitionSpec as P

AUX_COEF = 0.02
MESH = pl.DeviceIdType.MESH

NB = 8
NC = 4
NU = 3
AGL = 10
LAG = {'a': (2, 1), 'b': (3, 3), 'c': (4, 3), 'g': (4, 3), 'd': (6, 0), 'e': (7, 3)}
FIRST = {'a': (1, 2), 'b': (2, 3), 'c': (3, 3), 'g': (3, 3), 'd': (4, 3), 'e': (6, 1)}
DRAIN = (('a', 1), ('g', 5), ('e', 6), ('g', 4), ('a', 0), ('b', 2), ('c', 3), ('g', 3), ('d', 5), ('b', 1), ('d', 4),
         ('c', 2), ('g', 2), ('b', 0), ('d', 3), ('c', 1), ('g', 1), ('e', 5), ('d', 2), ('c', 0), ('g', 0), ('e', 4),
         ('d', 1), ('e', 3), ('d', 0), ('e', 2), ('e', 1), ('e', 0))

NT = (((1,), (1,)), ((), ()))
TN = (((0,), (0,)), ((), ()))


def step_kernel(n_lay, n_dev, tok_all, idx_hbm, eo_hbm, dy_hbm, u_hbm, w_hbm,
                fin, gout, wv, loss_out,
                idx_v, ebuf, ubuf, dbuf, part, rd, r1, r2, cnt_src, cnt_in, loss_src, loss_in,
                fcol, slot_v, lg_v, loss_acc,
                idx_sem, e_sem, u_sem, d_sem, w_sem, cs_sem, cr_sem, ls_sem, lr_sem, s_sem, r_sem):
    me = lax.axis_index('dp')
    core = me % 2
    xpos = (me // 2) % 2
    ypos = me // 4
    partner = me + 1 - 2 * core
    xn = me + 2 - 4 * xpos
    yn = me + 4 - 8 * ypos
    nbr_a = xn * (1 - core) + yn * core
    nbr_b = yn * (1 - core) + xn * core
    pa = xpos * (1 - core) + ypos * core
    pb = ypos * (1 - core) + xpos * core
    half = 4 * core
    quart = half + 2 * pa
    mine = quart + pb
    n_exp = w_hbm.shape[1]
    top_k = idx_hbm.shape[1]
    tok = u_hbm.shape[1]
    rows = ebuf.shape[1]
    ctok = rows // top_k

    def e_copy(lay, c, slot):
        return pltpu.make_async_copy(eo_hbm.at[lay, pl.ds(c * rows, rows)], ebuf.at[slot], e_sem.at[slot])

    def u_copy(lay):
        return pltpu.make_async_copy(u_hbm.at[lay], ubuf.at[lay % NU], u_sem.at[lay % NU])

    def d_copy(lay):
        return pltpu.make_async_copy(dy_hbm.at[lay], dbuf.at[lay % NU], d_sem.at[lay % NU])

    def w_copy(lay):
        return pltpu.make_async_copy(w_hbm.at[lay], wv.at[lay], w_sem.at[lay])

    idx_copy = pltpu.make_async_copy(idx_hbm, idx_v, idx_sem)
    idx_copy.start()
    for c in range(2):
        if c == 0:
            w_copy(0).start()
            u_copy(0).start()
            d_copy(0).start()
        else:
            w_copy(1).start()
            u_copy(1).start()
            d_copy(1).start()
        for j in range(NC):
            e_copy(c, j, c * NC + j).start()

    barrier = pltpu.get_barrier_semaphore()
    for d in range(1, n_dev):
        pl.semaphore_signal(barrier, inc=1, device_id=((me + d) % n_dev,), device_id_type=MESH)

    ones = jnp.ones((8, tok), jnp.bfloat16)
    row_id = lax.broadcasted_iota(jnp.int32, (8, 2 * n_exp), 0)
    e_id = lax.broadcasted_iota(jnp.int32, (n_exp, tok), 0)

    def count_rows(part_no, r0, r1):
        cnt = jnp.zeros((8, 2 * n_exp), jnp.float32)
        for r in range(r0, r1):
            hots = []
            for h in range(2):
                ids = idx_v[2 * r + h]
                acc = jnp.zeros((n_exp, tok), jnp.float32)
                for k in range(top_k):
                    acc = jnp.where(e_id == ids[k:k + 1], 1.0, acc)
                hots.append(acc.astype(jnp.bfloat16))
            both = jnp.concatenate(hots, axis=0)
            res = lax.dot_general(ones, both, NT, preferred_element_type=jnp.float32)
            cnt = jnp.where(row_id == r, res, cnt)
        cnt_src[part_no] = cnt
        cnt_in[part_no, me] = cnt

    def cnt_copy(p, to, frm):
        return pltpu.make_async_remote_copy(
            src_ref=cnt_src.at[p], dst_ref=cnt_in.at[p, frm], send_sem=cs_sem.at[p, to], recv_sem=cr_sem.at[p, frm],
            device_id=(to,), device_id_type=MESH)

    def send_counts(p):
        for d in range(1, n_dev):
            cnt_copy(p, (me + d) % n_dev, me).start()

    def take_counts(p, lo, hi):
        for d in range(1, n_dev):
            cnt_copy(p, (me + d) % n_dev, (me + d) % n_dev).wait_recv()
        tot = cnt_in[p, 0]
        for j in range(1, n_dev):
            tot = tot + cnt_in[p, j]
        cols = jnp.transpose(tot * pull)
        for i in range(lo, hi):
            o = (i % 2) * n_exp
            fcol[i] = jnp.broadcast_to(cols[o:o + n_exp, i // 2:i // 2 + 1], (n_exp, fcol.shape[2]))

    idx_copy.wait()
    count_rows(0, 0, 1)
    loss_acc[...] = jnp.zeros_like(loss_acc)
    pl.semaphore_wait(barrier, n_dev - 1)
    send_counts(0)

    def loss_copy(to, frm):
        return pltpu.make_async_remote_copy(
            src_ref=loss_src, dst_ref=loss_in.at[frm], send_sem=ls_sem.at[to], recv_sem=lr_sem.at[frm],
            device_id=(to,), device_id_type=MESH)

    def rcopy(stage, src, dst, m, dev):
        return pltpu.make_async_remote_copy(
            src_ref=src, dst_ref=dst, send_sem=s_sem.at[stage, m], recv_sem=r_sem.at[stage, m],
            device_id=(dev,), device_id_type=MESH)

    def c_pair(m):
        return rcopy(0, part.at[m, pl.ds(4 - half, 4)], rd.at[m], m, partner)

    def c_rs1(m):
        return rcopy(1, part.at[m, pl.ds(half + 2 - 2 * pa, 2)], r1.at[m], m, nbr_a)

    def c_rs2(m):
        return rcopy(2, part.at[m, pl.ds(quart + 1 - pb, 1)], r2.at[m], m, nbr_b)

    def c_ag1(m, p):
        return rcopy(3, fin.at[m, pl.ds(p, 1)], fin.at[m, pl.ds(p, 1)], m, nbr_b)

    def c_ag2(m, p):
        return rcopy(4, fin.at[m, pl.ds(p, 2)], fin.at[m, pl.ds(p, 2)], m, nbr_a)

    def c_out(m, p):
        return rcopy(5, fin.at[m, pl.ds(p, 4)], fin.at[m, pl.ds(p, 4)], m, partner)

    def do_a(m):
        c_pair(m).wait_recv()
        o = 2 - 2 * pa
        part[m, pl.ds(half + o, 2)] += rd[m, pl.ds(o, 2)]
        part[m, pl.ds(quart, 2)] += rd[m, pl.ds(2 * pa, 2)]
        c_rs1(m).start()

    def do_b(m):
        c_rs1(m).wait_recv()
        o = 1 - pb
        part[m, pl.ds(quart + o, 1)] += r1[m, pl.ds(o, 1)]
        part[m, pl.ds(mine, 1)] += r1[m, pl.ds(pb, 1)]
        c_rs2(m).start()

    def do_c(m):
        c_rs2(m).wait_recv()
        fin[m, pl.ds(mine, 1)] = part[m, pl.ds(mine, 1)] + r2[m]

    def do_ag1(m):
        c_ag1(m, mine).start()

    def do_d(m):
        c_ag1(m, quart + 1 - pb).wait_recv()
        c_ag2(m, quart).start()

    def do_e(m):
        c_ag2(m, half + 2 - 2 * pa).wait_recv()
        c_out(m, half).start()

    def do_f(m):
        c_out(m, 4 - half).wait_recv()

    hr = rows // 2
    lanes = 2 * ctok
    lane = lax.broadcasted_iota(jnp.int32, (top_k, lanes), 1)
    e_half = lax.broadcasted_iota(jnp.int32, (n_exp, lanes), 0)
    first = lax.broadcasted_iota(jnp.int32, (top_k, lanes), 0) == 0
    scale = float(tok_all)
    pull = AUX_COEF * n_exp / (top_k * tok_all)

    def slot_chunk(lay, c, slot):
        lo = (c // 2) * lanes
        dcols = dbuf[lay % NU, lo:lo + lanes, :]
        s = [lax.dot_general(ebuf[slot, h * hr:(h + 1) * hr, :], dcols, NT, preferred_element_type=jnp.float32) for h in range(2)]
        acc = jnp.zeros((top_k, lanes), jnp.float32)
        for i in range(ctok):
            j = i * top_k
            acc = jnp.where(lane == (c % 2) * ctok + i, s[j // hr][j % hr:j % hr + top_k], acc)
        if c % 2:
            slot_v[lay % 2, :, lo:lo + lanes] += acc
        else:
            slot_v[lay % 2, :, lo:lo + lanes] = acc

    def logit_part(lay):
        for h in range(2):
            lo = h * lanes
            lg_v[:, lo:lo + lanes] = lax.dot_general(
                wv[lay], ubuf[lay % NU, lo:lo + lanes, :], NT, preferred_element_type=jnp.float32)

    def g_part(lay, to, h, keep):
        lo = h * lanes
        logits = lg_v[:, lo:lo + lanes]
        ids = idx_v[lay, :, lo:lo + lanes]
        ex = jnp.exp(logits - jnp.max(logits, axis=0, keepdims=True))
        prob = ex / jnp.sum(ex, axis=0, keepdims=True)
        chosen = jnp.concatenate(
            [jnp.sum(jnp.where(e_half == ids[k:k + 1], logits, 0.0), axis=0, keepdims=True) for k in range(top_k)], axis=0)
        ge = jnp.exp(chosen - jnp.max(chosen, axis=0, keepdims=True))
        gate = ge / jnp.sum(ge, axis=0, keepdims=True)
        slots = slot_v[lay % 2, :, lo:lo + lanes]
        dd = scale * slots
        dch = gate * (dd - jnp.sum(gate * dd, axis=0, keepdims=True))
        pf = prob * fcol[lay]
        pf_sum = jnp.sum(pf, axis=0, keepdims=True)
        g = pf - prob * pf_sum
        for k in range(top_k):
            g = g + jnp.where(e_half == ids[k:k + 1], dch[k:k + 1], 0.0)
        main = gate * slots + jnp.where(first, pf_sum * (1.0 / tok_all), 0.0)
        total = loss_acc[:, lo:lo + lanes] + main
        loss_acc[:, lo:lo + lanes] = total if keep is None else jnp.where(keep, total, loss_acc[:, lo:lo + lanes])
        gout[to, :, lo:lo + lanes] = g.astype(jnp.bfloat16)

    def p_part(lay, to):
        dim = ubuf.shape[2]
        for h in range(2):
            lo = h * (dim // 2)
            pg = jnp.dot(gout[to], ubuf[lay % NU, :, lo:lo + dim // 2], preferred_element_type=jnp.float32)
            part[to, :, :, lo:lo + dim // 2] = pg.reshape(part.shape[1:3] + (dim // 2,))

    def refill(lay, c):
        @pl.when(lay + 2 < n_lay)
        def _():
            e_copy(lay + 2, c, (lay % 2) * NC + c).start()

    def fetch(lay):
        @pl.when(lay + 2 < n_lay)
        def _():
            w_copy(lay + 2).start()
            u_copy(lay + 2).start()
            d_copy(lay + 2).start()

    run = {'a': do_a, 'b': do_b, 'c': do_c, 'g': do_ag1, 'd': do_d, 'e': do_e}

    w_copy(0).wait()
    u_copy(0).wait()
    d_copy(0).wait()
    for c in range(NC):
        e_copy(0, c, c).wait()
        slot_chunk(0, c, c)
        if c == 0:
            logit_part(0)
        e_copy(2, c, c).start()
    w_copy(2).start()
    u_copy(2).start()
    d_copy(2).start()
    take_counts(0, 0, 2)
    for h in range(2):
        g_part(0, 0, h, None)
    p_part(0, 0)
    c_pair(0).start()
    count_rows(1, 1, n_lay // 2)
    send_counts(1)

    @pl.loop(1, n_lay)
    def _(lay):
        base = (lay % 2) * NC
        prev = lay - 1
        to = jnp.where(lay == 1, lay, prev)
        keep = lay >= 2

        def comm(c):
            for k in 'abcgde':
                if FIRST[k][1] == c:
                    @pl.when(lay == FIRST[k][0])
                    def _(k=k):
                        run[k](0)
                if LAG[k][1] == c:
                    lag = LAG[k][0]
                    hi = min(n_lay, lag + AGL) if k in 'gde' else n_lay

                    @pl.when(jnp.logical_and(lay > lag, lay < hi))
                    def _(k=k, lag=lag):
                        run[k](lay - lag)

        comm(0)
        w_copy(lay).wait()
        u_copy(lay).wait()
        d_copy(lay).wait()
        e_copy(lay, 0, base).wait()
        slot_chunk(lay, 0, base)
        g_part(prev, to, 0, keep)
        refill(lay, 0)

        comm(1)
        e_copy(lay, 1, base + 1).wait()
        slot_chunk(lay, 1, base + 1)
        g_part(prev, to, 1, keep)
        refill(lay, 1)

        comm(2)
        e_copy(lay, 2, base + 2).wait()
        slot_chunk(lay, 2, base + 2)
        p_part(prev, to)
        refill(lay, 2)
        fetch(lay)

        @pl.when(lay >= 2)
        def _():
            c_pair(lay - 1).start()

        comm(3)
        e_copy(lay, 3, base + 3).wait()
        slot_chunk(lay, 3, base + 3)
        logit_part(lay)
        refill(lay, 3)

        @pl.when(lay == 2)
        def _():
            take_counts(1, 2, n_lay)

    last = n_lay - 1
    for h in range(2):
        g_part(last, last, h, None)
    p_part(last, last)
    la = loss_acc[...]
    lv = la[:, :128]
    for j in range(1, tok // 128):
        lv = lv + la[:, 128 * j:128 * (j + 1)]
    loss_src[...] = lv
    loss_in[me] = lv
    c_pair(last).start()

    for d in range(1, n_dev):
        loss_copy((me + d) % n_dev, me).start()
    for k, back in DRAIN:
        run[k](last - back)

    for d in range(1, n_dev):
        loss_copy((me + d) % n_dev, (me + d) % n_dev).wait_recv()
    tot = loss_in[0]
    for j in range(1, n_dev):
        tot = tot + loss_in[j]
    loss_out[...] = tot
    for d in range(1, n_dev):
        cnt_copy(0, (me + d) % n_dev, me).wait_send()
        cnt_copy(1, (me + d) % n_dev, me).wait_send()
        loss_copy((me + d) % n_dev, me).wait_send()

    @pl.loop(0, n_lay)
    def _(m):
        do_f(m)
        c_pair(m).wait_send()
        c_rs1(m).wait_send()
        c_rs2(m).wait_send()
        c_ag1(m, mine).wait_send()
        c_ag2(m, quart).wait_send()
        c_out(m, half).wait_send()


def out_kernel(n_lay, g_v, w_v, f_v, l_v, dn_hbm, dr_hbm, loss, stage, st_sem, f_sem):
    def put(lay):
        return pltpu.make_async_copy(stage.at[lay], dn_hbm.at[lay], st_sem.at[lay])

    def put_f(lay):
        return pltpu.make_async_copy(f_v.at[lay], dr_hbm.at[lay], f_sem.at[lay])

    @pl.loop(0, n_lay)
    def _(lay):
        put_f(lay).start()

    @pl.loop(0, n_lay)
    def _(lay):
        dn = lax.dot_general(g_v[lay], w_v[lay], TN, preferred_element_type=jnp.float32)
        stage[lay] = dn.astype(jnp.bfloat16)
        put(lay).start()

    loss[0, 0] = jnp.sum(l_v[...])

    @pl.loop(0, n_lay)
    def _(lay):
        put(lay).wait()
        put_f(lay).wait()


def solution(mesh):
    n_dev = mesh.shape['dp']

    def local_step(u_norm, expert_idx, expert_out, d_out, w_router):
        n_lay, tok, dim = u_norm.shape
        n_exp = w_router.shape[2]
        top_k = expert_idx.shape[2]
        tok_all = tok * n_dev
        f32, bf16 = jnp.float32, jnp.bfloat16
        idx_t = jnp.swapaxes(expert_idx, 1, 2)
        w_t = jnp.swapaxes(w_router, 1, 2)
        eo = expert_out.reshape(n_lay, tok * top_k, dim)
        rows = tok * top_k // NC
        pieces = 8
        prow = n_exp // pieces
        any_spec = pl.BlockSpec(memory_space=pl.ANY)
        vm_spec = pl.BlockSpec(memory_space=pltpu.VMEM)
        dma = pltpu.SemaphoreType.DMA
        fin, g_all, w_all, loss_v = pl.pallas_call(
            lambda *refs: step_kernel(n_lay, n_dev, tok_all, *refs),
            out_shape=(
                pltpu.VMEM((n_lay, pieces, prow, dim), f32),
                pltpu.VMEM((n_lay, n_exp, tok), bf16),
                pltpu.VMEM((n_lay, n_exp, dim), bf16),
                pltpu.VMEM((8, 128), f32),
            ),
            in_specs=[any_spec] * 5,
            out_specs=(vm_spec,) * 4,
            scratch_shapes=[
                pltpu.VMEM((n_lay, top_k, tok), jnp.int32),
                pltpu.VMEM((NB, rows, dim), bf16),
                pltpu.VMEM((NU, tok, dim), bf16),
                pltpu.VMEM((NU, tok, dim), bf16),
                pltpu.VMEM((n_lay, pieces, prow, dim), f32),
                pltpu.VMEM((n_lay, pieces // 2, prow, dim), f32),
                pltpu.VMEM((n_lay, pieces // 4, prow, dim), f32),
                pltpu.VMEM((n_lay, pieces // 8, prow, dim), f32),
                pltpu.VMEM((2, 8, 128), f32),
                pltpu.VMEM((2, n_dev, 8, 128), f32),
                pltpu.VMEM((8, 128), f32),
                pltpu.VMEM((n_dev, 8, 128), f32),
                pltpu.VMEM((n_lay, n_exp, 128), f32),
                pltpu.VMEM((2, top_k, tok), f32),
                pltpu.VMEM((n_exp, tok), f32),
                pltpu.VMEM((top_k, tok), f32),
                dma, dma((NB,)), dma((NU,)), dma((NU,)), dma((n_lay,)),
                dma((2, n_dev)), dma((2, n_dev)), dma((n_dev,)), dma((n_dev,)),
                dma((6, n_lay)), dma((6, n_lay)),
            ],
            compiler_params=pltpu.CompilerParams(
                collective_id=0, has_side_effects=True, vmem_limit_bytes=48 << 20),
            name='router_step',
        )(idx_t, eo, d_out, u_norm, w_t)
        d_norm, d_rt, loss = pl.pallas_call(
            lambda *refs: out_kernel(n_lay, *refs),
            out_shape=(
                jax.ShapeDtypeStruct((n_lay, tok, dim), bf16),
                jax.ShapeDtypeStruct((n_lay, pieces, prow, dim), f32),
                jax.ShapeDtypeStruct((1, 1), f32),
            ),
            in_specs=[vm_spec] * 4,
            out_specs=(any_spec, any_spec, pl.BlockSpec(memory_space=pltpu.SMEM)),
            scratch_shapes=[pltpu.VMEM((n_lay, tok, dim), bf16), dma((n_lay,)), dma((n_lay,))],
            compiler_params=pltpu.CompilerParams(vmem_limit_bytes=20 << 20),
            name='router_out',
        )(g_all, w_all, fin, loss_v)
        d_router = jnp.swapaxes(d_rt.reshape(n_lay, n_exp, dim), 1, 2)
        return loss[0, 0], d_router, d_norm

    tok_spec = P(None, 'dp', None)
    return jax.shard_map(local_step, mesh=mesh, in_specs=(tok_spec, tok_spec, P(None, 'dp', None, None), tok_spec, P()), out_specs=(P(), P(), tok_spec), check_vma=False)
```

```python
import jax
import jax.numpy as jnp
from jax import lax
from jax.experimental import pallas as pl
from jax.experimental.pallas import tpu as pltpu
from jax.sharding import PartitionSpec as P

AUX_COEF = 0.02
MESH = pl.DeviceIdType.MESH

NB = 4
NC = 4
NU = 3
AGL = 10
LAG = {'a': (2, 1), 'b': (3, 3), 'c': (4, 3), 'g': (4, 3), 'd': (6, 0), 'e': (7, 3)}
FIRST = {'a': (1, 2), 'b': (2, 3), 'c': (3, 3), 'g': (3, 3), 'd': (4, 3), 'e': (6, 1)}
DRAIN = (('a', 1), ('g', 5), ('e', 6), ('g', 4), ('a', 0), ('b', 2), ('c', 3), ('g', 3), ('d', 5), ('b', 1), ('d', 4),
         ('c', 2), ('g', 2), ('b', 0), ('d', 3), ('c', 1), ('g', 1), ('e', 5), ('d', 2), ('c', 0), ('g', 0), ('e', 4),
         ('d', 1), ('e', 3), ('d', 0), ('e', 2), ('e', 1), ('e', 0))

NT = (((1,), (1,)), ((), ()))
TN = (((0,), (0,)), ((), ()))


def step_kernel(n_lay, n_dev, tok_all, idx_hbm, eo_hbm, dy_hbm, u_hbm, w_hbm,
                fin, gout, wv, loss_out,
                idx_v, ebuf, ubuf, dbuf, part, rd, r1, r2, cnt_src, cnt_in, loss_src, loss_in,
                fcol, slot_v, lg_v, loss_acc,
                idx_sem, e_sem, u_sem, d_sem, w_sem, cs_sem, cr_sem, ls_sem, lr_sem, s_sem, r_sem):
    me = lax.axis_index('dp')
    core = me % 2
    xpos = (me // 2) % 2
    ypos = me // 4
    partner = me + 1 - 2 * core
    xn = me + 2 - 4 * xpos
    yn = me + 4 - 8 * ypos
    nbr_a = xn * (1 - core) + yn * core
    nbr_b = yn * (1 - core) + xn * core
    pa = xpos * (1 - core) + ypos * core
    pb = ypos * (1 - core) + xpos * core
    half = 4 * core
    quart = half + 2 * pa
    mine = quart + pb
    n_exp = w_hbm.shape[1]
    top_k = idx_hbm.shape[1]
    tok = u_hbm.shape[1]
    rows = ebuf.shape[1]
    ctok = rows // top_k

    def e_copy(lay, c, slot):
        return pltpu.make_async_copy(eo_hbm.at[lay, pl.ds(c * rows, rows)], ebuf.at[slot], e_sem.at[slot])

    def u_copy(lay):
        return pltpu.make_async_copy(u_hbm.at[lay], ubuf.at[lay % NU], u_sem.at[lay % NU])

    def d_copy(lay):
        return pltpu.make_async_copy(dy_hbm.at[lay], dbuf.at[lay % NU], d_sem.at[lay % NU])

    def w_copy(lay):
        return pltpu.make_async_copy(w_hbm.at[lay], wv.at[lay], w_sem.at[lay])

    idx_copy = pltpu.make_async_copy(idx_hbm, idx_v, idx_sem)
    idx_copy.start()
    w_copy(0).start()
    u_copy(0).start()
    d_copy(0).start()
    for j in range(NC):
        e_copy(0, j, j).start()
    w_copy(1).start()
    u_copy(1).start()
    d_copy(1).start()

    barrier = pltpu.get_barrier_semaphore()
    for d in range(1, n_dev):
        pl.semaphore_signal(barrier, inc=1, device_id=((me + d) % n_dev,), device_id_type=MESH)

    ones = jnp.ones((8, tok), jnp.bfloat16)
    row_id = lax.broadcasted_iota(jnp.int32, (8, 2 * n_exp), 0)
    e_id = lax.broadcasted_iota(jnp.int32, (n_exp, tok), 0)

    def count_rows(part_no, r0, r1):
        cnt = jnp.zeros((8, 2 * n_exp), jnp.float32)
        for r in range(r0, r1):
            hots = []
            for h in range(2):
                ids = idx_v[2 * r + h]
                acc = jnp.zeros((n_exp, tok), jnp.float32)
                for k in range(top_k):
                    acc = jnp.where(e_id == ids[k:k + 1], 1.0, acc)
                hots.append(acc.astype(jnp.bfloat16))
            both = jnp.concatenate(hots, axis=0)
            res = lax.dot_general(ones, both, NT, preferred_element_type=jnp.float32)
            cnt = jnp.where(row_id == r, res, cnt)
        cnt_src[part_no] = cnt
        cnt_in[part_no, me] = cnt

    def cnt_copy(p, to, frm):
        return pltpu.make_async_remote_copy(
            src_ref=cnt_src.at[p], dst_ref=cnt_in.at[p, frm], send_sem=cs_sem.at[p, to], recv_sem=cr_sem.at[p, frm],
            device_id=(to,), device_id_type=MESH)

    def send_counts(p):
        for d in range(1, n_dev):
            cnt_copy(p, (me + d) % n_dev, me).start()

    def take_counts(p, lo, hi):
        for d in range(1, n_dev):
            cnt_copy(p, (me + d) % n_dev, (me + d) % n_dev).wait_recv()
        tot = cnt_in[p, 0]
        for j in range(1, n_dev):
            tot = tot + cnt_in[p, j]
        cols = jnp.transpose(tot * pull)
        for i in range(lo, hi):
            o = (i % 2) * n_exp
            fcol[i] = jnp.broadcast_to(cols[o:o + n_exp, i // 2:i // 2 + 1], (n_exp, fcol.shape[2]))

    idx_copy.wait()
    count_rows(0, 0, 1)
    loss_acc[...] = jnp.zeros_like(loss_acc)
    pl.semaphore_wait(barrier, n_dev - 1)
    send_counts(0)

    def loss_copy(to, frm):
        return pltpu.make_async_remote_copy(
            src_ref=loss_src, dst_ref=loss_in.at[frm], send_sem=ls_sem.at[to], recv_sem=lr_sem.at[frm],
            device_id=(to,), device_id_type=MESH)

    def rcopy(stage, src, dst, m, dev):
        return pltpu.make_async_remote_copy(
            src_ref=src, dst_ref=dst, send_sem=s_sem.at[stage, m], recv_sem=r_sem.at[stage, m],
            device_id=(dev,), device_id_type=MESH)

    def c_pair(m):
        return rcopy(0, part.at[m, pl.ds(4 - half, 4)], rd.at[m], m, partner)

    def c_rs1(m):
        return rcopy(1, part.at[m, pl.ds(half + 2 - 2 * pa, 2)], r1.at[m], m, nbr_a)

    def c_rs2(m):
        return rcopy(2, part.at[m, pl.ds(quart + 1 - pb, 1)], r2.at[m], m, nbr_b)

    def c_ag1(m, p):
        return rcopy(3, fin.at[m, pl.ds(p, 1)], fin.at[m, pl.ds(p, 1)], m, nbr_b)

    def c_ag2(m, p):
        return rcopy(4, fin.at[m, pl.ds(p, 2)], fin.at[m, pl.ds(p, 2)], m, nbr_a)

    def c_out(m, p):
        return rcopy(5, fin.at[m, pl.ds(p, 4)], fin.at[m, pl.ds(p, 4)], m, partner)

    def do_a(m):
        c_pair(m).wait_recv()
        o = 2 - 2 * pa
        part[m, pl.ds(half + o, 2)] += rd[m, pl.ds(o, 2)]
        part[m, pl.ds(quart, 2)] += rd[m, pl.ds(2 * pa, 2)]
        c_rs1(m).start()

    def do_b(m):
        c_rs1(m).wait_recv()
        o = 1 - pb
        part[m, pl.ds(quart + o, 1)] += r1[m, pl.ds(o, 1)]
        part[m, pl.ds(mine, 1)] += r1[m, pl.ds(pb, 1)]
        c_rs2(m).start()

    def do_c(m):
        c_rs2(m).wait_recv()
        fin[m, pl.ds(mine, 1)] = part[m, pl.ds(mine, 1)] + r2[m]

    def do_ag1(m):
        c_ag1(m, mine).start()

    def do_d(m):
        c_ag1(m, quart + 1 - pb).wait_recv()
        c_ag2(m, quart).start()

    def do_e(m):
        c_ag2(m, half + 2 - 2 * pa).wait_recv()
        c_out(m, half).start()

    def do_f(m):
        c_out(m, 4 - half).wait_recv()

    hr = rows // 2
    lanes = 2 * ctok
    lane = lax.broadcasted_iota(jnp.int32, (top_k, lanes), 1)
    e_half = lax.broadcasted_iota(jnp.int32, (n_exp, lanes), 0)
    first = lax.broadcasted_iota(jnp.int32, (top_k, lanes), 0) == 0
    scale = float(tok_all)
    pull = AUX_COEF * n_exp / (top_k * tok_all)

    def slot_chunk(lay, c, slot):
        lo = (c // 2) * lanes
        dcols = dbuf[lay % NU, lo:lo + lanes, :]
        s = [lax.dot_general(ebuf[slot, h * hr:(h + 1) * hr, :], dcols, NT, preferred_element_type=jnp.float32) for h in range(2)]
        acc = jnp.zeros((top_k, lanes), jnp.float32)
        for i in range(ctok):
            j = i * top_k
            acc = jnp.where(lane == (c % 2) * ctok + i, s[j // hr][j % hr:j % hr + top_k], acc)
        if c % 2:
            slot_v[lay % 2, :, lo:lo + lanes] += acc
        else:
            slot_v[lay % 2, :, lo:lo + lanes] = acc

    def logit_part(lay):
        for h in range(2):
            lo = h * lanes
            lg_v[:, lo:lo + lanes] = lax.dot_general(
                wv[lay], ubuf[lay % NU, lo:lo + lanes, :], NT, preferred_element_type=jnp.float32)

    def g_part(lay, to, h, keep):
        lo = h * lanes
        logits = lg_v[:, lo:lo + lanes]
        ids = idx_v[lay, :, lo:lo + lanes]
        ex = jnp.exp(logits - jnp.max(logits, axis=0, keepdims=True))
        prob = ex / jnp.sum(ex, axis=0, keepdims=True)
        chosen = jnp.concatenate(
            [jnp.sum(jnp.where(e_half == ids[k:k + 1], logits, 0.0), axis=0, keepdims=True) for k in range(top_k)], axis=0)
        ge = jnp.exp(chosen - jnp.max(chosen, axis=0, keepdims=True))
        gate = ge / jnp.sum(ge, axis=0, keepdims=True)
        slots = slot_v[lay % 2, :, lo:lo + lanes]
        dd = scale * slots
        dch = gate * (dd - jnp.sum(gate * dd, axis=0, keepdims=True))
        pf = prob * fcol[lay]
        pf_sum = jnp.sum(pf, axis=0, keepdims=True)
        g = pf - prob * pf_sum
        for k in range(top_k):
            g = g + jnp.where(e_half == ids[k:k + 1], dch[k:k + 1], 0.0)
        main = gate * slots + jnp.where(first, pf_sum * (1.0 / tok_all), 0.0)
        total = loss_acc[:, lo:lo + lanes] + main
        loss_acc[:, lo:lo + lanes] = total if keep is None else jnp.where(keep, total, loss_acc[:, lo:lo + lanes])
        gout[to, :, lo:lo + lanes] = g.astype(jnp.bfloat16)

    def p_part(lay, to):
        dim = ubuf.shape[2]
        for h in range(2):
            lo = h * (dim // 2)
            pg = jnp.dot(gout[to], ubuf[lay % NU, :, lo:lo + dim // 2], preferred_element_type=jnp.float32)
            part[to, :, :, lo:lo + dim // 2] = pg.reshape(part.shape[1:3] + (dim // 2,))

    def refill(lay, c):
        @pl.when(lay + 1 < n_lay)
        def _():
            e_copy(lay + 1, c, c).start()

    def fetch(lay):
        @pl.when(lay + 2 < n_lay)
        def _():
            w_copy(lay + 2).start()
            u_copy(lay + 2).start()
            d_copy(lay + 2).start()

    run = {'a': do_a, 'b': do_b, 'c': do_c, 'g': do_ag1, 'd': do_d, 'e': do_e}

    w_copy(0).wait()
    u_copy(0).wait()
    d_copy(0).wait()
    for c in range(NC):
        e_copy(0, c, c).wait()
        slot_chunk(0, c, c)
        if c == 0:
            logit_part(0)
        e_copy(1, c, c).start()
    w_copy(2).start()
    u_copy(2).start()
    d_copy(2).start()
    take_counts(0, 0, 2)
    for h in range(2):
        g_part(0, 0, h, None)
    p_part(0, 0)
    c_pair(0).start()
    count_rows(1, 1, n_lay // 2)
    send_counts(1)

    @pl.loop(1, n_lay)
    def _(lay):
        base = 0
        prev = lay - 1
        to = jnp.where(lay == 1, lay, prev)
        keep = lay >= 2

        def comm(c):
            for k in 'abcgde':
                if FIRST[k][1] == c:
                    @pl.when(lay == FIRST[k][0])
                    def _(k=k):
                        run[k](0)
                if LAG[k][1] == c:
                    lag = LAG[k][0]
                    hi = min(n_lay, lag + AGL) if k in 'gde' else n_lay

                    @pl.when(jnp.logical_and(lay > lag, lay < hi))
                    def _(k=k, lag=lag):
                        run[k](lay - lag)

        comm(0)
        w_copy(lay).wait()
        u_copy(lay).wait()
        d_copy(lay).wait()
        e_copy(lay, 0, base).wait()
        slot_chunk(lay, 0, base)
        g_part(prev, to, 0, keep)
        refill(lay, 0)

        comm(1)
        e_copy(lay, 1, base + 1).wait()
        slot_chunk(lay, 1, base + 1)
        g_part(prev, to, 1, keep)
        refill(lay, 1)

        comm(2)
        e_copy(lay, 2, base + 2).wait()
        slot_chunk(lay, 2, base + 2)
        p_part(prev, to)
        refill(lay, 2)
        fetch(lay)

        @pl.when(lay >= 2)
        def _():
            c_pair(lay - 1).start()

        comm(3)
        e_copy(lay, 3, base + 3).wait()
        slot_chunk(lay, 3, base + 3)
        logit_part(lay)
        refill(lay, 3)

        @pl.when(lay == 2)
        def _():
            take_counts(1, 2, n_lay)

    last = n_lay - 1
    for h in range(2):
        g_part(last, last, h, None)
    p_part(last, last)
    la = loss_acc[...]
    lv = la[:, :128]
    for j in range(1, tok // 128):
        lv = lv + la[:, 128 * j:128 * (j + 1)]
    loss_src[...] = lv
    loss_in[me] = lv
    c_pair(last).start()

    for d in range(1, n_dev):
        loss_copy((me + d) % n_dev, me).start()
    for k, back in DRAIN:
        run[k](last - back)

    for d in range(1, n_dev):
        loss_copy((me + d) % n_dev, (me + d) % n_dev).wait_recv()
    tot = loss_in[0]
    for j in range(1, n_dev):
        tot = tot + loss_in[j]
    loss_out[...] = tot
    for d in range(1, n_dev):
        cnt_copy(0, (me + d) % n_dev, me).wait_send()
        cnt_copy(1, (me + d) % n_dev, me).wait_send()
        loss_copy((me + d) % n_dev, me).wait_send()

    @pl.loop(0, n_lay)
    def _(m):
        do_f(m)
        c_pair(m).wait_send()
        c_rs1(m).wait_send()
        c_rs2(m).wait_send()
        c_ag1(m, mine).wait_send()
        c_ag2(m, quart).wait_send()
        c_out(m, half).wait_send()


def out_kernel(n_lay, g_v, w_v, f_v, l_v, dn_hbm, dr_hbm, loss, stage, st_sem, f_sem):
    def put(lay):
        return pltpu.make_async_copy(stage.at[lay], dn_hbm.at[lay], st_sem.at[lay])

    def put_f(lay):
        return pltpu.make_async_copy(f_v.at[lay], dr_hbm.at[lay], f_sem.at[lay])

    @pl.loop(0, n_lay)
    def _(lay):
        put_f(lay).start()

    @pl.loop(0, n_lay)
    def _(lay):
        dn = lax.dot_general(g_v[lay], w_v[lay], TN, preferred_element_type=jnp.float32)
        stage[lay] = dn.astype(jnp.bfloat16)
        put(lay).start()

    loss[0, 0] = jnp.sum(l_v[...])

    @pl.loop(0, n_lay)
    def _(lay):
        put(lay).wait()
        put_f(lay).wait()


def solution(mesh):
    n_dev = mesh.shape['dp']

    def local_step(u_norm, expert_idx, expert_out, d_out, w_router):
        n_lay, tok, dim = u_norm.shape
        n_exp = w_router.shape[2]
        top_k = expert_idx.shape[2]
        tok_all = tok * n_dev
        f32, bf16 = jnp.float32, jnp.bfloat16
        idx_t = jnp.swapaxes(expert_idx, 1, 2)
        w_t = jnp.swapaxes(w_router, 1, 2)
        eo = expert_out.reshape(n_lay, tok * top_k, dim)
        rows = tok * top_k // NC
        pieces = 8
        prow = n_exp // pieces
        any_spec = pl.BlockSpec(memory_space=pl.ANY)
        vm_spec = pl.BlockSpec(memory_space=pltpu.VMEM)
        dma = pltpu.SemaphoreType.DMA
        fin, g_all, w_all, loss_v = pl.pallas_call(
            lambda *refs: step_kernel(n_lay, n_dev, tok_all, *refs),
            out_shape=(
                pltpu.VMEM((n_lay, pieces, prow, dim), f32),
                pltpu.VMEM((n_lay, n_exp, tok), bf16),
                pltpu.VMEM((n_lay, n_exp, dim), bf16),
                pltpu.VMEM((8, 128), f32),
            ),
            in_specs=[any_spec] * 5,
            out_specs=(vm_spec,) * 4,
            scratch_shapes=[
                pltpu.VMEM((n_lay, top_k, tok), jnp.int32),
                pltpu.VMEM((NB, rows, dim), bf16),
                pltpu.VMEM((NU, tok, dim), bf16),
                pltpu.VMEM((NU, tok, dim), bf16),
                pltpu.VMEM((n_lay, pieces, prow, dim), f32),
                pltpu.VMEM((n_lay, pieces // 2, prow, dim), f32),
                pltpu.VMEM((n_lay, pieces // 4, prow, dim), f32),
                pltpu.VMEM((n_lay, pieces // 8, prow, dim), f32),
                pltpu.VMEM((2, 8, 128), f32),
                pltpu.VMEM((2, n_dev, 8, 128), f32),
                pltpu.VMEM((8, 128), f32),
                pltpu.VMEM((n_dev, 8, 128), f32),
                pltpu.VMEM((n_lay, n_exp, 128), f32),
                pltpu.VMEM((2, top_k, tok), f32),
                pltpu.VMEM((n_exp, tok), f32),
                pltpu.VMEM((top_k, tok), f32),
                dma, dma((NB,)), dma((NU,)), dma((NU,)), dma((n_lay,)),
                dma((2, n_dev)), dma((2, n_dev)), dma((n_dev,)), dma((n_dev,)),
                dma((6, n_lay)), dma((6, n_lay)),
            ],
            compiler_params=pltpu.CompilerParams(
                collective_id=0, has_side_effects=True, vmem_limit_bytes=48 << 20),
            name='router_step',
        )(idx_t, eo, d_out, u_norm, w_t)
        d_norm, d_rt, loss = pl.pallas_call(
            lambda *refs: out_kernel(n_lay, *refs),
            out_shape=(
                jax.ShapeDtypeStruct((n_lay, tok, dim), bf16),
                jax.ShapeDtypeStruct((n_lay, pieces, prow, dim), f32),
                jax.ShapeDtypeStruct((1, 1), f32),
            ),
            in_specs=[vm_spec] * 4,
            out_specs=(any_spec, any_spec, pl.BlockSpec(memory_space=pltpu.SMEM)),
            scratch_shapes=[pltpu.VMEM((n_lay, tok, dim), bf16), dma((n_lay,)), dma((n_lay,))],
            compiler_params=pltpu.CompilerParams(vmem_limit_bytes=20 << 20),
            name='router_out',
        )(g_all, w_all, fin, loss_v)
        d_router = jnp.swapaxes(d_rt.reshape(n_lay, n_exp, dim), 1, 2)
        return loss[0, 0], d_router, d_norm

    tok_spec = P(None, 'dp', None)
    return jax.shard_map(local_step, mesh=mesh, in_specs=(tok_spec, tok_spec, P(None, 'dp', None, None), tok_spec, P()), out_specs=(P(), P(), tok_spec), check_vma=False)
```

```python
import jax
import jax.numpy as jnp
from jax import lax
from jax.experimental import pallas as pl
from jax.experimental.pallas import tpu as pltpu
from jax.sharding import PartitionSpec as P

AUX_COEF = 0.02
MESH = pl.DeviceIdType.MESH

NB = 3
NC = 4
NU = 4
AGL = 10
LAG = {'a': (2, 1), 'b': (3, 3), 'c': (4, 3), 'g': (4, 3), 'd': (6, 0), 'e': (7, 3)}
FIRST = {'a': (1, 2), 'b': (2, 3), 'c': (3, 3), 'g': (3, 3), 'd': (4, 3), 'e': (6, 1)}
DRAIN = (('a', 1), ('g', 5), ('e', 6), ('g', 4), ('a', 0), ('b', 2), ('c', 3), ('g', 3), ('d', 5), ('b', 1), ('d', 4),
         ('c', 2), ('g', 2), ('b', 0), ('d', 3), ('c', 1), ('g', 1), ('e', 5), ('d', 2), ('c', 0), ('g', 0), ('e', 4),
         ('d', 1), ('e', 3), ('d', 0), ('e', 2), ('e', 1), ('e', 0))

NT = (((1,), (1,)), ((), ()))
TN = (((0,), (0,)), ((), ()))


def step_kernel(n_lay, n_dev, tok_all, idx_hbm, eo_hbm, dy_hbm, u_hbm, w_hbm,
                fin, gout, wv, loss_out,
                idx_v, ebuf, ubuf, dbuf, part, rd, r1, r2, cnt_src, cnt_in, loss_src, loss_in,
                fcol, slot_v, lg_v, loss_acc,
                idx_sem, e_sem, u_sem, d_sem, w_sem, cs_sem, cr_sem, ls_sem, lr_sem, s_sem, r_sem):
    me = lax.axis_index('dp')
    core = me % 2
    xpos = (me // 2) % 2
    ypos = me // 4
    partner = me + 1 - 2 * core
    xn = me + 2 - 4 * xpos
    yn = me + 4 - 8 * ypos
    nbr_a = xn * (1 - core) + yn * core
    nbr_b = yn * (1 - core) + xn * core
    pa = xpos * (1 - core) + ypos * core
    pb = ypos * (1 - core) + xpos * core
    half = 4 * core
    quart = half + 2 * pa
    mine = quart + pb
    n_exp = w_hbm.shape[1]
    top_k = idx_hbm.shape[1]
    tok = u_hbm.shape[1]
    rows = ebuf.shape[1]
    ctok = rows // top_k

    def e_copy(lay, c, slot):
        return pltpu.make_async_copy(eo_hbm.at[lay, pl.ds(c * rows, rows)], ebuf.at[slot], e_sem.at[slot])

    def u_copy(lay):
        return pltpu.make_async_copy(u_hbm.at[lay], ubuf.at[lay % NU], u_sem.at[lay % NU])

    def d_copy(lay):
        return pltpu.make_async_copy(dy_hbm.at[lay], dbuf.at[lay % NU], d_sem.at[lay % NU])

    def w_copy(lay):
        return pltpu.make_async_copy(w_hbm.at[lay], wv.at[lay], w_sem.at[lay])

    idx_copy = pltpu.make_async_copy(idx_hbm, idx_v, idx_sem)
    idx_copy.start()
    w_copy(0).start()
    u_copy(0).start()
    d_copy(0).start()
    for j in range(NB):
        e_copy(0, j, j).start()
    w_copy(1).start()
    u_copy(1).start()
    d_copy(1).start()

    barrier = pltpu.get_barrier_semaphore()
    for d in range(1, n_dev):
        pl.semaphore_signal(barrier, inc=1, device_id=((me + d) % n_dev,), device_id_type=MESH)

    ones = jnp.ones((8, tok), jnp.bfloat16)
    row_id = lax.broadcasted_iota(jnp.int32, (8, 2 * n_exp), 0)
    e_id = lax.broadcasted_iota(jnp.int32, (n_exp, tok), 0)

    def count_rows(part_no, r0, r1):
        cnt = jnp.zeros((8, 2 * n_exp), jnp.float32)
        for r in range(r0, r1):
            hots = []
            for h in range(2):
                ids = idx_v[2 * r + h]
                acc = jnp.zeros((n_exp, tok), jnp.float32)
                for k in range(top_k):
                    acc = jnp.where(e_id == ids[k:k + 1], 1.0, acc)
                hots.append(acc.astype(jnp.bfloat16))
            both = jnp.concatenate(hots, axis=0)
            res = lax.dot_general(ones, both, NT, preferred_element_type=jnp.float32)
            cnt = jnp.where(row_id == r, res, cnt)
        cnt_src[part_no] = cnt
        cnt_in[part_no, me] = cnt

    def cnt_copy(p, to, frm):
        return pltpu.make_async_remote_copy(
            src_ref=cnt_src.at[p], dst_ref=cnt_in.at[p, frm], send_sem=cs_sem.at[p, to], recv_sem=cr_sem.at[p, frm],
            device_id=(to,), device_id_type=MESH)

    def send_counts(p):
        for d in range(1, n_dev):
            cnt_copy(p, (me + d) % n_dev, me).start()

    def take_counts(p, lo, hi):
        for d in range(1, n_dev):
            cnt_copy(p, (me + d) % n_dev, (me + d) % n_dev).wait_recv()
        tot = cnt_in[p, 0]
        for j in range(1, n_dev):
            tot = tot + cnt_in[p, j]
        cols = jnp.transpose(tot * pull)
        for i in range(lo, hi):
            o = (i % 2) * n_exp
            fcol[i] = jnp.broadcast_to(cols[o:o + n_exp, i // 2:i // 2 + 1], (n_exp, fcol.shape[2]))

    idx_copy.wait()
    count_rows(0, 0, 1)
    loss_acc[...] = jnp.zeros_like(loss_acc)
    pl.semaphore_wait(barrier, n_dev - 1)
    send_counts(0)

    def loss_copy(to, frm):
        return pltpu.make_async_remote_copy(
            src_ref=loss_src, dst_ref=loss_in.at[frm], send_sem=ls_sem.at[to], recv_sem=lr_sem.at[frm],
            device_id=(to,), device_id_type=MESH)

    def rcopy(stage, src, dst, m, dev):
        return pltpu.make_async_remote_copy(
            src_ref=src, dst_ref=dst, send_sem=s_sem.at[stage, m], recv_sem=r_sem.at[stage, m],
            device_id=(dev,), device_id_type=MESH)

    def c_pair(m):
        return rcopy(0, part.at[m, pl.ds(4 - half, 4)], rd.at[m], m, partner)

    def c_rs1(m):
        return rcopy(1, part.at[m, pl.ds(half + 2 - 2 * pa, 2)], r1.at[m], m, nbr_a)

    def c_rs2(m):
        return rcopy(2, part.at[m, pl.ds(quart + 1 - pb, 1)], r2.at[m], m, nbr_b)

    def c_ag1(m, p):
        return rcopy(3, fin.at[m, pl.ds(p, 1)], fin.at[m, pl.ds(p, 1)], m, nbr_b)

    def c_ag2(m, p):
        return rcopy(4, fin.at[m, pl.ds(p, 2)], fin.at[m, pl.ds(p, 2)], m, nbr_a)

    def c_out(m, p):
        return rcopy(5, fin.at[m, pl.ds(p, 4)], fin.at[m, pl.ds(p, 4)], m, partner)

    def do_a(m):
        c_pair(m).wait_recv()
        o = 2 - 2 * pa
        part[m, pl.ds(half + o, 2)] += rd[m, pl.ds(o, 2)]
        part[m, pl.ds(quart, 2)] += rd[m, pl.ds(2 * pa, 2)]
        c_rs1(m).start()

    def do_b(m):
        c_rs1(m).wait_recv()
        o = 1 - pb
        part[m, pl.ds(quart + o, 1)] += r1[m, pl.ds(o, 1)]
        part[m, pl.ds(mine, 1)] += r1[m, pl.ds(pb, 1)]
        c_rs2(m).start()

    def do_c(m):
        c_rs2(m).wait_recv()
        fin[m, pl.ds(mine, 1)] = part[m, pl.ds(mine, 1)] + r2[m]

    def do_ag1(m):
        c_ag1(m, mine).start()

    def do_d(m):
        c_ag1(m, quart + 1 - pb).wait_recv()
        c_ag2(m, quart).start()

    def do_e(m):
        c_ag2(m, half + 2 - 2 * pa).wait_recv()
        c_out(m, half).start()

    def do_f(m):
        c_out(m, 4 - half).wait_recv()

    hr = rows // 2
    lanes = 2 * ctok
    lane = lax.broadcasted_iota(jnp.int32, (top_k, lanes), 1)
    e_half = lax.broadcasted_iota(jnp.int32, (n_exp, lanes), 0)
    first = lax.broadcasted_iota(jnp.int32, (top_k, lanes), 0) == 0
    scale = float(tok_all)
    pull = AUX_COEF * n_exp / (top_k * tok_all)

    def slot_chunk(lay, c, slot):
        lo = (c // 2) * lanes
        dcols = dbuf[lay % NU, lo:lo + lanes, :]
        s = [lax.dot_general(ebuf[slot, h * hr:(h + 1) * hr, :], dcols, NT, preferred_element_type=jnp.float32) for h in range(2)]
        acc = jnp.zeros((top_k, lanes), jnp.float32)
        for i in range(ctok):
            j = i * top_k
            acc = jnp.where(lane == (c % 2) * ctok + i, s[j // hr][j % hr:j % hr + top_k], acc)
        if c % 2:
            slot_v[lay % 2, :, lo:lo + lanes] += acc
        else:
            slot_v[lay % 2, :, lo:lo + lanes] = acc

    def logit_part(lay):
        for h in range(2):
            lo = h * lanes
            lg_v[:, lo:lo + lanes] = lax.dot_general(
                wv[lay], ubuf[lay % NU, lo:lo + lanes, :], NT, preferred_element_type=jnp.float32)

    def g_part(lay, to, h, keep):
        lo = h * lanes
        logits = lg_v[:, lo:lo + lanes]
        ids = idx_v[lay, :, lo:lo + lanes]
        ex = jnp.exp(logits - jnp.max(logits, axis=0, keepdims=True))
        prob = ex / jnp.sum(ex, axis=0, keepdims=True)
        chosen = jnp.concatenate(
            [jnp.sum(jnp.where(e_half == ids[k:k + 1], logits, 0.0), axis=0, keepdims=True) for k in range(top_k)], axis=0)
        ge = jnp.exp(chosen - jnp.max(chosen, axis=0, keepdims=True))
        gate = ge / jnp.sum(ge, axis=0, keepdims=True)
        slots = slot_v[lay % 2, :, lo:lo + lanes]
        dd = scale * slots
        dch = gate * (dd - jnp.sum(gate * dd, axis=0, keepdims=True))
        pf = prob * fcol[lay]
        pf_sum = jnp.sum(pf, axis=0, keepdims=True)
        g = pf - prob * pf_sum
        for k in range(top_k):
            g = g + jnp.where(e_half == ids[k:k + 1], dch[k:k + 1], 0.0)
        main = gate * slots + jnp.where(first, pf_sum * (1.0 / tok_all), 0.0)
        total = loss_acc[:, lo:lo + lanes] + main
        loss_acc[:, lo:lo + lanes] = total if keep is None else jnp.where(keep, total, loss_acc[:, lo:lo + lanes])
        gout[to, :, lo:lo + lanes] = g.astype(jnp.bfloat16)

    def p_part(lay, to):
        dim = ubuf.shape[2]
        for h in range(2):
            lo = h * (dim // 2)
            pg = jnp.dot(gout[to], ubuf[lay % NU, :, lo:lo + dim // 2], preferred_element_type=jnp.float32)
            part[to, :, :, lo:lo + dim // 2] = pg.reshape(part.shape[1:3] + (dim // 2,))

    def slot_of(lay, c):
        return (lay * NC + c) % NB

    def refill(lay, c):
        dl, dc = (c + NB) // NC, (c + NB) % NC

        @pl.when(lay + dl < n_lay)
        def _():
            e_copy(lay + dl, dc, slot_of(lay, c)).start()

    def fetch(copy, lay):
        @pl.when(lay + 2 < n_lay)
        def _():
            copy(lay + 2).start()

    run = {'a': do_a, 'b': do_b, 'c': do_c, 'g': do_ag1, 'd': do_d, 'e': do_e}

    w_copy(0).wait()
    u_copy(0).wait()
    d_copy(0).wait()
    for c in range(NC):
        e_copy(0, c, slot_of(0, c)).wait()
        slot_chunk(0, c, slot_of(0, c))
        if c == 0:
            logit_part(0)
        dl, dc = (c + NB) // NC, (c + NB) % NC
        e_copy(dl, dc, slot_of(0, c)).start()
    w_copy(2).start()
    u_copy(2).start()
    d_copy(2).start()
    take_counts(0, 0, 2)
    for h in range(2):
        g_part(0, 0, h, None)
    p_part(0, 0)
    c_pair(0).start()
    count_rows(1, 1, n_lay // 2)
    send_counts(1)

    @pl.loop(1, n_lay)
    def _(lay):
        prev = lay - 1
        to = jnp.where(lay == 1, lay, prev)
        keep = lay >= 2

        def comm(c):
            for k in 'abcgde':
                if FIRST[k][1] == c:
                    @pl.when(lay == FIRST[k][0])
                    def _(k=k):
                        run[k](0)
                if LAG[k][1] == c:
                    lag = LAG[k][0]
                    hi = min(n_lay, lag + AGL) if k in 'gde' else n_lay

                    @pl.when(jnp.logical_and(lay > lag, lay < hi))
                    def _(k=k, lag=lag):
                        run[k](lay - lag)

        comm(0)
        w_copy(lay).wait()
        u_copy(lay).wait()
        d_copy(lay).wait()
        e_copy(lay, 0, slot_of(lay, 0)).wait()
        slot_chunk(lay, 0, slot_of(lay, 0))
        g_part(prev, to, 0, keep)
        refill(lay, 0)
        fetch(d_copy, lay)

        comm(1)
        e_copy(lay, 1, slot_of(lay, 1)).wait()
        slot_chunk(lay, 1, slot_of(lay, 1))
        g_part(prev, to, 1, keep)
        refill(lay, 1)
        fetch(u_copy, lay)

        comm(2)
        e_copy(lay, 2, slot_of(lay, 2)).wait()
        slot_chunk(lay, 2, slot_of(lay, 2))
        p_part(prev, to)
        refill(lay, 2)
        fetch(w_copy, lay)

        @pl.when(lay >= 2)
        def _():
            c_pair(lay - 1).start()

        comm(3)
        e_copy(lay, 3, slot_of(lay, 3)).wait()
        slot_chunk(lay, 3, slot_of(lay, 3))
        logit_part(lay)
        refill(lay, 3)

        @pl.when(lay == 2)
        def _():
            take_counts(1, 2, n_lay)

    last = n_lay - 1
    for h in range(2):
        g_part(last, last, h, None)
    p_part(last, last)
    la = loss_acc[...]
    lv = la[:, :128]
    for j in range(1, tok // 128):
        lv = lv + la[:, 128 * j:128 * (j + 1)]
    loss_src[...] = lv
    loss_in[me] = lv
    c_pair(last).start()

    for d in range(1, n_dev):
        loss_copy((me + d) % n_dev, me).start()
    for k, back in DRAIN:
        run[k](last - back)

    for d in range(1, n_dev):
        loss_copy((me + d) % n_dev, (me + d) % n_dev).wait_recv()
    tot = loss_in[0]
    for j in range(1, n_dev):
        tot = tot + loss_in[j]
    loss_out[...] = tot
    for d in range(1, n_dev):
        cnt_copy(0, (me + d) % n_dev, me).wait_send()
        cnt_copy(1, (me + d) % n_dev, me).wait_send()
        loss_copy((me + d) % n_dev, me).wait_send()

    @pl.loop(0, n_lay)
    def _(m):
        do_f(m)
        c_pair(m).wait_send()
        c_rs1(m).wait_send()
        c_rs2(m).wait_send()
        c_ag1(m, mine).wait_send()
        c_ag2(m, quart).wait_send()
        c_out(m, half).wait_send()


def out_kernel(n_lay, g_v, w_v, f_v, l_v, dn_hbm, dr_hbm, loss, stage, st_sem, f_sem):
    def put(lay):
        return pltpu.make_async_copy(stage.at[lay], dn_hbm.at[lay], st_sem.at[lay])

    def put_f(lay):
        return pltpu.make_async_copy(f_v.at[lay], dr_hbm.at[lay], f_sem.at[lay])

    @pl.loop(0, n_lay)
    def _(lay):
        put_f(lay).start()

    @pl.loop(0, n_lay)
    def _(lay):
        dn = lax.dot_general(g_v[lay], w_v[lay], TN, preferred_element_type=jnp.float32)
        stage[lay] = dn.astype(jnp.bfloat16)
        put(lay).start()

    loss[0, 0] = jnp.sum(l_v[...])

    @pl.loop(0, n_lay)
    def _(lay):
        put(lay).wait()
        put_f(lay).wait()


def solution(mesh):
    n_dev = mesh.shape['dp']

    def local_step(u_norm, expert_idx, expert_out, d_out, w_router):
        n_lay, tok, dim = u_norm.shape
        n_exp = w_router.shape[2]
        top_k = expert_idx.shape[2]
        tok_all = tok * n_dev
        f32, bf16 = jnp.float32, jnp.bfloat16
        idx_t = jnp.swapaxes(expert_idx, 1, 2)
        w_t = jnp.swapaxes(w_router, 1, 2)
        eo = expert_out.reshape(n_lay, tok * top_k, dim)
        rows = tok * top_k // NC
        pieces = 8
        prow = n_exp // pieces
        any_spec = pl.BlockSpec(memory_space=pl.ANY)
        vm_spec = pl.BlockSpec(memory_space=pltpu.VMEM)
        dma = pltpu.SemaphoreType.DMA
        fin, g_all, w_all, loss_v = pl.pallas_call(
            lambda *refs: step_kernel(n_lay, n_dev, tok_all, *refs),
            out_shape=(
                pltpu.VMEM((n_lay, pieces, prow, dim), f32),
                pltpu.VMEM((n_lay, n_exp, tok), bf16),
                pltpu.VMEM((n_lay, n_exp, dim), bf16),
                pltpu.VMEM((8, 128), f32),
            ),
            in_specs=[any_spec] * 5,
            out_specs=(vm_spec,) * 4,
            scratch_shapes=[
                pltpu.VMEM((n_lay, top_k, tok), jnp.int32),
                pltpu.VMEM((NB, rows, dim), bf16),
                pltpu.VMEM((NU, tok, dim), bf16),
                pltpu.VMEM((NU, tok, dim), bf16),
                pltpu.VMEM((n_lay, pieces, prow, dim), f32),
                pltpu.VMEM((n_lay, pieces // 2, prow, dim), f32),
                pltpu.VMEM((n_lay, pieces // 4, prow, dim), f32),
                pltpu.VMEM((n_lay, pieces // 8, prow, dim), f32),
                pltpu.VMEM((2, 8, 128), f32),
                pltpu.VMEM((2, n_dev, 8, 128), f32),
                pltpu.VMEM((8, 128), f32),
                pltpu.VMEM((n_dev, 8, 128), f32),
                pltpu.VMEM((n_lay, n_exp, 128), f32),
                pltpu.VMEM((2, top_k, tok), f32),
                pltpu.VMEM((n_exp, tok), f32),
                pltpu.VMEM((top_k, tok), f32),
                dma, dma((NB,)), dma((NU,)), dma((NU,)), dma((n_lay,)),
                dma((2, n_dev)), dma((2, n_dev)), dma((n_dev,)), dma((n_dev,)),
                dma((6, n_lay)), dma((6, n_lay)),
            ],
            compiler_params=pltpu.CompilerParams(
                collective_id=0, has_side_effects=True, vmem_limit_bytes=48 << 20),
            name='router_step',
        )(idx_t, eo, d_out, u_norm, w_t)
        d_norm, d_rt, loss = pl.pallas_call(
            lambda *refs: out_kernel(n_lay, *refs),
            out_shape=(
                jax.ShapeDtypeStruct((n_lay, tok, dim), bf16),
                jax.ShapeDtypeStruct((n_lay, pieces, prow, dim), f32),
                jax.ShapeDtypeStruct((1, 1), f32),
            ),
            in_specs=[vm_spec] * 4,
            out_specs=(any_spec, any_spec, pl.BlockSpec(memory_space=pltpu.SMEM)),
            scratch_shapes=[pltpu.VMEM((n_lay, tok, dim), bf16), dma((n_lay,)), dma((n_lay,))],
            compiler_params=pltpu.CompilerParams(vmem_limit_bytes=20 << 20),
            name='router_out',
        )(g_all, w_all, fin, loss_v)
        d_router = jnp.swapaxes(d_rt.reshape(n_lay, n_exp, dim), 1, 2)
        return loss[0, 0], d_router, d_norm

    tok_spec = P(None, 'dp', None)
    return jax.shard_map(local_step, mesh=mesh, in_specs=(tok_spec, tok_spec, P(None, 'dp', None, None), tok_spec, P()), out_specs=(P(), P(), tok_spec), check_vma=False)
```

```python
import jax
import jax.numpy as jnp
from jax import lax
from jax.experimental import pallas as pl
from jax.experimental.pallas import tpu as pltpu
from jax.sharding import PartitionSpec as P

AUX_COEF = 0.02
MESH = pl.DeviceIdType.MESH

NB = 3
NC = 4
NU = 4
AGL = 12
LAG = {'a': (2, 1), 'b': (3, 3), 'c': (4, 3), 'g': (4, 3), 'd': (6, 0), 'e': (8, 1)}
FIRST = {'a': (1, 1), 'b': (2, 3), 'c': (3, 3), 'g': (3, 3), 'd': (5, 0), 'e': (6, 2)}
DRAIN = (('a', 1), ('d', 5), ('e', 7), ('e', 6), ('a', 0), ('b', 2), ('c', 3), ('d', 4), ('b', 1), ('g', 3), ('c', 2),
         ('e', 5), ('g', 2), ('b', 0), ('c', 1), ('g', 1), ('d', 3), ('e', 4), ('d', 2), ('x', 0), ('c', 0), ('g', 0), ('d', 1),
         ('e', 3), ('y', 0), ('d', 0), ('e', 2), ('e', 1), ('e', 0))
OLD = 9

NT = (((1,), (1,)), ((), ()))
TN = (((0,), (0,)), ((), ()))


def step_kernel(n_lay, n_dev, tok_all, idx_hbm, eo_hbm, dy_hbm, u_hbm, w_hbm,
                fin, gout, wv, loss_out,
                idx_v, ebuf, ubuf, dbuf, part, rd, r1, r2, cnt_src, cnt_in, loss_src, loss_in,
                fcol, slot_v, lg_v, loss_acc,
                idx_sem, e_sem, u_sem, d_sem, w_sem, cs_sem, cr_sem, ls_sem, lr_sem, s_sem, r_sem):
    me = lax.axis_index('dp')
    core = me % 2
    xpos = (me // 2) % 2
    ypos = me // 4
    partner = me + 1 - 2 * core
    xn = me + 2 - 4 * xpos
    yn = me + 4 - 8 * ypos
    nbr_a = xn * (1 - core) + yn * core
    nbr_b = yn * (1 - core) + xn * core
    pa = xpos * (1 - core) + ypos * core
    pb = ypos * (1 - core) + xpos * core
    half = 4 * core
    quart = half + 2 * pa
    mine = quart + pb
    n_exp = w_hbm.shape[1]
    top_k = idx_hbm.shape[1]
    tok = u_hbm.shape[1]
    rows = ebuf.shape[1]
    ctok = rows // top_k

    def e_copy(lay, c, slot):
        return pltpu.make_async_copy(eo_hbm.at[lay, pl.ds(c * rows, rows)], ebuf.at[slot], e_sem.at[slot])

    def u_copy(lay):
        return pltpu.make_async_copy(u_hbm.at[lay], ubuf.at[lay % NU], u_sem.at[lay % NU])

    def d_copy(lay):
        return pltpu.make_async_copy(dy_hbm.at[lay], dbuf.at[lay % NU], d_sem.at[lay % NU])

    def w_copy(lay):
        return pltpu.make_async_copy(w_hbm.at[lay], wv.at[lay], w_sem.at[lay])

    idx_copy = pltpu.make_async_copy(idx_hbm, idx_v, idx_sem)
    idx_copy.start()
    w_copy(0).start()
    u_copy(0).start()
    d_copy(0).start()
    for j in range(NB):
        e_copy(0, j, j).start()
    w_copy(1).start()
    u_copy(1).start()
    d_copy(1).start()

    barrier = pltpu.get_barrier_semaphore()
    for d in range(1, n_dev):
        pl.semaphore_signal(barrier, inc=1, device_id=((me + d) % n_dev,), device_id_type=MESH)

    ones = jnp.ones((8, tok), jnp.bfloat16)
    row_id = lax.broadcasted_iota(jnp.int32, (8, 2 * n_exp), 0)
    e_id = lax.broadcasted_iota(jnp.int32, (n_exp, tok), 0)

    def count_rows(part_no, r0, r1):
        cnt = jnp.zeros((8, 2 * n_exp), jnp.float32)
        for r in range(r0, r1):
            hots = []
            for h in range(2):
                ids = idx_v[2 * r + h]
                acc = jnp.zeros((n_exp, tok), jnp.float32)
                for k in range(top_k):
                    acc = jnp.where(e_id == ids[k:k + 1], 1.0, acc)
                hots.append(acc.astype(jnp.bfloat16))
            both = jnp.concatenate(hots, axis=0)
            res = lax.dot_general(ones, both, NT, preferred_element_type=jnp.float32)
            cnt = jnp.where(row_id == r, res, cnt)
        cnt_src[part_no] = cnt
        cnt_in[part_no, me] = cnt

    def cnt_copy(p, to, frm):
        return pltpu.make_async_remote_copy(
            src_ref=cnt_src.at[p], dst_ref=cnt_in.at[p, frm], send_sem=cs_sem.at[p, to], recv_sem=cr_sem.at[p, frm],
            device_id=(to,), device_id_type=MESH)

    def send_counts(p):
        for d in range(1, n_dev):
            cnt_copy(p, (me + d) % n_dev, me).start()

    def take_counts(p, lo, hi):
        for d in range(1, n_dev):
            cnt_copy(p, (me + d) % n_dev, (me + d) % n_dev).wait_recv()
        tot = cnt_in[p, 0]
        for j in range(1, n_dev):
            tot = tot + cnt_in[p, j]
        cols = jnp.transpose(tot * pull)
        for i in range(lo, hi):
            o = (i % 2) * n_exp
            fcol[i] = jnp.broadcast_to(cols[o:o + n_exp, i // 2:i // 2 + 1], (n_exp, fcol.shape[2]))

    idx_copy.wait()
    count_rows(0, 0, 1)
    loss_acc[...] = jnp.zeros_like(loss_acc)

    def loss_copy(to, frm):
        return pltpu.make_async_remote_copy(
            src_ref=loss_src, dst_ref=loss_in.at[frm], send_sem=ls_sem.at[to], recv_sem=lr_sem.at[frm],
            device_id=(to,), device_id_type=MESH)

    def rcopy(stage, src, dst, m, dev):
        return pltpu.make_async_remote_copy(
            src_ref=src, dst_ref=dst, send_sem=s_sem.at[stage, m], recv_sem=r_sem.at[stage, m],
            device_id=(dev,), device_id_type=MESH)

    def c_pair(m):
        return rcopy(0, part.at[m, pl.ds(4 - half, 4)], rd.at[m], m, partner)

    def c_rs1(m):
        return rcopy(1, part.at[m, pl.ds(half + 2 - 2 * pa, 2)], r1.at[m], m, nbr_a)

    def c_rs2(m):
        return rcopy(2, part.at[m, pl.ds(quart + 1 - pb, 1)], r2.at[m], m, nbr_b)

    def c_ag1(m, p):
        return rcopy(3, fin.at[m, pl.ds(p, 1)], fin.at[m, pl.ds(p, 1)], m, nbr_b)

    def c_ag2(m, p):
        return rcopy(4, fin.at[m, pl.ds(p, 2)], fin.at[m, pl.ds(p, 2)], m, nbr_a)

    def c_out(m, p):
        return rcopy(5, fin.at[m, pl.ds(p, 4)], fin.at[m, pl.ds(p, 4)], m, partner)

    def do_a(m):
        c_pair(m).wait_recv()
        o = 2 - 2 * pa
        part[m, pl.ds(half + o, 2)] += rd[m, pl.ds(o, 2)]
        part[m, pl.ds(quart, 2)] += rd[m, pl.ds(2 * pa, 2)]
        c_rs1(m).start()

    def do_b(m):
        c_rs1(m).wait_recv()
        o = 1 - pb
        part[m, pl.ds(quart + o, 1)] += r1[m, pl.ds(o, 1)]
        part[m, pl.ds(mine, 1)] += r1[m, pl.ds(pb, 1)]
        c_rs2(m).start()

    def do_c(m):
        c_rs2(m).wait_recv()
        fin[m, pl.ds(mine, 1)] = part[m, pl.ds(mine, 1)] + r2[m]

    def do_ag1(m):
        c_ag1(m, mine).start()

    def do_d(m):
        c_ag1(m, quart + 1 - pb).wait_recv()
        c_ag2(m, quart).start()

    def do_e(m):
        c_ag2(m, half + 2 - 2 * pa).wait_recv()
        c_out(m, half).start()

    def do_f(m):
        c_out(m, 4 - half).wait_recv()

    hr = rows // 2
    lanes = 2 * ctok
    lane = lax.broadcasted_iota(jnp.int32, (top_k, lanes), 1)
    e_half = lax.broadcasted_iota(jnp.int32, (n_exp, lanes), 0)
    first = lax.broadcasted_iota(jnp.int32, (top_k, lanes), 0) == 0
    scale = float(tok_all)
    pull = AUX_COEF * n_exp / (top_k * tok_all)

    def slot_chunk(lay, c, slot):
        lo = (c // 2) * lanes
        dcols = dbuf[lay % NU, lo:lo + lanes, :]
        s = [lax.dot_general(ebuf[slot, h * hr:(h + 1) * hr, :], dcols, NT, preferred_element_type=jnp.float32) for h in range(2)]
        acc = jnp.zeros((top_k, lanes), jnp.float32)
        for i in range(ctok):
            j = i * top_k
            acc = jnp.where(lane == (c % 2) * ctok + i, s[j // hr][j % hr:j % hr + top_k], acc)
        if c % 2:
            slot_v[lay % 2, :, lo:lo + lanes] += acc
        else:
            slot_v[lay % 2, :, lo:lo + lanes] = acc

    def logit_part(lay):
        for h in range(2):
            lo = h * lanes
            lg_v[:, lo:lo + lanes] = lax.dot_general(
                wv[lay], ubuf[lay % NU, lo:lo + lanes, :], NT, preferred_element_type=jnp.float32)

    def g_part(lay, to, h, keep):
        lo = h * lanes
        logits = lg_v[:, lo:lo + lanes]
        ids = idx_v[lay, :, lo:lo + lanes]
        ex = jnp.exp(logits - jnp.max(logits, axis=0, keepdims=True))
        prob = ex / jnp.sum(ex, axis=0, keepdims=True)
        chosen = jnp.concatenate(
            [jnp.sum(jnp.where(e_half == ids[k:k + 1], logits, 0.0), axis=0, keepdims=True) for k in range(top_k)], axis=0)
        ge = jnp.exp(chosen - jnp.max(chosen, axis=0, keepdims=True))
        gate = ge / jnp.sum(ge, axis=0, keepdims=True)
        slots = slot_v[lay % 2, :, lo:lo + lanes]
        dd = scale * slots
        dch = gate * (dd - jnp.sum(gate * dd, axis=0, keepdims=True))
        pf = prob * fcol[lay]
        pf_sum = jnp.sum(pf, axis=0, keepdims=True)
        g = pf - prob * pf_sum
        for k in range(top_k):
            g = g + jnp.where(e_half == ids[k:k + 1], dch[k:k + 1], 0.0)
        main = gate * slots + jnp.where(first, pf_sum * (1.0 / tok_all), 0.0)
        total = loss_acc[:, lo:lo + lanes] + main
        loss_acc[:, lo:lo + lanes] = total if keep is None else jnp.where(keep, total, loss_acc[:, lo:lo + lanes])
        gout[to, :, lo:lo + lanes] = g.astype(jnp.bfloat16)

    def p_part(lay, to):
        dim = ubuf.shape[2]
        for h in range(2):
            lo = h * (dim // 2)
            pg = jnp.dot(gout[to], ubuf[lay % NU, :, lo:lo + dim // 2], preferred_element_type=jnp.float32)
            part[to, :, :, lo:lo + dim // 2] = pg.reshape(part.shape[1:3] + (dim // 2,))

    def slot_of(lay, c):
        return (lay * NC + c) % NB

    def refill(lay, c):
        dl, dc = (c + NB) // NC, (c + NB) % NC

        @pl.when(lay + dl < n_lay)
        def _():
            e_copy(lay + dl, dc, slot_of(lay, c)).start()

    def fetch(copy, lay):
        @pl.when(lay + 2 < n_lay)
        def _():
            copy(lay + 2).start()

    run = {'a': do_a, 'b': do_b, 'c': do_c, 'g': do_ag1, 'd': do_d, 'e': do_e}

    w_copy(0).wait()
    u_copy(0).wait()
    d_copy(0).wait()
    for c in range(NC):
        e_copy(0, c, slot_of(0, c)).wait()
        slot_chunk(0, c, slot_of(0, c))
        if c == 0:
            pl.semaphore_wait(barrier, n_dev - 1)
            send_counts(0)
            logit_part(0)
        dl, dc = (c + NB) // NC, (c + NB) % NC
        e_copy(dl, dc, slot_of(0, c)).start()
    w_copy(2).start()
    u_copy(2).start()
    d_copy(2).start()
    take_counts(0, 0, 2)
    for h in range(2):
        g_part(0, 0, h, None)
    p_part(0, 0)
    c_pair(0).start()
    count_rows(1, 1, n_lay // 2)
    send_counts(1)

    @pl.loop(1, n_lay)
    def _(lay):
        prev = lay - 1
        to = jnp.where(lay == 1, lay, prev)
        keep = lay >= 2

        def comm(c):
            for k in 'abcgde':
                if FIRST[k][1] == c:
                    @pl.when(lay == FIRST[k][0])
                    def _(k=k):
                        run[k](0)
                if LAG[k][1] == c:
                    lag = LAG[k][0]
                    hi = min(n_lay, lag + AGL) if k in 'gde' else n_lay

                    @pl.when(jnp.logical_and(lay > lag, lay < hi))
                    def _(k=k, lag=lag):
                        run[k](lay - lag)

        comm(0)
        w_copy(lay).wait()
        u_copy(lay).wait()
        d_copy(lay).wait()
        e_copy(lay, 0, slot_of(lay, 0)).wait()
        slot_chunk(lay, 0, slot_of(lay, 0))
        g_part(prev, to, 0, keep)
        refill(lay, 0)
        fetch(d_copy, lay)

        comm(1)
        e_copy(lay, 1, slot_of(lay, 1)).wait()
        slot_chunk(lay, 1, slot_of(lay, 1))
        g_part(prev, to, 1, keep)
        refill(lay, 1)
        fetch(u_copy, lay)

        comm(2)
        e_copy(lay, 2, slot_of(lay, 2)).wait()
        slot_chunk(lay, 2, slot_of(lay, 2))
        p_part(prev, to)
        refill(lay, 2)
        fetch(w_copy, lay)

        @pl.when(lay >= 2)
        def _():
            c_pair(lay - 1).start()

        comm(3)
        e_copy(lay, 3, slot_of(lay, 3)).wait()
        slot_chunk(lay, 3, slot_of(lay, 3))
        logit_part(lay)
        refill(lay, 3)

        @pl.when(lay == 2)
        def _():
            take_counts(1, 2, n_lay)

    last = n_lay - 1
    for h in range(2):
        g_part(last, last, h, None)
    p_part(last, last)
    la = loss_acc[...]
    lv = la[:, :128]
    for j in range(1, tok // 128):
        lv = lv + la[:, 128 * j:128 * (j + 1)]
    loss_src[...] = lv
    loss_in[me] = lv
    c_pair(last).start()

    for d in range(1, n_dev):
        loss_copy((me + d) % n_dev, me).start()
    def sent(lo, hi):
        @pl.loop(lo, hi)
        def _(m):
            c_pair(m).wait_send()
            c_rs1(m).wait_send()
            c_rs2(m).wait_send()
            c_ag1(m, mine).wait_send()
            c_ag2(m, quart).wait_send()

    def whole(lo, hi):
        @pl.loop(lo, hi)
        def _(m):
            do_f(m)
            c_out(m, half).wait_send()

    def old(_):
        sent(0, OLD)
        whole(0, OLD)

    def take_loss(_):
        for d in range(1, n_dev):
            loss_copy((me + d) % n_dev, (me + d) % n_dev).wait_recv()
        tot = loss_in[0]
        for j in range(1, n_dev):
            tot = tot + loss_in[j]
        loss_out[...] = tot
        for d in range(1, n_dev):
            cnt_copy(0, (me + d) % n_dev, me).wait_send()
            cnt_copy(1, (me + d) % n_dev, me).wait_send()
            loss_copy((me + d) % n_dev, me).wait_send()

    run['x'], run['y'] = old, take_loss
    for k, back in DRAIN:
        run[k](last - back)
    sent(OLD, n_lay)
    whole(OLD, n_lay)


def out_kernel(n_lay, g_v, w_v, f_v, l_v, dn_hbm, dr_hbm, loss, stage, st_sem, f_sem):
    def put(lay):
        return pltpu.make_async_copy(stage.at[lay], dn_hbm.at[lay], st_sem.at[lay])

    def put_f(lay):
        return pltpu.make_async_copy(f_v.at[lay], dr_hbm.at[lay], f_sem.at[lay])

    @pl.loop(0, n_lay)
    def _(lay):
        put_f(lay).start()

    @pl.loop(0, n_lay)
    def _(lay):
        dn = lax.dot_general(g_v[lay], w_v[lay], TN, preferred_element_type=jnp.float32)
        stage[lay] = dn.astype(jnp.bfloat16)
        put(lay).start()

    loss[0, 0] = jnp.sum(l_v[...])

    @pl.loop(0, n_lay)
    def _(lay):
        put(lay).wait()
        put_f(lay).wait()


def solution(mesh):
    n_dev = mesh.shape['dp']

    def local_step(u_norm, expert_idx, expert_out, d_out, w_router):
        n_lay, tok, dim = u_norm.shape
        n_exp = w_router.shape[2]
        top_k = expert_idx.shape[2]
        tok_all = tok * n_dev
        f32, bf16 = jnp.float32, jnp.bfloat16
        idx_t = jnp.swapaxes(expert_idx, 1, 2)
        w_t = jnp.swapaxes(w_router, 1, 2)
        eo = expert_out.reshape(n_lay, tok * top_k, dim)
        rows = tok * top_k // NC
        pieces = 8
        prow = n_exp // pieces
        any_spec = pl.BlockSpec(memory_space=pl.ANY)
        vm_spec = pl.BlockSpec(memory_space=pltpu.VMEM)
        dma = pltpu.SemaphoreType.DMA
        fin, g_all, w_all, loss_v = pl.pallas_call(
            lambda *refs: step_kernel(n_lay, n_dev, tok_all, *refs),
            out_shape=(
                pltpu.VMEM((n_lay, pieces, prow, dim), f32),
                pltpu.VMEM((n_lay, n_exp, tok), bf16),
                pltpu.VMEM((n_lay, n_exp, dim), bf16),
                pltpu.VMEM((8, 128), f32),
            ),
            in_specs=[any_spec] * 5,
            out_specs=(vm_spec,) * 4,
            scratch_shapes=[
                pltpu.VMEM((n_lay, top_k, tok), jnp.int32),
                pltpu.VMEM((NB, rows, dim), bf16),
                pltpu.VMEM((NU, tok, dim), bf16),
                pltpu.VMEM((NU, tok, dim), bf16),
                pltpu.VMEM((n_lay, pieces, prow, dim), f32),
                pltpu.VMEM((n_lay, pieces // 2, prow, dim), f32),
                pltpu.VMEM((n_lay, pieces // 4, prow, dim), f32),
                pltpu.VMEM((n_lay, pieces // 8, prow, dim), f32),
                pltpu.VMEM((2, 8, 128), f32),
                pltpu.VMEM((2, n_dev, 8, 128), f32),
                pltpu.VMEM((8, 128), f32),
                pltpu.VMEM((n_dev, 8, 128), f32),
                pltpu.VMEM((n_lay, n_exp, 128), f32),
                pltpu.VMEM((2, top_k, tok), f32),
                pltpu.VMEM((n_exp, tok), f32),
                pltpu.VMEM((top_k, tok), f32),
                dma, dma((NB,)), dma((NU,)), dma((NU,)), dma((n_lay,)),
                dma((2, n_dev)), dma((2, n_dev)), dma((n_dev,)), dma((n_dev,)),
                dma((6, n_lay)), dma((6, n_lay)),
            ],
            compiler_params=pltpu.CompilerParams(
                collective_id=0, has_side_effects=True, vmem_limit_bytes=48 << 20),
            name='router_step',
        )(idx_t, eo, d_out, u_norm, w_t)
        d_norm, d_rt, loss = pl.pallas_call(
            lambda *refs: out_kernel(n_lay, *refs),
            out_shape=(
                jax.ShapeDtypeStruct((n_lay, tok, dim), bf16),
                jax.ShapeDtypeStruct((n_lay, pieces, prow, dim), f32),
                jax.ShapeDtypeStruct((1, 1), f32),
            ),
            in_specs=[vm_spec] * 4,
            out_specs=(any_spec, any_spec, pl.BlockSpec(memory_space=pltpu.SMEM)),
            scratch_shapes=[pltpu.VMEM((n_lay, tok, dim), bf16), dma((n_lay,)), dma((n_lay,))],
            compiler_params=pltpu.CompilerParams(vmem_limit_bytes=20 << 20),
            name='router_out',
        )(g_all, w_all, fin, loss_v)
        d_router = jnp.swapaxes(d_rt.reshape(n_lay, n_exp, dim), 1, 2)
        return loss[0, 0], d_router, d_norm

    tok_spec = P(None, 'dp', None)
    return jax.shard_map(local_step, mesh=mesh, in_specs=(tok_spec, tok_spec, P(None, 'dp', None, None), tok_spec, P()), out_specs=(P(), P(), tok_spec), check_vma=False)
```

```python
import jax
import jax.numpy as jnp
from jax import lax
from jax.experimental import pallas as pl
from jax.experimental.pallas import tpu as pltpu
from jax.sharding import PartitionSpec as P

AUX_COEF = 0.02
MESH = pl.DeviceIdType.MESH

NB = 3
NC = 4
NU = 4
AGL = 10
LAG = {'a': (2, 1), 'b': (3, 3), 'c': (4, 3), 'g': (4, 3), 'd': (6, 0), 'e': (7, 3)}
FIRST = {'a': (1, 2), 'b': (2, 3), 'c': (3, 3), 'g': (3, 3), 'd': (4, 3), 'e': (6, 1)}
DRAIN = (('a', 1), ('g', 5), ('e', 6), ('g', 4), ('a', 0), ('b', 2), ('c', 3), ('g', 3), ('d', 5), ('b', 1), ('d', 4),
         ('c', 2), ('g', 2), ('b', 0), ('d', 3), ('c', 1), ('g', 1), ('e', 5), ('d', 2), ('x', 0), ('c', 0), ('g', 0), ('e', 4),
         ('d', 1), ('e', 3), ('y', 0), ('d', 0), ('e', 2), ('e', 1), ('e', 0))
OLD = 9

NT = (((1,), (1,)), ((), ()))
TN = (((0,), (0,)), ((), ()))


def step_kernel(n_lay, n_dev, tok_all, idx_hbm, eo_hbm, dy_hbm, u_hbm, w_hbm,
                fin, gout, wv, loss_out,
                idx_v, ebuf, ubuf, dbuf, part, rd, r1, r2, cnt_src, cnt_in, loss_src, loss_in,
                fcol, slot_v, lg_v, loss_acc,
                idx_sem, e_sem, u_sem, d_sem, w_sem, cs_sem, cr_sem, ls_sem, lr_sem, s_sem, r_sem):
    me = lax.axis_index('dp')
    core = me % 2
    xpos = (me // 2) % 2
    ypos = me // 4
    partner = me + 1 - 2 * core
    xn = me + 2 - 4 * xpos
    yn = me + 4 - 8 * ypos
    nbr_a = xn * (1 - core) + yn * core
    nbr_b = yn * (1 - core) + xn * core
    pa = xpos * (1 - core) + ypos * core
    pb = ypos * (1 - core) + xpos * core
    half = 4 * core
    quart = half + 2 * pa
    mine = quart + pb
    n_exp = w_hbm.shape[1]
    top_k = idx_hbm.shape[1]
    tok = u_hbm.shape[1]
    rows = ebuf.shape[1]
    ctok = rows // top_k

    def e_copy(lay, c, slot):
        return pltpu.make_async_copy(eo_hbm.at[lay, pl.ds(c * rows, rows)], ebuf.at[slot], e_sem.at[slot])

    def u_copy(lay):
        return pltpu.make_async_copy(u_hbm.at[lay], ubuf.at[lay % NU], u_sem.at[lay % NU])

    def d_copy(lay):
        return pltpu.make_async_copy(dy_hbm.at[lay], dbuf.at[lay % NU], d_sem.at[lay % NU])

    def w_copy(lay):
        return pltpu.make_async_copy(w_hbm.at[lay], wv.at[lay], w_sem.at[lay])

    idx_copy = pltpu.make_async_copy(idx_hbm, idx_v, idx_sem)
    idx_copy.start()
    w_copy(0).start()
    u_copy(0).start()
    d_copy(0).start()
    for j in range(NB):
        e_copy(0, j, j).start()
    w_copy(1).start()
    u_copy(1).start()
    d_copy(1).start()

    barrier = pltpu.get_barrier_semaphore()
    for d in range(1, n_dev):
        pl.semaphore_signal(barrier, inc=1, device_id=((me + d) % n_dev,), device_id_type=MESH)

    ones = jnp.ones((8, tok), jnp.bfloat16)
    row_id = lax.broadcasted_iota(jnp.int32, (8, 2 * n_exp), 0)
    e_id = lax.broadcasted_iota(jnp.int32, (n_exp, tok), 0)

    def count_rows(part_no, r0, r1):
        cnt = jnp.zeros((8, 2 * n_exp), jnp.float32)
        for r in range(r0, r1):
            hots = []
            for h in range(2):
                ids = idx_v[2 * r + h]
                acc = jnp.zeros((n_exp, tok), jnp.float32)
                for k in range(top_k):
                    acc = jnp.where(e_id == ids[k:k + 1], 1.0, acc)
                hots.append(acc.astype(jnp.bfloat16))
            both = jnp.concatenate(hots, axis=0)
            res = lax.dot_general(ones, both, NT, preferred_element_type=jnp.float32)
            cnt = jnp.where(row_id == r, res, cnt)
        cnt_src[part_no] = cnt
        cnt_in[part_no, me] = cnt

    def cnt_copy(p, to, frm):
        return pltpu.make_async_remote_copy(
            src_ref=cnt_src.at[p], dst_ref=cnt_in.at[p, frm], send_sem=cs_sem.at[p, to], recv_sem=cr_sem.at[p, frm],
            device_id=(to,), device_id_type=MESH)

    def send_counts(p):
        for d in range(1, n_dev):
            cnt_copy(p, (me + d) % n_dev, me).start()

    def take_counts(p, lo, hi):
        for d in range(1, n_dev):
            cnt_copy(p, (me + d) % n_dev, (me + d) % n_dev).wait_recv()
        tot = cnt_in[p, 0]
        for j in range(1, n_dev):
            tot = tot + cnt_in[p, j]
        cols = jnp.transpose(tot * pull)
        for i in range(lo, hi):
            o = (i % 2) * n_exp
            fcol[i] = jnp.broadcast_to(cols[o:o + n_exp, i // 2:i // 2 + 1], (n_exp, fcol.shape[2]))

    idx_copy.wait()
    count_rows(0, 0, 1)
    loss_acc[...] = jnp.zeros_like(loss_acc)
    pl.semaphore_wait(barrier, n_dev - 1)
    send_counts(0)

    def loss_copy(to, frm):
        return pltpu.make_async_remote_copy(
            src_ref=loss_src, dst_ref=loss_in.at[frm], send_sem=ls_sem.at[to], recv_sem=lr_sem.at[frm],
            device_id=(to,), device_id_type=MESH)

    def rcopy(stage, src, dst, m, dev):
        return pltpu.make_async_remote_copy(
            src_ref=src, dst_ref=dst, send_sem=s_sem.at[stage, m], recv_sem=r_sem.at[stage, m],
            device_id=(dev,), device_id_type=MESH)

    def c_pair(m):
        return rcopy(0, part.at[m, pl.ds(4 - half, 4)], rd.at[m], m, partner)

    def c_rs1(m):
        return rcopy(1, part.at[m, pl.ds(half + 2 - 2 * pa, 2)], r1.at[m], m, nbr_a)

    def c_rs2(m):
        return rcopy(2, part.at[m, pl.ds(quart + 1 - pb, 1)], r2.at[m], m, nbr_b)

    def c_ag1(m, p):
        return rcopy(3, fin.at[m, pl.ds(p, 1)], fin.at[m, pl.ds(p, 1)], m, nbr_b)

    def c_ag2(m, p):
        return rcopy(4, fin.at[m, pl.ds(p, 2)], fin.at[m, pl.ds(p, 2)], m, nbr_a)

    def c_out(m, p):
        return rcopy(5, fin.at[m, pl.ds(p, 4)], fin.at[m, pl.ds(p, 4)], m, partner)

    def do_a(m):
        c_pair(m).wait_recv()
        o = 2 - 2 * pa
        part[m, pl.ds(half + o, 2)] += rd[m, pl.ds(o, 2)]
        part[m, pl.ds(quart, 2)] += rd[m, pl.ds(2 * pa, 2)]
        c_rs1(m).start()

    def do_b(m):
        c_rs1(m).wait_recv()
        o = 1 - pb
        part[m, pl.ds(quart + o, 1)] += r1[m, pl.ds(o, 1)]
        part[m, pl.ds(mine, 1)] += r1[m, pl.ds(pb, 1)]
        c_rs2(m).start()

    def do_c(m):
        c_rs2(m).wait_recv()
        fin[m, pl.ds(mine, 1)] = part[m, pl.ds(mine, 1)] + r2[m]

    def do_ag1(m):
        c_ag1(m, mine).start()

    def do_d(m):
        c_ag1(m, quart + 1 - pb).wait_recv()
        c_ag2(m, quart).start()

    def do_e(m):
        c_ag2(m, half + 2 - 2 * pa).wait_recv()
        c_out(m, half).start()

    def do_f(m):
        c_out(m, 4 - half).wait_recv()

    hr = rows // 2
    lanes = 2 * ctok
    lane = lax.broadcasted_iota(jnp.int32, (top_k, lanes), 1)
    e_half = lax.broadcasted_iota(jnp.int32, (n_exp, lanes), 0)
    first = lax.broadcasted_iota(jnp.int32, (top_k, lanes), 0) == 0
    scale = float(tok_all)
    pull = AUX_COEF * n_exp / (top_k * tok_all)

    def slot_chunk(lay, c, slot):
        lo = (c // 2) * lanes
        dcols = dbuf[lay % NU, lo:lo + lanes, :]
        s = [lax.dot_general(ebuf[slot, h * hr:(h + 1) * hr, :], dcols, NT, preferred_element_type=jnp.float32) for h in range(2)]
        acc = jnp.zeros((top_k, lanes), jnp.float32)
        for i in range(ctok):
            j = i * top_k
            acc = jnp.where(lane == (c % 2) * ctok + i, s[j // hr][j % hr:j % hr + top_k], acc)
        if c % 2:
            slot_v[lay % 2, :, lo:lo + lanes] += acc
        else:
            slot_v[lay % 2, :, lo:lo + lanes] = acc

    def logit_part(lay):
        for h in range(2):
            lo = h * lanes
            lg_v[:, lo:lo + lanes] = lax.dot_general(
                wv[lay], ubuf[lay % NU, lo:lo + lanes, :], NT, preferred_element_type=jnp.float32)

    def g_part(lay, to, h, keep):
        lo = h * lanes
        logits = lg_v[:, lo:lo + lanes]
        ids = idx_v[lay, :, lo:lo + lanes]
        ex = jnp.exp(logits - jnp.max(logits, axis=0, keepdims=True))
        prob = ex / jnp.sum(ex, axis=0, keepdims=True)
        chosen = jnp.concatenate(
            [jnp.sum(jnp.where(e_half == ids[k:k + 1], logits, 0.0), axis=0, keepdims=True) for k in range(top_k)], axis=0)
        ge = jnp.exp(chosen - jnp.max(chosen, axis=0, keepdims=True))
        gate = ge / jnp.sum(ge, axis=0, keepdims=True)
        slots = slot_v[lay % 2, :, lo:lo + lanes]
        dd = scale * slots
        dch = gate * (dd - jnp.sum(gate * dd, axis=0, keepdims=True))
        pf = prob * fcol[lay]
        pf_sum = jnp.sum(pf, axis=0, keepdims=True)
        g = pf - prob * pf_sum
        for k in range(top_k):
            g = g + jnp.where(e_half == ids[k:k + 1], dch[k:k + 1], 0.0)
        main = gate * slots + jnp.where(first, pf_sum * (1.0 / tok_all), 0.0)
        total = loss_acc[:, lo:lo + lanes] + main
        loss_acc[:, lo:lo + lanes] = total if keep is None else jnp.where(keep, total, loss_acc[:, lo:lo + lanes])
        gout[to, :, lo:lo + lanes] = g.astype(jnp.bfloat16)

    def p_part(lay, to):
        dim = ubuf.shape[2]
        for h in range(2):
            lo = h * (dim // 2)
            pg = jnp.dot(gout[to], ubuf[lay % NU, :, lo:lo + dim // 2], preferred_element_type=jnp.float32)
            part[to, :, :, lo:lo + dim // 2] = pg.reshape(part.shape[1:3] + (dim // 2,))

    def slot_of(lay, c):
        return (lay * NC + c) % NB

    def refill(lay, c):
        dl, dc = (c + NB) // NC, (c + NB) % NC

        @pl.when(lay + dl < n_lay)
        def _():
            e_copy(lay + dl, dc, slot_of(lay, c)).start()

    def fetch(copy, lay):
        @pl.when(lay + 2 < n_lay)
        def _():
            copy(lay + 2).start()

    run = {'a': do_a, 'b': do_b, 'c': do_c, 'g': do_ag1, 'd': do_d, 'e': do_e}

    w_copy(0).wait()
    u_copy(0).wait()
    d_copy(0).wait()
    for c in range(NC):
        e_copy(0, c, slot_of(0, c)).wait()
        slot_chunk(0, c, slot_of(0, c))
        if c == 0:
            logit_part(0)
        dl, dc = (c + NB) // NC, (c + NB) % NC
        e_copy(dl, dc, slot_of(0, c)).start()
    w_copy(2).start()
    u_copy(2).start()
    d_copy(2).start()
    take_counts(0, 0, 2)
    for h in range(2):
        g_part(0, 0, h, None)
    p_part(0, 0)
    c_pair(0).start()
    count_rows(1, 1, n_lay // 2)
    send_counts(1)

    @pl.loop(1, n_lay)
    def _(lay):
        prev = lay - 1
        to = jnp.where(lay == 1, lay, prev)
        keep = lay >= 2

        def comm(c):
            for k in 'abcgde':
                if FIRST[k][1] == c:
                    @pl.when(lay == FIRST[k][0])
                    def _(k=k):
                        run[k](0)
                if LAG[k][1] == c:
                    lag = LAG[k][0]
                    hi = min(n_lay, lag + AGL) if k in 'gde' else n_lay

                    @pl.when(jnp.logical_and(lay > lag, lay < hi))
                    def _(k=k, lag=lag):
                        run[k](lay - lag)

        comm(0)
        w_copy(lay).wait()
        u_copy(lay).wait()
        d_copy(lay).wait()
        e_copy(lay, 0, slot_of(lay, 0)).wait()
        slot_chunk(lay, 0, slot_of(lay, 0))
        g_part(prev, to, 0, keep)
        refill(lay, 0)
        fetch(d_copy, lay)

        comm(1)
        e_copy(lay, 1, slot_of(lay, 1)).wait()
        slot_chunk(lay, 1, slot_of(lay, 1))
        g_part(prev, to, 1, keep)
        refill(lay, 1)
        fetch(u_copy, lay)

        comm(2)
        e_copy(lay, 2, slot_of(lay, 2)).wait()
        slot_chunk(lay, 2, slot_of(lay, 2))
        p_part(prev, to)
        refill(lay, 2)
        fetch(w_copy, lay)

        @pl.when(lay >= 2)
        def _():
            c_pair(lay - 1).start()

        comm(3)
        e_copy(lay, 3, slot_of(lay, 3)).wait()
        slot_chunk(lay, 3, slot_of(lay, 3))
        logit_part(lay)
        refill(lay, 3)

        @pl.when(lay == 2)
        def _():
            take_counts(1, 2, n_lay)

    last = n_lay - 1
    for h in range(2):
        g_part(last, last, h, None)
    p_part(last, last)
    la = loss_acc[...]
    lv = la[:, :128]
    for j in range(1, tok // 128):
        lv = lv + la[:, 128 * j:128 * (j + 1)]
    loss_src[...] = lv
    loss_in[me] = lv
    c_pair(last).start()

    for d in range(1, n_dev):
        loss_copy((me + d) % n_dev, me).start()
    def sent(lo, hi):
        @pl.loop(lo, hi)
        def _(m):
            c_pair(m).wait_send()
            c_rs1(m).wait_send()
            c_rs2(m).wait_send()
            c_ag1(m, mine).wait_send()
            c_ag2(m, quart).wait_send()

    def whole(lo, hi):
        @pl.loop(lo, hi)
        def _(m):
            do_f(m)
            c_out(m, half).wait_send()

    def old(_):
        sent(0, OLD)
        whole(0, OLD)

    def take_loss(_):
        for d in range(1, n_dev):
            loss_copy((me + d) % n_dev, (me + d) % n_dev).wait_recv()
        tot = loss_in[0]
        for j in range(1, n_dev):
            tot = tot + loss_in[j]
        loss_out[...] = tot
        for d in range(1, n_dev):
            cnt_copy(0, (me + d) % n_dev, me).wait_send()
            cnt_copy(1, (me + d) % n_dev, me).wait_send()
            loss_copy((me + d) % n_dev, me).wait_send()

    run['x'], run['y'] = old, take_loss
    for k, back in DRAIN:
        run[k](last - back)
    sent(OLD, n_lay)
    whole(OLD, n_lay)


def out_kernel(n_lay, g_v, w_v, f_v, l_v, dn_hbm, dr_hbm, loss, stage, st_sem, f_sem):
    def put(lay):
        return pltpu.make_async_copy(stage.at[lay], dn_hbm.at[lay], st_sem.at[lay])

    def put_f(lay):
        return pltpu.make_async_copy(f_v.at[lay], dr_hbm.at[lay], f_sem.at[lay])

    @pl.loop(0, n_lay)
    def _(lay):
        put_f(lay).start()

    @pl.loop(0, n_lay)
    def _(lay):
        dn = lax.dot_general(g_v[lay], w_v[lay], TN, preferred_element_type=jnp.float32)
        stage[lay] = dn.astype(jnp.bfloat16)
        put(lay).start()

    loss[0, 0] = jnp.sum(l_v[...])

    @pl.loop(0, n_lay)
    def _(lay):
        put(lay).wait()
        put_f(lay).wait()


def solution(mesh):
    n_dev = mesh.shape['dp']

    def local_step(u_norm, expert_idx, expert_out, d_out, w_router):
        n_lay, tok, dim = u_norm.shape
        n_exp = w_router.shape[2]
        top_k = expert_idx.shape[2]
        tok_all = tok * n_dev
        f32, bf16 = jnp.float32, jnp.bfloat16
        idx_t = jnp.swapaxes(expert_idx, 1, 2)
        w_t = jnp.swapaxes(w_router, 1, 2)
        eo = expert_out.reshape(n_lay, tok * top_k, dim)
        rows = tok * top_k // NC
        pieces = 8
        prow = n_exp // pieces
        any_spec = pl.BlockSpec(memory_space=pl.ANY)
        vm_spec = pl.BlockSpec(memory_space=pltpu.VMEM)
        dma = pltpu.SemaphoreType.DMA
        fin, g_all, w_all, loss_v = pl.pallas_call(
            lambda *refs: step_kernel(n_lay, n_dev, tok_all, *refs),
            out_shape=(
                pltpu.VMEM((n_lay, pieces, prow, dim), f32),
                pltpu.VMEM((n_lay, n_exp, tok), bf16),
                pltpu.VMEM((n_lay, n_exp, dim), bf16),
                pltpu.VMEM((8, 128), f32),
            ),
            in_specs=[any_spec] * 5,
            out_specs=(vm_spec,) * 4,
            scratch_shapes=[
                pltpu.VMEM((n_lay, top_k, tok), jnp.int32),
                pltpu.VMEM((NB, rows, dim), bf16),
                pltpu.VMEM((NU, tok, dim), bf16),
                pltpu.VMEM((NU, tok, dim), bf16),
                pltpu.VMEM((n_lay, pieces, prow, dim), f32),
                pltpu.VMEM((n_lay, pieces // 2, prow, dim), f32),
                pltpu.VMEM((n_lay, pieces // 4, prow, dim), f32),
                pltpu.VMEM((n_lay, pieces // 8, prow, dim), f32),
                pltpu.VMEM((2, 8, 128), f32),
                pltpu.VMEM((2, n_dev, 8, 128), f32),
                pltpu.VMEM((8, 128), f32),
                pltpu.VMEM((n_dev, 8, 128), f32),
                pltpu.VMEM((n_lay, n_exp, 128), f32),
                pltpu.VMEM((2, top_k, tok), f32),
                pltpu.VMEM((n_exp, tok), f32),
                pltpu.VMEM((top_k, tok), f32),
                dma, dma((NB,)), dma((NU,)), dma((NU,)), dma((n_lay,)),
                dma((2, n_dev)), dma((2, n_dev)), dma((n_dev,)), dma((n_dev,)),
                dma((6, n_lay)), dma((6, n_lay)),
            ],
            compiler_params=pltpu.CompilerParams(
                collective_id=0, has_side_effects=True, vmem_limit_bytes=48 << 20),
            name='router_step',
        )(idx_t, eo, d_out, u_norm, w_t)
        d_norm, d_rt, loss = pl.pallas_call(
            lambda *refs: out_kernel(n_lay, *refs),
            out_shape=(
                jax.ShapeDtypeStruct((n_lay, tok, dim), bf16),
                jax.ShapeDtypeStruct((n_lay, pieces, prow, dim), f32),
                jax.ShapeDtypeStruct((1, 1), f32),
            ),
            in_specs=[vm_spec] * 4,
            out_specs=(any_spec, any_spec, pl.BlockSpec(memory_space=pltpu.SMEM)),
            scratch_shapes=[pltpu.VMEM((n_lay, tok, dim), bf16), dma((n_lay,)), dma((n_lay,))],
            compiler_params=pltpu.CompilerParams(vmem_limit_bytes=20 << 20),
            name='router_out',
        )(g_all, w_all, fin, loss_v)
        d_router = jnp.swapaxes(d_rt.reshape(n_lay, n_exp, dim), 1, 2)
        return loss[0, 0], d_router, d_norm

    tok_spec = P(None, 'dp', None)
    return jax.shard_map(local_step, mesh=mesh, in_specs=(tok_spec, tok_spec, P(None, 'dp', None, None), tok_spec, P()), out_specs=(P(), P(), tok_spec), check_vma=False)
```

```python
import jax
import jax.numpy as jnp
from jax import lax
from jax.experimental import pallas as pl
from jax.experimental.pallas import tpu as pltpu
from jax.sharding import PartitionSpec as P

AUX_COEF = 0.02
MESH = pl.DeviceIdType.MESH

NB = 3
NC = 4
NU = 4
AGL = 10
LAG = {'a': (2, 1), 'b': (3, 3), 'c': (4, 3), 'g': (4, 3), 'd': (6, 0), 'e': (7, 3)}
FIRST = {'a': (1, 2), 'b': (2, 3), 'c': (3, 3), 'g': (3, 3), 'd': (4, 3), 'e': (6, 1)}
DRAIN = (('a', 1), ('g', 5), ('e', 6), ('g', 4), ('a', 0), ('b', 2), ('c', 3), ('g', 3), ('d', 5), ('b', 1), ('d', 4),
         ('c', 2), ('g', 2), ('b', 0), ('d', 3), ('c', 1), ('g', 1), ('e', 5), ('d', 2), ('x', 0), ('c', 0), ('g', 0), ('e', 4),
         ('d', 1), ('e', 3), ('y', 0), ('d', 0), ('e', 2), ('e', 1), ('e', 0))
OLD = 9

NT = (((1,), (1,)), ((), ()))
TN = (((0,), (0,)), ((), ()))


def step_kernel(n_lay, n_dev, tok_all, idx_hbm, eo_hbm, dy_hbm, u_hbm, w_hbm,
                fin, gout, wv, loss_out,
                idx_v, ebuf, ubuf, dbuf, part, rd, r1, r2, cnt_src, cnt_in, loss_src, loss_in,
                fcol, slot_v, lg_v, loss_acc,
                idx_sem, e_sem, u_sem, d_sem, w_sem, cs_sem, cr_sem, ls_sem, lr_sem, s_sem, r_sem):
    me = lax.axis_index('dp')
    core = me % 2
    xpos = (me // 2) % 2
    ypos = me // 4
    partner = me + 1 - 2 * core
    xn = me + 2 - 4 * xpos
    yn = me + 4 - 8 * ypos
    nbr_a = xn * (1 - core) + yn * core
    nbr_b = yn * (1 - core) + xn * core
    pa = xpos * (1 - core) + ypos * core
    pb = ypos * (1 - core) + xpos * core
    half = 4 * core
    quart = half + 2 * pa
    mine = quart + pb
    n_exp = w_hbm.shape[1]
    top_k = idx_hbm.shape[1]
    tok = u_hbm.shape[1]
    rows = ebuf.shape[1]
    ctok = rows // top_k

    def e_copy(lay, c, slot):
        return pltpu.make_async_copy(eo_hbm.at[lay, pl.ds(c * rows, rows)], ebuf.at[slot], e_sem.at[slot])

    def u_copy(lay):
        return pltpu.make_async_copy(u_hbm.at[lay], ubuf.at[lay % NU], u_sem.at[lay % NU])

    def d_copy(lay):
        return pltpu.make_async_copy(dy_hbm.at[lay], dbuf.at[lay % NU], d_sem.at[lay % NU])

    def w_copy(lay):
        return pltpu.make_async_copy(w_hbm.at[lay], wv.at[lay], w_sem.at[lay])

    idx_copy = pltpu.make_async_copy(idx_hbm, idx_v, idx_sem)
    idx_copy.start()
    d_copy(0).start()
    e_copy(0, 0, 0).start()
    e_copy(0, 1, 1).start()
    w_copy(0).start()
    u_copy(0).start()
    for j in range(2, NB):
        e_copy(0, j, j).start()
    d_copy(1).start()
    w_copy(1).start()
    u_copy(1).start()

    barrier = pltpu.get_barrier_semaphore()
    for d in range(1, n_dev):
        pl.semaphore_signal(barrier, inc=1, device_id=((me + d) % n_dev,), device_id_type=MESH)

    ones = jnp.ones((8, tok), jnp.bfloat16)
    row_id = lax.broadcasted_iota(jnp.int32, (8, 2 * n_exp), 0)
    e_id = lax.broadcasted_iota(jnp.int32, (n_exp, tok), 0)

    def count_rows(part_no, r0, r1):
        cnt = jnp.zeros((8, 2 * n_exp), jnp.float32)
        for r in range(r0, r1):
            hots = []
            for h in range(2):
                ids = idx_v[2 * r + h]
                acc = jnp.zeros((n_exp, tok), jnp.float32)
                for k in range(top_k):
                    acc = jnp.where(e_id == ids[k:k + 1], 1.0, acc)
                hots.append(acc.astype(jnp.bfloat16))
            both = jnp.concatenate(hots, axis=0)
            res = lax.dot_general(ones, both, NT, preferred_element_type=jnp.float32)
            cnt = jnp.where(row_id == r, res, cnt)
        cnt_src[part_no] = cnt
        cnt_in[part_no, me] = cnt

    def cnt_copy(p, to, frm):
        return pltpu.make_async_remote_copy(
            src_ref=cnt_src.at[p], dst_ref=cnt_in.at[p, frm], send_sem=cs_sem.at[p, to], recv_sem=cr_sem.at[p, frm],
            device_id=(to,), device_id_type=MESH)

    def send_counts(p):
        for d in range(1, n_dev):
            cnt_copy(p, (me + d) % n_dev, me).start()

    def take_counts(p, lo, hi):
        for d in range(1, n_dev):
            cnt_copy(p, (me + d) % n_dev, (me + d) % n_dev).wait_recv()
        tot = cnt_in[p, 0]
        for j in range(1, n_dev):
            tot = tot + cnt_in[p, j]
        cols = jnp.transpose(tot * pull)
        for i in range(lo, hi):
            o = (i % 2) * n_exp
            fcol[i] = jnp.broadcast_to(cols[o:o + n_exp, i // 2:i // 2 + 1], (n_exp, fcol.shape[2]))

    idx_copy.wait()
    count_rows(0, 0, 2)
    loss_acc[...] = jnp.zeros_like(loss_acc)
    pl.semaphore_wait(barrier, n_dev - 1)
    send_counts(0)

    def loss_copy(to, frm):
        return pltpu.make_async_remote_copy(
            src_ref=loss_src, dst_ref=loss_in.at[frm], send_sem=ls_sem.at[to], recv_sem=lr_sem.at[frm],
            device_id=(to,), device_id_type=MESH)

    def rcopy(stage, src, dst, m, dev):
        return pltpu.make_async_remote_copy(
            src_ref=src, dst_ref=dst, send_sem=s_sem.at[stage, m], recv_sem=r_sem.at[stage, m],
            device_id=(dev,), device_id_type=MESH)

    def c_pair(m):
        return rcopy(0, part.at[m, pl.ds(4 - half, 4)], rd.at[m], m, partner)

    def c_rs1(m):
        return rcopy(1, part.at[m, pl.ds(half + 2 - 2 * pa, 2)], r1.at[m], m, nbr_a)

    def c_rs2(m):
        return rcopy(2, part.at[m, pl.ds(quart + 1 - pb, 1)], r2.at[m], m, nbr_b)

    def c_ag1(m, p):
        return rcopy(3, fin.at[m, pl.ds(p, 1)], fin.at[m, pl.ds(p, 1)], m, nbr_b)

    def c_ag2(m, p):
        return rcopy(4, fin.at[m, pl.ds(p, 2)], fin.at[m, pl.ds(p, 2)], m, nbr_a)

    def c_out(m, p):
        return rcopy(5, fin.at[m, pl.ds(p, 4)], fin.at[m, pl.ds(p, 4)], m, partner)

    def do_a(m):
        c_pair(m).wait_recv()
        o = 2 - 2 * pa
        part[m, pl.ds(half + o, 2)] += rd[m, pl.ds(o, 2)]
        part[m, pl.ds(quart, 2)] += rd[m, pl.ds(2 * pa, 2)]
        c_rs1(m).start()

    def do_b(m):
        c_rs1(m).wait_recv()
        o = 1 - pb
        part[m, pl.ds(quart + o, 1)] += r1[m, pl.ds(o, 1)]
        part[m, pl.ds(mine, 1)] += r1[m, pl.ds(pb, 1)]
        c_rs2(m).start()

    def do_c(m):
        c_rs2(m).wait_recv()
        fin[m, pl.ds(mine, 1)] = part[m, pl.ds(mine, 1)] + r2[m]

    def do_ag1(m):
        c_ag1(m, mine).start()

    def do_d(m):
        c_ag1(m, quart + 1 - pb).wait_recv()
        c_ag2(m, quart).start()

    def do_e(m):
        c_ag2(m, half + 2 - 2 * pa).wait_recv()
        c_out(m, half).start()

    def do_f(m):
        c_out(m, 4 - half).wait_recv()

    hr = rows // 2
    lanes = 2 * ctok
    lane = lax.broadcasted_iota(jnp.int32, (top_k, lanes), 1)
    e_half = lax.broadcasted_iota(jnp.int32, (n_exp, lanes), 0)
    first = lax.broadcasted_iota(jnp.int32, (top_k, lanes), 0) == 0
    scale = float(tok_all)
    pull = AUX_COEF * n_exp / (top_k * tok_all)

    def slot_chunk(lay, c, slot):
        lo = (c // 2) * lanes
        dcols = dbuf[lay % NU, lo:lo + lanes, :]
        s = [lax.dot_general(ebuf[slot, h * hr:(h + 1) * hr, :], dcols, NT, preferred_element_type=jnp.float32) for h in range(2)]
        acc = jnp.zeros((top_k, lanes), jnp.float32)
        for i in range(ctok):
            j = i * top_k
            acc = jnp.where(lane == (c % 2) * ctok + i, s[j // hr][j % hr:j % hr + top_k], acc)
        if c % 2:
            slot_v[lay % 2, :, lo:lo + lanes] += acc
        else:
            slot_v[lay % 2, :, lo:lo + lanes] = acc

    def logit_part(lay):
        for h in range(2):
            lo = h * lanes
            lg_v[:, lo:lo + lanes] = lax.dot_general(
                wv[lay], ubuf[lay % NU, lo:lo + lanes, :], NT, preferred_element_type=jnp.float32)

    def g_part(lay, to, h, keep):
        lo = h * lanes
        logits = lg_v[:, lo:lo + lanes]
        ids = idx_v[lay, :, lo:lo + lanes]
        ex = jnp.exp(logits - jnp.max(logits, axis=0, keepdims=True))
        prob = ex / jnp.sum(ex, axis=0, keepdims=True)
        chosen = jnp.concatenate(
            [jnp.sum(jnp.where(e_half == ids[k:k + 1], logits, 0.0), axis=0, keepdims=True) for k in range(top_k)], axis=0)
        ge = jnp.exp(chosen - jnp.max(chosen, axis=0, keepdims=True))
        gate = ge / jnp.sum(ge, axis=0, keepdims=True)
        slots = slot_v[lay % 2, :, lo:lo + lanes]
        dd = scale * slots
        dch = gate * (dd - jnp.sum(gate * dd, axis=0, keepdims=True))
        pf = prob * fcol[lay]
        pf_sum = jnp.sum(pf, axis=0, keepdims=True)
        g = pf - prob * pf_sum
        for k in range(top_k):
            g = g + jnp.where(e_half == ids[k:k + 1], dch[k:k + 1], 0.0)
        main = gate * slots + jnp.where(first, pf_sum * (1.0 / tok_all), 0.0)
        total = loss_acc[:, lo:lo + lanes] + main
        loss_acc[:, lo:lo + lanes] = total if keep is None else jnp.where(keep, total, loss_acc[:, lo:lo + lanes])
        gout[to, :, lo:lo + lanes] = g.astype(jnp.bfloat16)

    def p_part(lay, to):
        dim = ubuf.shape[2]
        for h in range(2):
            lo = h * (dim // 2)
            pg = jnp.dot(gout[to], ubuf[lay % NU, :, lo:lo + dim // 2], preferred_element_type=jnp.float32)
            part[to, :, :, lo:lo + dim // 2] = pg.reshape(part.shape[1:3] + (dim // 2,))

    def slot_of(lay, c):
        return (lay * NC + c) % NB

    def refill(lay, c):
        dl, dc = (c + NB) // NC, (c + NB) % NC

        @pl.when(lay + dl < n_lay)
        def _():
            e_copy(lay + dl, dc, slot_of(lay, c)).start()

    def fetch(copy, lay):
        @pl.when(lay + 2 < n_lay)
        def _():
            copy(lay + 2).start()

    run = {'a': do_a, 'b': do_b, 'c': do_c, 'g': do_ag1, 'd': do_d, 'e': do_e}

    d_copy(0).wait()
    for c in range(NC):
        e_copy(0, c, slot_of(0, c)).wait()
        slot_chunk(0, c, slot_of(0, c))
        if c == NC - 1:
            w_copy(0).wait()
            u_copy(0).wait()
            logit_part(0)
        dl, dc = (c + NB) // NC, (c + NB) % NC
        e_copy(dl, dc, slot_of(0, c)).start()
    w_copy(2).start()
    u_copy(2).start()
    d_copy(2).start()
    take_counts(0, 0, 4)
    for h in range(2):
        g_part(0, 0, h, None)
    p_part(0, 0)
    c_pair(0).start()
    @pl.loop(1, n_lay)
    def _(lay):
        prev = lay - 1
        to = jnp.where(lay == 1, lay, prev)
        keep = lay >= 2

        def comm(c):
            for k in 'abcgde':
                if FIRST[k][1] == c:
                    @pl.when(lay == FIRST[k][0])
                    def _(k=k):
                        run[k](0)
                if LAG[k][1] == c:
                    lag = LAG[k][0]
                    hi = min(n_lay, lag + AGL) if k in 'gde' else n_lay

                    @pl.when(jnp.logical_and(lay > lag, lay < hi))
                    def _(k=k, lag=lag):
                        run[k](lay - lag)

        comm(0)
        w_copy(lay).wait()
        u_copy(lay).wait()
        d_copy(lay).wait()
        e_copy(lay, 0, slot_of(lay, 0)).wait()
        slot_chunk(lay, 0, slot_of(lay, 0))
        g_part(prev, to, 0, keep)
        refill(lay, 0)
        fetch(d_copy, lay)

        comm(1)
        e_copy(lay, 1, slot_of(lay, 1)).wait()
        slot_chunk(lay, 1, slot_of(lay, 1))
        g_part(prev, to, 1, keep)
        refill(lay, 1)
        fetch(u_copy, lay)

        comm(2)
        e_copy(lay, 2, slot_of(lay, 2)).wait()
        slot_chunk(lay, 2, slot_of(lay, 2))
        p_part(prev, to)
        refill(lay, 2)
        fetch(w_copy, lay)

        @pl.when(lay >= 2)
        def _():
            c_pair(lay - 1).start()

        comm(3)
        e_copy(lay, 3, slot_of(lay, 3)).wait()
        slot_chunk(lay, 3, slot_of(lay, 3))
        logit_part(lay)
        refill(lay, 3)

        @pl.when(lay == 2)
        def _():
            count_rows(1, 2, n_lay // 2)
            send_counts(1)

        @pl.when(lay == 4)
        def _():
            take_counts(1, 4, n_lay)

    last = n_lay - 1
    for h in range(2):
        g_part(last, last, h, None)
    p_part(last, last)
    la = loss_acc[...]
    lv = la[:, :128]
    for j in range(1, tok // 128):
        lv = lv + la[:, 128 * j:128 * (j + 1)]
    loss_src[...] = lv
    loss_in[me] = lv
    c_pair(last).start()

    for d in range(1, n_dev):
        loss_copy((me + d) % n_dev, me).start()
    def sent(lo, hi):
        @pl.loop(lo, hi)
        def _(m):
            c_pair(m).wait_send()
            c_rs1(m).wait_send()
            c_rs2(m).wait_send()
            c_ag1(m, mine).wait_send()
            c_ag2(m, quart).wait_send()

    def whole(lo, hi):
        @pl.loop(lo, hi)
        def _(m):
            do_f(m)
            c_out(m, half).wait_send()

    def old(_):
        sent(0, OLD)
        whole(0, OLD)

    def take_loss(_):
        for d in range(1, n_dev):
            loss_copy((me + d) % n_dev, (me + d) % n_dev).wait_recv()
        tot = loss_in[0]
        for j in range(1, n_dev):
            tot = tot + loss_in[j]
        loss_out[...] = tot
        for d in range(1, n_dev):
            cnt_copy(0, (me + d) % n_dev, me).wait_send()
            cnt_copy(1, (me + d) % n_dev, me).wait_send()
            loss_copy((me + d) % n_dev, me).wait_send()

    run['x'], run['y'] = old, take_loss
    for k, back in DRAIN:
        run[k](last - back)
    sent(OLD, n_lay)
    whole(OLD, n_lay)


def out_kernel(n_lay, g_v, w_v, f_v, l_v, dn_hbm, dr_hbm, loss, stage, st_sem, f_sem):
    def put(lay):
        return pltpu.make_async_copy(stage.at[lay], dn_hbm.at[lay], st_sem.at[lay])

    def put_f(lay):
        return pltpu.make_async_copy(f_v.at[lay], dr_hbm.at[lay], f_sem.at[lay])

    @pl.loop(0, n_lay)
    def _(lay):
        put_f(lay).start()

    @pl.loop(0, n_lay)
    def _(lay):
        dn = lax.dot_general(g_v[lay], w_v[lay], TN, preferred_element_type=jnp.float32)
        stage[lay] = dn.astype(jnp.bfloat16)
        put(lay).start()

    loss[0, 0] = jnp.sum(l_v[...])

    @pl.loop(0, n_lay)
    def _(lay):
        put(lay).wait()
        put_f(lay).wait()


def solution(mesh):
    n_dev = mesh.shape['dp']

    def local_step(u_norm, expert_idx, expert_out, d_out, w_router):
        n_lay, tok, dim = u_norm.shape
        n_exp = w_router.shape[2]
        top_k = expert_idx.shape[2]
        tok_all = tok * n_dev
        f32, bf16 = jnp.float32, jnp.bfloat16
        idx_t = jnp.swapaxes(expert_idx, 1, 2)
        w_t = jnp.swapaxes(w_router, 1, 2)
        eo = expert_out.reshape(n_lay, tok * top_k, dim)
        rows = tok * top_k // NC
        pieces = 8
        prow = n_exp // pieces
        any_spec = pl.BlockSpec(memory_space=pl.ANY)
        vm_spec = pl.BlockSpec(memory_space=pltpu.VMEM)
        dma = pltpu.SemaphoreType.DMA
        fin, g_all, w_all, loss_v = pl.pallas_call(
            lambda *refs: step_kernel(n_lay, n_dev, tok_all, *refs),
            out_shape=(
                pltpu.VMEM((n_lay, pieces, prow, dim), f32),
                pltpu.VMEM((n_lay, n_exp, tok), bf16),
                pltpu.VMEM((n_lay, n_exp, dim), bf16),
                pltpu.VMEM((8, 128), f32),
            ),
            in_specs=[any_spec] * 5,
            out_specs=(vm_spec,) * 4,
            scratch_shapes=[
                pltpu.VMEM((n_lay, top_k, tok), jnp.int32),
                pltpu.VMEM((NB, rows, dim), bf16),
                pltpu.VMEM((NU, tok, dim), bf16),
                pltpu.VMEM((NU, tok, dim), bf16),
                pltpu.VMEM((n_lay, pieces, prow, dim), f32),
                pltpu.VMEM((n_lay, pieces // 2, prow, dim), f32),
                pltpu.VMEM((n_lay, pieces // 4, prow, dim), f32),
                pltpu.VMEM((n_lay, pieces // 8, prow, dim), f32),
                pltpu.VMEM((2, 8, 128), f32),
                pltpu.VMEM((2, n_dev, 8, 128), f32),
                pltpu.VMEM((8, 128), f32),
                pltpu.VMEM((n_dev, 8, 128), f32),
                pltpu.VMEM((n_lay, n_exp, 128), f32),
                pltpu.VMEM((2, top_k, tok), f32),
                pltpu.VMEM((n_exp, tok), f32),
                pltpu.VMEM((top_k, tok), f32),
                dma, dma((NB,)), dma((NU,)), dma((NU,)), dma((n_lay,)),
                dma((2, n_dev)), dma((2, n_dev)), dma((n_dev,)), dma((n_dev,)),
                dma((6, n_lay)), dma((6, n_lay)),
            ],
            compiler_params=pltpu.CompilerParams(
                collective_id=0, has_side_effects=True, vmem_limit_bytes=48 << 20),
            name='router_step',
        )(idx_t, eo, d_out, u_norm, w_t)
        d_norm, d_rt, loss = pl.pallas_call(
            lambda *refs: out_kernel(n_lay, *refs),
            out_shape=(
                jax.ShapeDtypeStruct((n_lay, tok, dim), bf16),
                jax.ShapeDtypeStruct((n_lay, pieces, prow, dim), f32),
                jax.ShapeDtypeStruct((1, 1), f32),
            ),
            in_specs=[vm_spec] * 4,
            out_specs=(any_spec, any_spec, pl.BlockSpec(memory_space=pltpu.SMEM)),
            scratch_shapes=[pltpu.VMEM((n_lay, tok, dim), bf16), dma((n_lay,)), dma((n_lay,))],
            compiler_params=pltpu.CompilerParams(vmem_limit_bytes=20 << 20),
            name='router_out',
        )(g_all, w_all, fin, loss_v)
        d_router = jnp.swapaxes(d_rt.reshape(n_lay, n_exp, dim), 1, 2)
        return loss[0, 0], d_router, d_norm

    tok_spec = P(None, 'dp', None)
    return jax.shard_map(local_step, mesh=mesh, in_specs=(tok_spec, tok_spec, P(None, 'dp', None, None), tok_spec, P()), out_specs=(P(), P(), tok_spec), check_vma=False)
```

```python
import jax
import jax.numpy as jnp
from jax import lax
from jax.experimental import pallas as pl
from jax.experimental.pallas import tpu as pltpu
from jax.sharding import PartitionSpec as P

AUX_COEF = 0.02
MESH = pl.DeviceIdType.MESH

NB = 3
NC = 4
NU = 4
AGL = 12
LAG = {'a': (2, 1), 'b': (3, 3), 'c': (4, 3), 'g': (4, 3), 'd': (6, 0), 'e': (8, 1)}
FIRST = {'a': (1, 1), 'b': (2, 3), 'c': (3, 3), 'g': (3, 3), 'd': (5, 0), 'e': (6, 2)}
DRAIN = (('a', 1), ('d', 5), ('e', 7), ('e', 6), ('a', 0), ('b', 2), ('c', 3), ('d', 4), ('b', 1), ('g', 3), ('c', 2),
         ('e', 5), ('g', 2), ('b', 0), ('c', 1), ('g', 1), ('d', 3), ('e', 4), ('d', 2), ('x', 0), ('c', 0), ('g', 0), ('d', 1),
         ('e', 3), ('y', 0), ('d', 0), ('e', 2), ('e', 1), ('e', 0))
OLD = 9

NT = (((1,), (1,)), ((), ()))
TN = (((0,), (0,)), ((), ()))


def step_kernel(n_lay, n_dev, tok_all, idx_hbm, eo_hbm, dy_hbm, u_hbm, w_hbm,
                fin, gout, wv, loss_out,
                idx_v, ebuf, ubuf, dbuf, part, rd, r1, r2, cnt_src, cnt_in, loss_src, loss_in,
                fcol, slot_v, lg_v, loss_acc,
                idx_sem, e_sem, u_sem, d_sem, w_sem, cs_sem, cr_sem, ls_sem, lr_sem, s_sem, r_sem):
    me = lax.axis_index('dp')
    core = me % 2
    xpos = (me // 2) % 2
    ypos = me // 4
    partner = me + 1 - 2 * core
    xn = me + 2 - 4 * xpos
    yn = me + 4 - 8 * ypos
    nbr_a = xn * (1 - core) + yn * core
    nbr_b = yn * (1 - core) + xn * core
    pa = xpos * (1 - core) + ypos * core
    pb = ypos * (1 - core) + xpos * core
    half = 4 * core
    quart = half + 2 * pa
    mine = quart + pb
    n_exp = w_hbm.shape[1]
    top_k = idx_hbm.shape[1]
    tok = u_hbm.shape[1]
    rows = ebuf.shape[1]
    ctok = rows // top_k

    def e_copy(lay, c, slot):
        return pltpu.make_async_copy(eo_hbm.at[lay, pl.ds(c * rows, rows)], ebuf.at[slot], e_sem.at[slot])

    def u_copy(lay):
        return pltpu.make_async_copy(u_hbm.at[lay], ubuf.at[lay % NU], u_sem.at[lay % NU])

    def d_copy(lay):
        return pltpu.make_async_copy(dy_hbm.at[lay], dbuf.at[lay % NU], d_sem.at[lay % NU])

    def w_copy(lay):
        return pltpu.make_async_copy(w_hbm.at[lay], wv.at[lay], w_sem.at[lay])

    idx_copy = pltpu.make_async_copy(idx_hbm, idx_v, idx_sem)
    idx_copy.start()
    d_copy(0).start()
    e_copy(0, 0, 0).start()
    e_copy(0, 1, 1).start()
    w_copy(0).start()
    u_copy(0).start()
    for j in range(2, NB):
        e_copy(0, j, j).start()
    d_copy(1).start()
    w_copy(1).start()
    u_copy(1).start()

    barrier = pltpu.get_barrier_semaphore()
    for d in range(1, n_dev):
        pl.semaphore_signal(barrier, inc=1, device_id=((me + d) % n_dev,), device_id_type=MESH)

    ones = jnp.ones((8, tok), jnp.bfloat16)
    row_id = lax.broadcasted_iota(jnp.int32, (8, 2 * n_exp), 0)
    e_id = lax.broadcasted_iota(jnp.int32, (n_exp, tok), 0)

    def count_rows(part_no, r0, r1):
        cnt = jnp.zeros((8, 2 * n_exp), jnp.float32)
        for r in range(r0, r1):
            hots = []
            for h in range(2):
                ids = idx_v[2 * r + h]
                acc = jnp.zeros((n_exp, tok), jnp.float32)
                for k in range(top_k):
                    acc = jnp.where(e_id == ids[k:k + 1], 1.0, acc)
                hots.append(acc.astype(jnp.bfloat16))
            both = jnp.concatenate(hots, axis=0)
            res = lax.dot_general(ones, both, NT, preferred_element_type=jnp.float32)
            cnt = jnp.where(row_id == r, res, cnt)
        cnt_src[part_no] = cnt
        cnt_in[part_no, me] = cnt

    def cnt_copy(p, to, frm):
        return pltpu.make_async_remote_copy(
            src_ref=cnt_src.at[p], dst_ref=cnt_in.at[p, frm], send_sem=cs_sem.at[p, to], recv_sem=cr_sem.at[p, frm],
            device_id=(to,), device_id_type=MESH)

    def send_counts(p):
        for d in range(1, n_dev):
            cnt_copy(p, (me + d) % n_dev, me).start()

    def take_counts(p, lo, hi):
        for d in range(1, n_dev):
            cnt_copy(p, (me + d) % n_dev, (me + d) % n_dev).wait_recv()
        tot = cnt_in[p, 0]
        for j in range(1, n_dev):
            tot = tot + cnt_in[p, j]
        cols = jnp.transpose(tot * pull)
        for i in range(lo, hi):
            o = (i % 2) * n_exp
            fcol[i] = jnp.broadcast_to(cols[o:o + n_exp, i // 2:i // 2 + 1], (n_exp, fcol.shape[2]))

    idx_copy.wait()
    count_rows(0, 0, 2)
    loss_acc[...] = jnp.zeros_like(loss_acc)
    pl.semaphore_wait(barrier, n_dev - 1)
    send_counts(0)

    def loss_copy(to, frm):
        return pltpu.make_async_remote_copy(
            src_ref=loss_src, dst_ref=loss_in.at[frm], send_sem=ls_sem.at[to], recv_sem=lr_sem.at[frm],
            device_id=(to,), device_id_type=MESH)

    def rcopy(stage, src, dst, m, dev):
        return pltpu.make_async_remote_copy(
            src_ref=src, dst_ref=dst, send_sem=s_sem.at[stage, m], recv_sem=r_sem.at[stage, m],
            device_id=(dev,), device_id_type=MESH)

    def c_pair(m):
        return rcopy(0, part.at[m, pl.ds(4 - half, 4)], rd.at[m], m, partner)

    def c_rs1(m):
        return rcopy(1, part.at[m, pl.ds(half + 2 - 2 * pa, 2)], r1.at[m], m, nbr_a)

    def c_rs2(m):
        return rcopy(2, part.at[m, pl.ds(quart + 1 - pb, 1)], r2.at[m], m, nbr_b)

    def c_ag1(m, p):
        return rcopy(3, fin.at[m, pl.ds(p, 1)], fin.at[m, pl.ds(p, 1)], m, nbr_b)

    def c_ag2(m, p):
        return rcopy(4, fin.at[m, pl.ds(p, 2)], fin.at[m, pl.ds(p, 2)], m, nbr_a)

    def c_out(m, p):
        return rcopy(5, fin.at[m, pl.ds(p, 4)], fin.at[m, pl.ds(p, 4)], m, partner)

    def do_a(m):
        c_pair(m).wait_recv()
        o = 2 - 2 * pa
        part[m, pl.ds(half + o, 2)] += rd[m, pl.ds(o, 2)]
        part[m, pl.ds(quart, 2)] += rd[m, pl.ds(2 * pa, 2)]
        c_rs1(m).start()

    def do_b(m):
        c_rs1(m).wait_recv()
        o = 1 - pb
        part[m, pl.ds(quart + o, 1)] += r1[m, pl.ds(o, 1)]
        part[m, pl.ds(mine, 1)] += r1[m, pl.ds(pb, 1)]
        c_rs2(m).start()

    def do_c(m):
        c_rs2(m).wait_recv()
        fin[m, pl.ds(mine, 1)] = part[m, pl.ds(mine, 1)] + r2[m]

    def do_ag1(m):
        c_ag1(m, mine).start()

    def do_d(m):
        c_ag1(m, quart + 1 - pb).wait_recv()
        c_ag2(m, quart).start()

    def do_e(m):
        c_ag2(m, half + 2 - 2 * pa).wait_recv()
        c_out(m, half).start()

    def do_f(m):
        c_out(m, 4 - half).wait_recv()

    hr = rows // 2
    lanes = 2 * ctok
    lane = lax.broadcasted_iota(jnp.int32, (top_k, lanes), 1)
    e_half = lax.broadcasted_iota(jnp.int32, (n_exp, lanes), 0)
    first = lax.broadcasted_iota(jnp.int32, (top_k, lanes), 0) == 0
    scale = float(tok_all)
    pull = AUX_COEF * n_exp / (top_k * tok_all)

    def slot_chunk(lay, c, slot):
        lo = (c // 2) * lanes
        dcols = dbuf[lay % NU, lo:lo + lanes, :]
        s = [lax.dot_general(ebuf[slot, h * hr:(h + 1) * hr, :], dcols, NT, preferred_element_type=jnp.float32) for h in range(2)]
        acc = jnp.zeros((top_k, lanes), jnp.float32)
        for i in range(ctok):
            j = i * top_k
            acc = jnp.where(lane == (c % 2) * ctok + i, s[j // hr][j % hr:j % hr + top_k], acc)
        if c % 2:
            slot_v[lay % 2, :, lo:lo + lanes] += acc
        else:
            slot_v[lay % 2, :, lo:lo + lanes] = acc

    def logit_part(lay):
        for h in range(2):
            lo = h * lanes
            lg_v[:, lo:lo + lanes] = lax.dot_general(
                wv[lay], ubuf[lay % NU, lo:lo + lanes, :], NT, preferred_element_type=jnp.float32)

    def g_part(lay, to, h, keep):
        lo = h * lanes
        logits = lg_v[:, lo:lo + lanes]
        ids = idx_v[lay, :, lo:lo + lanes]
        ex = jnp.exp(logits - jnp.max(logits, axis=0, keepdims=True))
        prob = ex / jnp.sum(ex, axis=0, keepdims=True)
        chosen = jnp.concatenate(
            [jnp.sum(jnp.where(e_half == ids[k:k + 1], logits, 0.0), axis=0, keepdims=True) for k in range(top_k)], axis=0)
        ge = jnp.exp(chosen - jnp.max(chosen, axis=0, keepdims=True))
        gate = ge / jnp.sum(ge, axis=0, keepdims=True)
        slots = slot_v[lay % 2, :, lo:lo + lanes]
        dd = scale * slots
        dch = gate * (dd - jnp.sum(gate * dd, axis=0, keepdims=True))
        pf = prob * fcol[lay]
        pf_sum = jnp.sum(pf, axis=0, keepdims=True)
        g = pf - prob * pf_sum
        for k in range(top_k):
            g = g + jnp.where(e_half == ids[k:k + 1], dch[k:k + 1], 0.0)
        main = gate * slots + jnp.where(first, pf_sum * (1.0 / tok_all), 0.0)
        total = loss_acc[:, lo:lo + lanes] + main
        loss_acc[:, lo:lo + lanes] = total if keep is None else jnp.where(keep, total, loss_acc[:, lo:lo + lanes])
        gout[to, :, lo:lo + lanes] = g.astype(jnp.bfloat16)

    def p_part(lay, to):
        dim = ubuf.shape[2]
        for h in range(2):
            lo = h * (dim // 2)
            pg = jnp.dot(gout[to], ubuf[lay % NU, :, lo:lo + dim // 2], preferred_element_type=jnp.float32)
            part[to, :, :, lo:lo + dim // 2] = pg.reshape(part.shape[1:3] + (dim // 2,))

    def slot_of(lay, c):
        return (lay * NC + c) % NB

    def refill(lay, c):
        dl, dc = (c + NB) // NC, (c + NB) % NC

        @pl.when(lay + dl < n_lay)
        def _():
            e_copy(lay + dl, dc, slot_of(lay, c)).start()

    def fetch(copy, lay):
        @pl.when(lay + 2 < n_lay)
        def _():
            copy(lay + 2).start()

    run = {'a': do_a, 'b': do_b, 'c': do_c, 'g': do_ag1, 'd': do_d, 'e': do_e}

    d_copy(0).wait()
    for c in range(NC):
        e_copy(0, c, slot_of(0, c)).wait()
        slot_chunk(0, c, slot_of(0, c))
        if c == NC - 1:
            w_copy(0).wait()
            u_copy(0).wait()
            logit_part(0)
        dl, dc = (c + NB) // NC, (c + NB) % NC
        e_copy(dl, dc, slot_of(0, c)).start()
    w_copy(2).start()
    u_copy(2).start()
    d_copy(2).start()
    take_counts(0, 0, 4)
    for h in range(2):
        g_part(0, 0, h, None)
    p_part(0, 0)
    c_pair(0).start()
    @pl.loop(1, n_lay)
    def _(lay):
        prev = lay - 1
        to = jnp.where(lay == 1, lay, prev)
        keep = lay >= 2

        def comm(c):
            for k in 'abcgde':
                if FIRST[k][1] == c:
                    @pl.when(lay == FIRST[k][0])
                    def _(k=k):
                        run[k](0)
                if LAG[k][1] == c:
                    lag = LAG[k][0]
                    hi = min(n_lay, lag + AGL) if k in 'gde' else n_lay

                    @pl.when(jnp.logical_and(lay > lag, lay < hi))
                    def _(k=k, lag=lag):
                        run[k](lay - lag)

        comm(0)
        w_copy(lay).wait()
        u_copy(lay).wait()
        d_copy(lay).wait()
        e_copy(lay, 0, slot_of(lay, 0)).wait()
        slot_chunk(lay, 0, slot_of(lay, 0))
        g_part(prev, to, 0, keep)
        refill(lay, 0)
        fetch(d_copy, lay)

        comm(1)
        e_copy(lay, 1, slot_of(lay, 1)).wait()
        slot_chunk(lay, 1, slot_of(lay, 1))
        g_part(prev, to, 1, keep)
        refill(lay, 1)
        fetch(u_copy, lay)

        comm(2)
        e_copy(lay, 2, slot_of(lay, 2)).wait()
        slot_chunk(lay, 2, slot_of(lay, 2))
        p_part(prev, to)
        refill(lay, 2)
        fetch(w_copy, lay)

        @pl.when(lay >= 2)
        def _():
            c_pair(lay - 1).start()

        comm(3)
        e_copy(lay, 3, slot_of(lay, 3)).wait()
        slot_chunk(lay, 3, slot_of(lay, 3))
        logit_part(lay)
        refill(lay, 3)

        @pl.when(lay == 2)
        def _():
            count_rows(1, 2, n_lay // 2)
            send_counts(1)

        @pl.when(lay == 4)
        def _():
            take_counts(1, 4, n_lay)

    last = n_lay - 1
    for h in range(2):
        g_part(last, last, h, None)
    p_part(last, last)
    la = loss_acc[...]
    lv = la[:, :128]
    for j in range(1, tok // 128):
        lv = lv + la[:, 128 * j:128 * (j + 1)]
    loss_src[...] = lv
    loss_in[me] = lv
    c_pair(last).start()

    for d in range(1, n_dev):
        loss_copy((me + d) % n_dev, me).start()
    def sent(lo, hi):
        @pl.loop(lo, hi)
        def _(m):
            c_pair(m).wait_send()
            c_rs1(m).wait_send()
            c_rs2(m).wait_send()
            c_ag1(m, mine).wait_send()
            c_ag2(m, quart).wait_send()

    def whole(lo, hi):
        @pl.loop(lo, hi)
        def _(m):
            do_f(m)
            c_out(m, half).wait_send()

    def old(_):
        sent(0, OLD)
        whole(0, OLD)

    def take_loss(_):
        for d in range(1, n_dev):
            loss_copy((me + d) % n_dev, (me + d) % n_dev).wait_recv()
        tot = loss_in[0]
        for j in range(1, n_dev):
            tot = tot + loss_in[j]
        loss_out[...] = tot
        for d in range(1, n_dev):
            cnt_copy(0, (me + d) % n_dev, me).wait_send()
            cnt_copy(1, (me + d) % n_dev, me).wait_send()
            loss_copy((me + d) % n_dev, me).wait_send()

    run['x'], run['y'] = old, take_loss
    for k, back in DRAIN:
        run[k](last - back)
    sent(OLD, n_lay)
    whole(OLD, n_lay)


def out_kernel(n_lay, g_v, w_v, f_v, l_v, dn_hbm, dr_hbm, loss, stage, st_sem, f_sem):
    def put(lay):
        return pltpu.make_async_copy(stage.at[lay], dn_hbm.at[lay], st_sem.at[lay])

    def put_f(lay):
        return pltpu.make_async_copy(f_v.at[lay], dr_hbm.at[lay], f_sem.at[lay])

    @pl.loop(0, n_lay)
    def _(lay):
        put_f(lay).start()

    @pl.loop(0, n_lay)
    def _(lay):
        dn = lax.dot_general(g_v[lay], w_v[lay], TN, preferred_element_type=jnp.float32)
        stage[lay] = dn.astype(jnp.bfloat16)
        put(lay).start()

    loss[0, 0] = jnp.sum(l_v[...])

    @pl.loop(0, n_lay)
    def _(lay):
        put(lay).wait()
        put_f(lay).wait()


def solution(mesh):
    n_dev = mesh.shape['dp']

    def local_step(u_norm, expert_idx, expert_out, d_out, w_router):
        n_lay, tok, dim = u_norm.shape
        n_exp = w_router.shape[2]
        top_k = expert_idx.shape[2]
        tok_all = tok * n_dev
        f32, bf16 = jnp.float32, jnp.bfloat16
        idx_t = jnp.swapaxes(expert_idx, 1, 2)
        w_t = jnp.swapaxes(w_router, 1, 2)
        eo = expert_out.reshape(n_lay, tok * top_k, dim)
        rows = tok * top_k // NC
        pieces = 8
        prow = n_exp // pieces
        any_spec = pl.BlockSpec(memory_space=pl.ANY)
        vm_spec = pl.BlockSpec(memory_space=pltpu.VMEM)
        dma = pltpu.SemaphoreType.DMA
        fin, g_all, w_all, loss_v = pl.pallas_call(
            lambda *refs: step_kernel(n_lay, n_dev, tok_all, *refs),
            out_shape=(
                pltpu.VMEM((n_lay, pieces, prow, dim), f32),
                pltpu.VMEM((n_lay, n_exp, tok), bf16),
                pltpu.VMEM((n_lay, n_exp, dim), bf16),
                pltpu.VMEM((8, 128), f32),
            ),
            in_specs=[any_spec] * 5,
            out_specs=(vm_spec,) * 4,
            scratch_shapes=[
                pltpu.VMEM((n_lay, top_k, tok), jnp.int32),
                pltpu.VMEM((NB, rows, dim), bf16),
                pltpu.VMEM((NU, tok, dim), bf16),
                pltpu.VMEM((NU, tok, dim), bf16),
                pltpu.VMEM((n_lay, pieces, prow, dim), f32),
                pltpu.VMEM((n_lay, pieces // 2, prow, dim), f32),
                pltpu.VMEM((n_lay, pieces // 4, prow, dim), f32),
                pltpu.VMEM((n_lay, pieces // 8, prow, dim), f32),
                pltpu.VMEM((2, 8, 128), f32),
                pltpu.VMEM((2, n_dev, 8, 128), f32),
                pltpu.VMEM((8, 128), f32),
                pltpu.VMEM((n_dev, 8, 128), f32),
                pltpu.VMEM((n_lay, n_exp, 128), f32),
                pltpu.VMEM((2, top_k, tok), f32),
                pltpu.VMEM((n_exp, tok), f32),
                pltpu.VMEM((top_k, tok), f32),
                dma, dma((NB,)), dma((NU,)), dma((NU,)), dma((n_lay,)),
                dma((2, n_dev)), dma((2, n_dev)), dma((n_dev,)), dma((n_dev,)),
                dma((6, n_lay)), dma((6, n_lay)),
            ],
            compiler_params=pltpu.CompilerParams(
                collective_id=0, has_side_effects=True, vmem_limit_bytes=48 << 20),
            name='router_step',
        )(idx_t, eo, d_out, u_norm, w_t)
        d_norm, d_rt, loss = pl.pallas_call(
            lambda *refs: out_kernel(n_lay, *refs),
            out_shape=(
                jax.ShapeDtypeStruct((n_lay, tok, dim), bf16),
                jax.ShapeDtypeStruct((n_lay, pieces, prow, dim), f32),
                jax.ShapeDtypeStruct((1, 1), f32),
            ),
            in_specs=[vm_spec] * 4,
            out_specs=(any_spec, any_spec, pl.BlockSpec(memory_space=pltpu.SMEM)),
            scratch_shapes=[pltpu.VMEM((n_lay, tok, dim), bf16), dma((n_lay,)), dma((n_lay,))],
            compiler_params=pltpu.CompilerParams(vmem_limit_bytes=20 << 20),
            name='router_out',
        )(g_all, w_all, fin, loss_v)
        d_router = jnp.swapaxes(d_rt.reshape(n_lay, n_exp, dim), 1, 2)
        return loss[0, 0], d_router, d_norm

    tok_spec = P(None, 'dp', None)
    return jax.shard_map(local_step, mesh=mesh, in_specs=(tok_spec, tok_spec, P(None, 'dp', None, None), tok_spec, P()), out_specs=(P(), P(), tok_spec), check_vma=False)
```
